32 devices in a mesh: dp: 4 (over z), ctx: 2 (over y), tensor: 4 (over x, core).
Axes of the slice: x: 2, y: 2, z: 4, core: 2. Of those that a mesh axis runs over, the one named last changes fastest.
Arguments:
- hidden_in: bfloat16 [4, 1024, 2048], P('dp', 'ctx', 'tensor'), may hold values from -6 to 6
- segments: int32 [4, 1024], P('dp'), may hold values from 0 to 2, never falling along the last dimension, each value on 1 to 512 neighbouring positions
- ln_gain: float32 [2048], replicated, may hold values from 0.5 to 1.5
- ln_bias: float32 [2048], replicated, may hold values from -2 to 2
- qkv_weight: bfloat16 [2048, 3, 2048], P(('dp', 'ctx'), None, 'tensor'), may hold values from -1 to 1
- qkv_bias: float32 [3, 2048], P(None, 'tensor'), may hold values from -2 to 2
- dense_weight: bfloat16 [2048, 2048], P('tensor', ('dp', 'ctx')), may hold values from -0.75 to 0.75
- dense_bias: float32 [2048], P('tensor'), may hold values from -2 to 2
- fc1_weight: bfloat16 [2048, 8192], P(('dp', 'ctx'), 'tensor'), may hold values from -0.125 to 0.125
- fc1_bias: float32 [8192], P('tensor'), may hold values from -2 to 2
- fc2_weight: bfloat16 [8192, 2048], P('tensor', ('dp', 'ctx')), may hold values from -0.0625 to 0.0625
- fc2_bias: float32 [2048], P('tensor'), may hold values from -2 to 2
- cotangent: bfloat16 [4, 1024, 2048], P('dp', 'ctx', 'tensor'), may hold values from -6 to 6
Outputs:
- block_out: bfloat16 [4, 1024, 2048], P('dp', 'ctx', 'tensor')
- grad_input: float32 [4, 1024, 2048], P('dp', 'ctx', 'tensor')
- grad_qkv_weight: float32 [2048, 3, 2048], P(('dp', 'ctx'), None, 'tensor')
- grad_qkv_bias: float32 [3, 2048], P(None, 'tensor')
- grad_dense_weight: float32 [2048, 2048], P('tensor', ('dp', 'ctx'))
- grad_dense_bias: float32 [2048], P('tensor')
- grad_fc1_weight: float32 [2048, 8192], P(('dp', 'ctx'), 'tensor')
- grad_fc1_bias: float32 [8192], P('tensor')
- grad_fc2_weight: float32 [8192, 2048], P('tensor', ('dp', 'ctx'))
- grad_fc2_bias: float32 [2048], P('tensor')
- grad_ln_gain: float32 [2048], P('tensor')
- grad_ln_bias: float32 [2048], P('tensor')
The draws below stay inside these ranges and needn't reach their ends.
Inputs may be any that keep to these rules, and one draw needn't show every extreme that they name: `segments`: within a sequence, segment numbers never fall and each document holds at most 512 tokens.
All inputs are finite; a program needn't handle non-finite values.
Results may differ from the reference program's by a relative error of at most 0.013.
Values may be sent and summed in bfloat16 or wider, within the bound.
A program may use at most 256 MiB of HBM per device.

```python
import math
from functools import partial
import jax
import jax.numpy as jnp
import numpy as np
from jax import lax

D = 2048
H = 32
HD = 64
ROT = 32
FF = 8192
SEQ_LEN = 1024
SEQ_ALL = 4


def draw_qkv_weight(key, part):
    drawn = jax.random.normal(key, (D, 3, D), jnp.float32) / math.sqrt(D)
    return jnp.clip(drawn, -1.0, 1.0).astype(jnp.bfloat16)


def steps_of(rng, shape, split, least, top_value):
    def one(position, blocks):
        heights = jax.random.uniform(jax.random.fold_in(jax.random.fold_in(rng, 6), position), (blocks,), jnp.float32, least / len(split), top_value / len(split))
        return jnp.repeat(jnp.exp(heights), shape[position] // blocks).reshape((-1,) + (1,) * (len(shape) - position - 1))

    level = one(*split[0])
    for cut in split[1:]:
        level = level * one(*cut)
    return level


def split_up(number_of, total, most, slope):
    loads = [(1 << 20) // math.isqrt(rank ** slope) + 1 for rank in range(2, number_of + 1)]
    rest, counts = total - most - (number_of - 1), [1] * (number_of - 1)
    while rest > 0:
        free = [i for i in range(number_of - 1) if counts[i] < most]
        pool, remaining = sum([loads[i] for i in free]), rest
        for i in free:
            more = min(most - counts[i], max(1, remaining * loads[i] // pool), rest)
            counts[i] = counts[i] + more
            rest = rest - more
    return np.array([most] + counts)


def uneven(rng, number_of, total, most, skew):
    if number_of == 2:
        one = jax.random.randint(rng, (), max(1, total - most), min(most, total - 1) + 1)
        return jnp.stack([one, total - one])
    sizes = jnp.asarray(split_up(number_of, total, most, skew), jnp.int32)
    pairs = (number_of - 1) // 2
    source_of, receiver = sizes[1:1 + 2 * pairs:2], sizes[2:2 + 2 * pairs:2]
    margin = jnp.minimum(source_of - 1, most - receiver)
    moved = jax.random.randint(jax.random.fold_in(rng, 1), (pairs,), 0, 1 << 20) % (margin + 1)
    sizes = sizes.at[1:1 + 2 * pairs:2].set(source_of - moved).at[2:2 + 2 * pairs:2].set(receiver + moved)
    return sizes[jax.random.permutation(jax.random.fold_in(rng, 2), number_of)]


def noise(rng, extent, spread, most, cuts=(), kind=jnp.bfloat16):
    array = spread * jax.random.normal(rng, extent, jnp.float32)
    if cuts:
        array = array * steps_of(rng, extent, cuts, -0.22, 0.18)
    return jnp.clip(array, -most, most).astype(kind)


def setup_inputs(seed: int = 0) -> dict:
    streams_of = jax.random.split(jax.random.key(seed), 14)
    hidden_in = noise(streams_of[0], (SEQ_ALL, SEQ_LEN, D), 1.0, 6.0, ((0, 4), (1, 2), (2, 4)))
    segments = jax.vmap(lambda own: jnp.searchsorted(jnp.cumsum(uneven(own, max(3, SEQ_LEN // 512), SEQ_LEN, SEQ_LEN // 2, 1)), jnp.arange(SEQ_LEN), side="right"))(jax.random.split(streams_of[1], SEQ_ALL)).reshape((SEQ_ALL, SEQ_LEN)).astype(jnp.int32)
    ln_gain = jnp.clip(1.0 + 0.1 * jax.random.normal(streams_of[2], (D,), jnp.float32), 0.5, 1.5)
    ln_bias = noise(streams_of[3], (D,), 0.3, 2.0, (), jnp.float32)
    qkv_weight = draw_qkv_weight(jax.random.fold_in(streams_of[13], 71), 0)
    qkv_bias = noise(streams_of[5], (3, D), 0.3, 2.0, ((1, 4),), jnp.float32)
    dense_weight = noise(streams_of[6], (D, D), HD ** -0.5, 0.75, ((0, 4), (1, 8)))
    dense_bias = noise(streams_of[7], (D,), 0.3, 2.0, ((0, 4),), jnp.float32)
    fc1_weight = noise(streams_of[8], (D, FF), D ** -0.5, 0.125, ((0, 8), (1, 4)))
    fc1_bias = noise(streams_of[9], (FF,), 0.3, 2.0, ((0, 4),), jnp.float32)
    fc2_weight = noise(streams_of[10], (FF, D), FF ** -0.5, 0.0625, ((0, 4), (1, 8)))
    fc2_bias = noise(streams_of[11], (D,), 0.3, 2.0, ((0, 4),), jnp.float32)
    cotangent = noise(streams_of[12], (SEQ_ALL, SEQ_LEN, D), 1.0, 6.0, ((0, 4), (1, 2), (2, 4)))
    return dict(hidden_in=hidden_in, segments=segments, ln_gain=ln_gain, ln_bias=ln_bias, qkv_weight=qkv_weight, qkv_bias=qkv_bias, dense_weight=dense_weight, dense_bias=dense_bias, fc1_weight=fc1_weight, fc1_bias=fc1_bias, fc2_weight=fc2_weight, fc2_bias=fc2_bias, cotangent=cotangent)


ln_eps = 1e-05
rope_base = 10000.0
mask_fill = -1e+30

def doc_positions(segment_ids):
    last_axis = segment_ids.ndim - 1
    index_all = lax.broadcasted_iota(jnp.int32, segment_ids.shape, last_axis)
    first_col = jnp.ones(segment_ids.shape[:-1] + (1,), dtype=jnp.bool_)
    change = jnp.concatenate([first_col, segment_ids[..., 1:] != segment_ids[..., :-1]], axis=last_axis)
    starts = lax.cummax(jnp.where(change, index_all, 0).astype(jnp.int32), axis=last_axis)
    return (index_all - starts).astype(jnp.int32)

def rope_tables(segment_ids):
    half_rot = ROT // 2
    freqs = rope_base ** (-(jnp.arange(half_rot, dtype=jnp.float32) * 2.0) / ROT)
    angles = doc_positions(segment_ids).astype(jnp.float32)[..., None] * freqs
    return (jnp.cos(angles), jnp.sin(angles))

def rotate(values_in, cosine, sine):
    half_rot = ROT // 2
    first_half = values_in[..., :half_rot]
    second_half = values_in[..., half_rot:ROT]
    return jnp.concatenate([first_half * cosine - second_half * sine, second_half * cosine + first_half * sine, values_in[..., ROT:]], axis=-1)

def unrotate(grads_in, cosine, sine):
    half_rot = ROT // 2
    first_half = grads_in[..., :half_rot]
    second_half = grads_in[..., half_rot:ROT]
    return jnp.concatenate([first_half * cosine + second_half * sine, second_half * cosine - first_half * sine, grads_in[..., ROT:]], axis=-1)

def head_scores(queries, keys_rot, allowed):
    raw_scores = jnp.einsum('qd,kd->qk', queries.astype(jnp.float32), keys_rot.astype(jnp.float32)) * (1.0 / math.sqrt(HD))
    return jnp.where(allowed, raw_scores, mask_fill)

def reference(hidden_in, segments, ln_gain, ln_bias, qkv_weight, qkv_bias, dense_weight, dense_bias, fc1_weight, fc1_bias, fc2_weight, fc2_bias, cotangent):
    flat_qkv = qkv_weight.reshape(D, 3 * D)
    scale = 1.0 / math.sqrt(HD)
    gelu_tanh = partial(jax.nn.gelu, approximate=True)

    def one_sequence(carry, inputs):
        hidden_seq, seg_seq, cot_seq = inputs
        inputs_f = hidden_seq.astype(jnp.float32)
        mean_val = lax.optimization_barrier(jnp.mean(inputs_f, axis=1, keepdims=True))
        centered = inputs_f - mean_val
        inv_std = lax.rsqrt(lax.optimization_barrier(jnp.mean(centered * centered, axis=1, keepdims=True)) + ln_eps)
        standard = centered * inv_std
        normed = (standard * ln_gain + ln_bias).astype(jnp.bfloat16)
        projected = (jnp.dot(normed, flat_qkv, preferred_element_type=jnp.float32) + qkv_bias.reshape(-1)).astype(jnp.bfloat16)
        hidden_pre = jnp.dot(normed, fc1_weight, preferred_element_type=jnp.float32) + fc1_bias
        activated = gelu_tanh(hidden_pre).astype(jnp.bfloat16)
        per_head = projected.reshape(SEQ_LEN, 3, H, HD).transpose(1, 2, 0, 3)
        cosine, sine = rope_tables(seg_seq)
        queries = rotate(per_head[0].astype(jnp.float32), cosine[None], sine[None]).astype(jnp.bfloat16)
        keys_rot = rotate(per_head[1].astype(jnp.float32), cosine[None], sine[None]).astype(jnp.bfloat16)
        values_h = per_head[2]
        query_pos = lax.broadcasted_iota(jnp.int32, (SEQ_LEN, SEQ_LEN), 0)
        key_pos = lax.broadcasted_iota(jnp.int32, (SEQ_LEN, SEQ_LEN), 1)
        allowed = (key_pos <= query_pos) & (seg_seq[:, None] == seg_seq[None, :])

        def head_forward(head_in):
            query_h, key_h, value_h = head_in
            scores = head_scores(query_h, key_h, allowed)
            top_score = lax.optimization_barrier(jnp.max(scores, axis=1, keepdims=True))
            log_total = top_score[:, 0] + jnp.log(lax.optimization_barrier(jnp.sum(jnp.exp(scores - top_score), axis=1)))
            probs_b = jnp.exp(scores - log_total[:, None]).astype(jnp.bfloat16)
            output_h = jnp.einsum('qk,kd->qd', probs_b.astype(jnp.float32), value_h.astype(jnp.float32)).astype(jnp.bfloat16)
            return (output_h, log_total)
        attended_h, log_totals = lax.map(head_forward, (queries, keys_rot, values_h))
        attended = attended_h.transpose(1, 0, 2).reshape(SEQ_LEN, D)
        mixed = jnp.dot(attended, dense_weight, preferred_element_type=jnp.float32) + jnp.dot(activated, fc2_weight, preferred_element_type=jnp.float32)
        block_seq = (inputs_f + mixed + dense_bias + fc2_bias).astype(jnp.bfloat16)
        cot_f = cot_seq.astype(jnp.float32)
        grad_attended = jnp.dot(cot_seq, dense_weight.T, preferred_element_type=jnp.float32).astype(jnp.bfloat16)
        grad_activated = jnp.dot(cot_seq, fc2_weight.T, preferred_element_type=jnp.float32)
        grad_dense = jnp.dot(attended.T, cot_seq, preferred_element_type=jnp.float32)
        grad_fc2 = jnp.dot(activated.T, cot_seq, preferred_element_type=jnp.float32)
        out_bias_grad = lax.optimization_barrier(jnp.sum(cot_f, axis=0))
        gelu_value, gelu_pull = jax.vjp(gelu_tanh, hidden_pre)
        grad_hidden = gelu_pull(grad_activated)[0]
        grad_hidden_b = grad_hidden.astype(jnp.bfloat16)
        fc1_bias_grad = lax.optimization_barrier(jnp.sum(grad_hidden, axis=0))
        grad_fc1 = jnp.dot(normed.T, grad_hidden_b, preferred_element_type=jnp.float32)
        grad_out_h = grad_attended.reshape(SEQ_LEN, H, HD).transpose(1, 0, 2)

        def head_backward(head_in):
            query_h, key_h, value_h, lse_h, grad_h, output_h = head_in
            delta_h = lax.optimization_barrier(jnp.sum(grad_h.astype(jnp.float32) * output_h.astype(jnp.float32), axis=1))
            scores = head_scores(query_h, key_h, allowed)
            probs = jnp.exp(scores - lse_h[:, None])
            probs_b = probs.astype(jnp.bfloat16)
            grad_value = jnp.einsum('qk,qd->kd', probs_b.astype(jnp.float32), grad_h.astype(jnp.float32))
            grad_probs = jnp.einsum('qd,kd->qk', grad_h.astype(jnp.float32), value_h.astype(jnp.float32))
            grad_scores = (probs * (grad_probs - delta_h[:, None])).astype(jnp.bfloat16).astype(jnp.float32)
            grad_query = jnp.einsum('qk,kd->qd', grad_scores, key_h.astype(jnp.float32)) * scale
            grad_key = jnp.einsum('qk,qd->kd', grad_scores, query_h.astype(jnp.float32)) * scale
            return (grad_query, grad_key, grad_value)
        grad_queries, grad_keys, grad_values = lax.map(head_backward, (queries, keys_rot, values_h, log_totals, grad_out_h, attended_h))
        stacked = jnp.stack([unrotate(grad_queries, cosine[None], sine[None]), unrotate(grad_keys, cosine[None], sine[None]), grad_values], axis=0).astype(jnp.bfloat16)
        grad_projected = stacked.transpose(2, 0, 1, 3).reshape(SEQ_LEN, 3 * D)
        qkv_bias_grad = lax.optimization_barrier(jnp.sum(grad_projected.astype(jnp.float32), axis=0))
        grad_qkv = jnp.dot(normed.T, grad_projected, preferred_element_type=jnp.float32)
        grad_normed = jnp.dot(grad_projected, flat_qkv.T, preferred_element_type=jnp.float32) + jnp.dot(grad_hidden_b, fc1_weight.T, preferred_element_type=jnp.float32)
        scaled = grad_normed * ln_gain
        mean_grad = lax.optimization_barrier(jnp.mean(scaled, axis=1, keepdims=True))
        mean_proj = lax.optimization_barrier(jnp.mean(scaled * standard, axis=1, keepdims=True))
        grad_in_seq = cot_f + inv_std * (scaled - mean_grad - standard * mean_proj)
        gain_grad = lax.optimization_barrier(jnp.sum(grad_normed * standard, axis=0))
        ln_bias_grad = lax.optimization_barrier(jnp.sum(grad_normed, axis=0))
        terms = (grad_qkv, qkv_bias_grad, grad_dense, out_bias_grad, grad_fc1, fc1_bias_grad, grad_fc2, gain_grad, ln_bias_grad)
        new_carry = tuple((total + term for total, term in zip(carry, terms)))
        return (new_carry, (block_seq, grad_in_seq))
    zero_carry = (jnp.zeros((D, 3 * D), jnp.float32), jnp.zeros((3 * D,), jnp.float32), jnp.zeros((D, D), jnp.float32), jnp.zeros((D,), jnp.float32), jnp.zeros((D, FF), jnp.float32), jnp.zeros((FF,), jnp.float32), jnp.zeros((FF, D), jnp.float32), jnp.zeros((D,), jnp.float32), jnp.zeros((D,), jnp.float32))
    totals, stacked_out = lax.scan(one_sequence, zero_carry, (hidden_in, segments, cotangent))
    block_out, grad_input = stacked_out
    return (block_out, grad_input, totals[0].reshape(D, 3, D), totals[1].reshape(3, D), totals[2], totals[3], totals[4], totals[5], totals[6], totals[3], totals[7], totals[8])
```

```python
from functools import partial
import math

import jax
import jax.numpy as jnp
from jax import lax
from jax.experimental import pallas as pl
from jax.experimental.pallas import tpu as pltpu
from jax.sharding import PartitionSpec as P

HD = 64
ROT = 32
DOC_MAX = 512
BLOCK = 256

ln_eps = 1e-05
rope_base = 10000.0
mask_fill = -1e30
contract_rows = (((0,), (0,)), ((), ()))
contract_cols = (((1,), (1,)), ((), ()))
contract_in = (((1,), (0,)), ((), ()))


def fdot(a, b, dims):
    return lax.dot_general(a, b, dims, preferred_element_type=jnp.float32)


def doc_starts(segment_ids):
    index_all = lax.broadcasted_iota(jnp.int32, segment_ids.shape, 1)
    first_col = jnp.ones(segment_ids.shape[:-1] + (1,), dtype=jnp.bool_)
    change = jnp.concatenate([first_col, segment_ids[..., 1:] != segment_ids[..., :-1]], axis=1)
    return lax.cummax(jnp.where(change, index_all, 0), axis=1)


def rope_lanes(starts, heads):
    half = ROT // 2
    positions = lax.broadcasted_iota(jnp.int32, starts.shape, 1) - starts
    freqs = rope_base ** (-(jnp.arange(half, dtype=jnp.float32) * 2.0) / ROT)
    angles = positions.astype(jnp.float32)[..., None] * freqs
    cosine, sine = jnp.cos(angles), jnp.sin(angles)
    rest = jnp.zeros(angles.shape[:-1] + (HD - ROT,), jnp.float32)
    zero = jnp.zeros_like(sine)
    keep = jnp.concatenate([cosine, cosine, rest + 1.0], axis=-1)
    ahead = jnp.concatenate([-sine, zero, rest], axis=-1)
    behind = jnp.concatenate([zero, sine, rest], axis=-1)
    return [jnp.tile(t, (1, 1, heads)) for t in (keep, ahead, behind)]


def attention_kernel(
    heads, qkv, grad_out, starts, keep, ahead, behind, out, grad_qkv, qs, ks, vs, gs, dq, dk, dv
):
    length = qkv.shape[1]
    hw = heads * HD
    half = ROT // 2
    scale = 1.0 / math.sqrt(HD)

    def turn(values, sign):
        turned = pltpu.roll(values, hw - half, 1) * ahead[0] + pltpu.roll(values, half, 1) * behind[0]
        return values * keep[0] + (turned if sign > 0 else -turned)

    queries = turn(qkv[0, :, :hw].astype(jnp.float32), 1).astype(jnp.bfloat16)
    keys_all = turn(qkv[0, :, hw : 2 * hw].astype(jnp.float32), 1).astype(jnp.bfloat16)
    for head in range(heads):
        cols = slice(head * HD, (head + 1) * HD)
        qs[head] = queries[:, cols]
        ks[head] = keys_all[:, cols]
        vs[head] = qkv[0, :, 2 * hw + head * HD : 2 * hw + (head + 1) * HD]
        gs[head] = grad_out[0, :, cols]
    dk[...] = jnp.zeros_like(dk)
    dv[...] = jnp.zeros_like(dv)

    def one_head(head, carry):
        for row in range(0, length, BLOCK):
            low = max(0, row - DOC_MAX)
            span = row + BLOCK - low
            rows, cols = pl.ds(row, BLOCK), pl.ds(low, span)
            query, key, value, grad = qs[head, rows], ks[head, cols], vs[head, cols], gs[head, rows]
            query_pos = row + lax.broadcasted_iota(jnp.int32, (BLOCK, span), 0)
            key_pos = low + lax.broadcasted_iota(jnp.int32, (BLOCK, span), 1)
            allowed = (key_pos >= starts[0, rows]) & (key_pos <= query_pos)
            scores = jnp.where(allowed, fdot(query, key, contract_cols) * scale, mask_fill)
            weights = jnp.exp(scores - jnp.max(scores, axis=1, keepdims=True))
            probs = weights * (1.0 / jnp.sum(weights, axis=1, keepdims=True))
            probs_b = probs.astype(jnp.bfloat16)
            attended = fdot(probs_b, value, contract_in).astype(jnp.bfloat16)
            qs_out = attended.astype(jnp.float32)
            delta = jnp.sum(grad.astype(jnp.float32) * qs_out, axis=1, keepdims=True)
            grad_probs = fdot(grad, value, contract_cols)
            grad_scores = (probs * (grad_probs - delta)).astype(jnp.bfloat16)
            dv[head, cols] += fdot(probs_b, grad, contract_rows)
            dk[head, cols] += fdot(grad_scores, query, contract_rows)
            dq[head, rows] = fdot(grad_scores, key, contract_in)
            gs[head, rows] = attended
        return carry

    lax.fori_loop(0, heads, one_head, 0)
    out[0] = jnp.concatenate([gs[h] for h in range(heads)], axis=1)
    grad_q = jnp.concatenate([dq[h] for h in range(heads)], axis=1) * scale
    grad_k = jnp.concatenate([dk[h] for h in range(heads)], axis=1) * scale
    grad_v = jnp.concatenate([dv[h] for h in range(heads)], axis=1)
    grad_qkv[0, :, :hw] = turn(grad_q, -1).astype(jnp.bfloat16)
    grad_qkv[0, :, hw : 2 * hw] = turn(grad_k, -1).astype(jnp.bfloat16)
    grad_qkv[0, :, 2 * hw :] = grad_v.astype(jnp.bfloat16)


def attention(projected, grad_attended, starts):
    seqs, length, triple = projected.shape
    hw = triple // 3
    heads = hw // HD
    tables = rope_lanes(starts, heads)

    def whole(shape):
        return pl.BlockSpec((1,) + shape, lambda s: (s, 0, 0))

    return pl.pallas_call(
        partial(attention_kernel, heads),
        grid=(seqs,),
        in_specs=[whole((length, triple)), whole((length, hw)), whole((length, 1))]
        + [whole((length, hw))] * 3,
        out_specs=[whole((length, hw)), whole((length, triple))],
        out_shape=[
            jax.ShapeDtypeStruct((seqs, length, hw), jnp.bfloat16),
            jax.ShapeDtypeStruct((seqs, length, triple), jnp.bfloat16),
        ],
        scratch_shapes=[pltpu.VMEM((heads, length, HD), jnp.bfloat16)] * 4
        + [pltpu.VMEM((heads, length, HD), jnp.float32)] * 3,
        name="attention_both_ways",
    )(projected, grad_attended, starts[..., None], *tables)


def body(
    hidden_in,
    segments,
    ln_gain,
    ln_bias,
    qkv_weight,
    qkv_bias,
    dense_weight,
    dense_bias,
    fc1_weight,
    fc1_bias,
    fc2_weight,
    fc2_bias,
    cotangent,
):
    seqs, piece, lw = hidden_in.shape
    n_ctx = lax.axis_size("ctx")
    n_ten = lax.axis_size("tensor")
    n_dp = lax.axis_size("dp")
    length = piece * n_ctx
    width = ln_gain.shape[0]
    tokens = seqs * length
    hw = lw // n_ctx
    fw = fc1_weight.shape[1] // n_ctx
    ctx = lax.axis_index("ctx")
    bf16, f32 = jnp.bfloat16, jnp.float32

    def swap(array, split_axis, concat_axis):
        return lax.all_to_all(array, "ctx", split_axis=split_axis, concat_axis=concat_axis, tiled=True)

    def gather_rows(array):
        return lax.all_gather(array, "dp", axis=0, tiled=True)

    fc1 = gather_rows(swap(fc1_weight, 1, 0))
    qkv = gather_rows(swap(qkv_weight, 2, 0).reshape(-1, 3 * hw))
    dense = lax.all_gather(swap(dense_weight, 0, 1), "dp", axis=0)
    fc2 = lax.all_gather(swap(fc2_weight, 0, 1), "dp", axis=0)

    def gather_tokens(array):
        both = lax.all_gather(array, ("ctx", "tensor"), axis=0)
        both = both.reshape(n_ctx, n_ten, seqs, piece, lw).transpose(2, 0, 3, 1, 4)
        return both.reshape(tokens, width)

    def scatter_tokens(array):
        split = array.astype(bf16).reshape(seqs, n_ctx, piece, n_ten, lw).transpose(1, 3, 0, 2, 4)
        split = split.reshape(n_ctx * n_ten, seqs, piece, lw)
        return lax.psum_scatter(split, ("ctx", "tensor"), scatter_dimension=0, tiled=False).astype(f32)

    inputs_f = gather_tokens(hidden_in).astype(f32)
    cot = gather_tokens(cotangent)
    mean_val = jnp.mean(inputs_f, axis=1, keepdims=True)
    centered = inputs_f - mean_val
    inv_std = lax.rsqrt(jnp.mean(centered * centered, axis=1, keepdims=True) + ln_eps)
    normed = (centered * inv_std * ln_gain + ln_bias).astype(bf16)

    fc1_bias_own = lax.dynamic_slice_in_dim(fc1_bias, ctx * fw, fw, 0)
    hidden_pre = fdot(normed, fc1, contract_in) + fc1_bias_own
    gelu_tanh = partial(jax.nn.gelu, approximate=True)
    activated_f, gelu_pull = jax.vjp(gelu_tanh, hidden_pre)
    activated = activated_f.astype(bf16)

    def cols_grad(left):
        terms = jnp.einsum(
            "tk,tzn->zkn", left, cot.reshape(tokens, n_dp, width // n_dp), preferred_element_type=f32
        )
        own = lax.psum_scatter(terms.astype(bf16), "dp", scatter_dimension=0, tiled=False)
        return swap(own, 1, 0).astype(f32)

    grad_fc2 = cols_grad(activated)

    qkv_bias_own = lax.dynamic_slice_in_dim(qkv_bias, ctx * hw, hw, 1).reshape(-1)
    projected = (fdot(normed, qkv, contract_in) + qkv_bias_own).astype(bf16)
    cot_z = cot.reshape(tokens, n_dp, width // n_dp)
    grad_attended = jnp.einsum("tzn,zkn->tk", cot_z, dense, preferred_element_type=f32).astype(bf16)
    starts = doc_starts(segments)
    attended, grad_projected = attention(
        projected.reshape(seqs, length, 3 * hw), grad_attended.reshape(seqs, length, hw), starts
    )
    attended = attended.reshape(tokens, hw)
    grad_projected = grad_projected.reshape(tokens, 3 * hw)
    grad_dense = cols_grad(attended)

    def rows_grad(right, shape, split_axis):
        terms = fdot(normed, right, contract_rows).astype(bf16)
        own = lax.psum_scatter(terms, "dp", scatter_dimension=0, tiled=True)
        return swap(own.reshape((-1,) + shape), 0, split_axis).astype(f32)

    grad_qkv = rows_grad(grad_projected, (3, hw), 2)
    grad_activated = jnp.einsum("tzn,zkn->tk", cot_z, fc2, preferred_element_type=f32)
    grad_hidden = gelu_pull(grad_activated)[0]
    grad_hidden_b = grad_hidden.astype(bf16)
    grad_fc1 = rows_grad(grad_hidden_b, (fw,), 1)

    mixed = jnp.einsum("tk,zkn->tzn", attended, dense, preferred_element_type=f32) + jnp.einsum(
        "tk,zkn->tzn", activated, fc2, preferred_element_type=f32
    )
    summed = scatter_tokens(mixed)
    hidden_f = hidden_in.astype(f32)
    block_out = (hidden_f + summed + dense_bias + fc2_bias).astype(bf16)

    grad_normed = scatter_tokens(
        fdot(grad_projected, qkv, contract_cols) + fdot(grad_hidden_b, fc1, contract_cols)
    )
    first = lax.axis_index("tensor") * lw

    def own_rows(array):
        return lax.dynamic_slice_in_dim(array.reshape(seqs, length, 1), ctx * piece, piece, 1)

    inv_own = own_rows(inv_std)
    standard = (hidden_f - own_rows(mean_val)) * inv_own
    scaled = grad_normed * lax.dynamic_slice_in_dim(ln_gain, first, lw, 0)
    stats = jnp.stack([jnp.sum(scaled, axis=2), jnp.sum(scaled * standard, axis=2)])
    stats = lax.psum(stats, "tensor") / width
    grad_input = cotangent.astype(f32) + inv_own * (
        scaled - stats[0][..., None] - standard * stats[1][..., None]
    )
    qkv_bias_grad = jnp.sum(grad_projected.astype(f32), axis=0).reshape(3, hw)
    qkv_bias_grad = lax.dynamic_update_slice(jnp.zeros((3, lw), f32), qkv_bias_grad, (0, ctx * hw))
    fc1_bias_grad = jnp.sum(grad_hidden, axis=0)
    fc1_bias_grad = lax.dynamic_update_slice(
        jnp.zeros((fw * n_ctx,), f32), fc1_bias_grad, (ctx * fw,)
    )
    small = lax.psum(
        (
            qkv_bias_grad,
            fc1_bias_grad,
            jnp.sum(cotangent.astype(f32), axis=(0, 1)),
            jnp.sum(grad_normed * standard, axis=(0, 1)),
            jnp.sum(grad_normed, axis=(0, 1)),
        ),
        ("dp", "ctx"),
    )
    return (
        block_out,
        grad_input,
        grad_qkv,
        small[0],
        grad_dense,
        small[2],
        grad_fc1,
        small[1],
        grad_fc2,
        small[2],
        small[3],
        small[4],
    )


def solution(mesh):
    in_specs = (
        P("dp", "ctx", "tensor"),
        P("dp", None),
        P(),
        P(),
        P(("dp", "ctx"), None, "tensor"),
        P(None, "tensor"),
        P("tensor", ("dp", "ctx")),
        P("tensor"),
        P(("dp", "ctx"), "tensor"),
        P("tensor"),
        P("tensor", ("dp", "ctx")),
        P("tensor"),
        P("dp", "ctx", "tensor"),
    )
    out_specs = (
        P("dp", "ctx", "tensor"),
        P("dp", "ctx", "tensor"),
        P(("dp", "ctx"), None, "tensor"),
        P(None, "tensor"),
        P("tensor", ("dp", "ctx")),
        P("tensor"),
        P(("dp", "ctx"), "tensor"),
        P("tensor"),
        P("tensor", ("dp", "ctx")),
        P("tensor"),
        P("tensor"),
        P("tensor"),
    )
    return jax.shard_map(body, mesh=mesh, in_specs=in_specs, out_specs=out_specs, check_vma=False)
```

```python
from functools import partial
import math

import jax
import jax.numpy as jnp
from jax import lax
from jax.experimental import pallas as pl
from jax.experimental.pallas import tpu as pltpu
from jax.sharding import PartitionSpec as P

HD = 64
ROT = 32
DOC_MAX = 512
BLOCK = 256
ROWS = 512

ln_eps = 1e-05
rope_base = 10000.0
mask_fill = -1e30
contract_rows = (((0,), (0,)), ((), ()))
contract_cols = (((1,), (1,)), ((), ()))
contract_in = (((1,), (0,)), ((), ()))
f32, bf16 = jnp.float32, jnp.bfloat16
FC1, QKV, DENSE, FC2 = range(4)
MESH = pl.DeviceIdType.MESH


def fdot(a, b, dims=contract_in):
    return lax.dot_general(a, b, dims, preferred_element_type=f32)


def doc_starts(segment_ids):
    index_all = lax.broadcasted_iota(jnp.int32, segment_ids.shape, 1)
    first_col = jnp.ones(segment_ids.shape[:-1] + (1,), dtype=jnp.bool_)
    change = jnp.concatenate([first_col, segment_ids[..., 1:] != segment_ids[..., :-1]], axis=1)
    return lax.cummax(jnp.where(change, index_all, 0), axis=1)


def rope_lanes(starts, heads):
    half = ROT // 2
    positions = lax.broadcasted_iota(jnp.int32, starts.shape, 0) - starts
    freqs = rope_base ** (-(jnp.arange(half, dtype=f32) * 2.0) / ROT)
    angles = positions.astype(f32)[:, None] * freqs
    cosine, sine = jnp.cos(angles), jnp.sin(angles)
    rest = jnp.zeros((angles.shape[0], HD - ROT), f32)
    zero = jnp.zeros_like(sine)
    keep = jnp.concatenate([cosine, cosine, rest + 1.0], axis=-1)
    ahead = jnp.concatenate([-sine, zero, rest], axis=-1)
    behind = jnp.concatenate([zero, sine, rest], axis=-1)
    return [jnp.tile(table, (1, heads)) for table in (keep, ahead, behind)]


def tiles(total, size, step):
    if total == size:
        step(0)
    else:
        pl.loop(0, total // size)(lambda i: step(pl.multiple_of(i * size, size)))


def bits_of(count):
    return [1 << i for i in range(count.bit_length() - 1)]


def block_kernel(dims, *refs):
    Z, C, T, r, fw, hw, lw, piece = dims
    (
        hid, cot_in, fc1w, qkvw, densew, fc2w, gain, bias, fc1b, qkvb, gain_own, out_bias,
        starts, keep, ahead, behind,
        block_out, grad_input, g_fc1, g_qkv, g_dense, g_fc2,
        o_fc1b, o_qkvb, o_outb, o_gain, o_bias,
        X, COT, W1, WQ, WD, W2, ACT, DG, TT, QV, GA, ATT, MI,
        G2, R2, GQ, RQ, GD, RD, RT, RC, SM, SMR, ST, STR,
        y_s, y_r, own_s, ag_s, ag_r, rs_s, rs_r, fin_s, fin_r, out_s,
        aa_s, aa_r, ar_s, ar_r, sm_s, sm_r, st_s, st_r, free, ar_free,
    ) = refs
    L, D, U = piece * C, T * lw, Z * C
    z, c, t = lax.axis_index("dp"), lax.axis_index("ctx"), lax.axis_index("tensor")
    last = Z - 1

    def remote(src, dst, send, recv, **where):
        return pltpu.make_async_remote_copy(
            src_ref=src, dst_ref=dst, send_sem=send, recv_sem=recv,
            device_id=where, device_id_type=MESH,
        )

    barrier = pltpu.get_barrier_semaphore()
    for dz in range(Z):
        for dc in range(C):
            if dz or dc:
                pl.semaphore_signal(
                    barrier, 1, device_id={"dp": (z + dz) % Z, "ctx": (c + dc) % C},
                    device_id_type=MESH,
                )
    for dt in range(1, T):
        pl.semaphore_signal(barrier, 1, device_id={"tensor": (t + dt) % T}, device_id_type=MESH)
    pl.semaphore_wait(barrier, U - 1 + T - 1)

    weight = [
        lambda u: W1.at[pl.ds(pl.multiple_of(u * r, r), r)],
        lambda u: WQ.at[pl.ds(pl.multiple_of(u * r, r), r)],
        lambda u: WD.at[u],
        lambda u: W2.at[u],
    ]
    shard = [
        lambda k: fc1w.at[:, pl.ds(pl.multiple_of(k * fw, fw), fw)],
        lambda k: qkvw.at[k],
        lambda k: densew.at[k],
        lambda k: fc2w.at[k],
    ]

    def ag_y(p):
        for o in range(1, C):
            k = (c + o) % C
            remote(shard[p](k), weight[p](z * C + c), y_s.at[p, o], y_r.at[p, o], ctx=k).start()
        pltpu.make_async_copy(shard[p](c), weight[p](z * C + c), own_s.at[p]).start()

    def ag_copy(p, u, src, way):
        step = 1 if way == 0 else -1
        return remote(src, weight[p](u), ag_s.at[p, way, u], ag_r.at[p, u], dp=z + step)

    def ag_both(p, u, src):
        pl.when(z < last)(lambda: ag_copy(p, u, src, 0).start())
        pl.when(z > 0)(lambda: ag_copy(p, u, src, 1).start())

    def ag_first(p):
        ag_both(p, z * C + c, shard[p](c))

    def ag_second(p):
        for o in range(1, C):
            u = z * C + (c - o) % C
            k = (c + o) % C
            remote(shard[p](k), weight[p](u), y_s.at[p, o], y_r.at[p, o], ctx=k).wait_recv()
            ag_both(p, u, weight[p](u))

    def ag_step(p, s):
        for cs in range(C):
            right, left = (z - s) * C + cs, (z + s) * C + cs

            @pl.when(z >= s)
            def _():
                ag_copy(p, right, weight[p](right), 0).wait_recv()
                pl.when(z < last)(lambda: ag_copy(p, right, weight[p](right), 0).start())

            @pl.when(z + s <= last)
            def _():
                ag_copy(p, left, weight[p](left), 1).wait_recv()
                pl.when(z > 0)(lambda: ag_copy(p, left, weight[p](left), 1).start())

    def ag_own(p):
        pltpu.make_async_copy(shard[p](c), weight[p](z * C + c), own_s.at[p]).wait()

    def ag_end(p):
        for o in range(1, C):
            k = (c + o) % C
            remote(shard[p](k), weight[p](z * C + c), y_s.at[p, o], y_r.at[p, o], ctx=k).wait_send()
        for zs in range(Z):
            for cs in range(C):
                u = zs * C + cs

                @pl.when((z < last) & (z >= zs))
                def _():
                    ag_copy(p, u, weight[p](u), 0).wait_send()

                @pl.when((z > 0) & (z <= zs))
                def _():
                    ag_copy(p, u, weight[p](u), 1).wait_send()

    def doubling(a, array, own, order):
        masks, width_c, index = [0], 1, 0
        plan = []
        for axis, bit in order:
            plan.append((axis, bit, width_c, tuple(masks), index))
            index += len(masks)
            if axis == "c":
                width_c *= 2
            else:
                masks = masks + [m ^ bit for m in masks]

        def copies(stage):
            axis, bit, count, sent, first = plan[stage]
            group = (c // count) * count
            where = {"ctx": c ^ bit} if axis == "c" else {"tensor": t ^ bit}
            found = []
            for j, m in enumerate(sent):
                span = pl.ds(pl.multiple_of(group * piece, piece), count * piece)
                cols = pl.ds(pl.multiple_of((t ^ m) * lw, lw), lw)
                dst = array.at[span, cols]
                src = own if stage == 0 else dst
                found.append(remote(src, dst, aa_s.at[a, first + j], aa_r.at[a, first + j], **where))
            return found

        def begin(stage):
            for copy in copies(stage):
                copy.start()

        def arrive(stage):
            for copy in copies(stage):
                copy.wait_recv()

        def end():
            for stage in range(len(plan)):
                for copy in copies(stage):
                    copy.wait_send()

        def place(sem):
            cols = pl.ds(pl.multiple_of(t * lw, lw), lw)
            return pltpu.make_async_copy(
                own, array.at[pl.ds(pl.multiple_of(c * piece, piece), piece), cols], sem
            )

        return begin, arrive, end, place

    cbits = [("c", b) for b in bits_of(C)]
    tbits = [("t", b) for b in reversed(bits_of(T))]
    h_begin, h_arrive, h_end, h_place = doubling(0, X, hid, cbits + tbits)
    c_begin, c_arrive, c_end, c_place = doubling(1, COT, cot_in, tbits[:-1] + cbits + tbits[-1:])
    stages = len(cbits) + len(tbits)

    grads = {FC2: (G2, R2, fw, g_fc2), FC1: (G2, R2, fw, g_fc1)}
    grads[QKV] = (GQ, RQ, 3 * hw, g_qkv)
    grads[DENSE] = (GD, RD, hw, g_dense)

    def rs_copy(p, u, way):
        G, R, _, _ = grads[p]
        step, slot = (1, u + C) if way == 0 else (-1, u)
        return remote(G.at[u], R.at[slot], rs_s.at[p, way, u], rs_r.at[p, way, u], dp=z + step)

    def rs_add(p, u, slot):
        G, R, k, _ = grads[p]
        size = min(BLOCK, k)

        def add(row):
            rows = pl.ds(row, size)
            G[u, rows] = (G[u, rows].astype(f32) + R[slot, rows].astype(f32)).astype(bf16)

        tiles(k, size, add)

    def rs_step(p, s):
        for cs in range(C):
            right = (last + z - s) * C + cs
            left = (s - last + z) * C + cs

            @pl.when(z <= s)
            def _():
                @pl.when(z > 0)
                def _():
                    rs_copy(p, right, 0).wait_recv()
                    rs_add(p, right, right + C)

                rs_copy(p, right, 0).start()

            @pl.when(last - z <= s)
            def _():
                @pl.when(z < last)
                def _():
                    rs_copy(p, left, 1).wait_recv()
                    rs_add(p, left, left)

                rs_copy(p, left, 1).start()

    def fin_copy(p, o):
        G, _, _, out = grads[p]
        k = (c + o) % C
        return remote(G.at[z * C + k], out.at[c], fin_s.at[p, o], fin_r.at[p, o], ctx=k)

    def fin_own(p):
        G, _, _, out = grads[p]
        return pltpu.make_async_copy(G.at[z * C + c], out.at[c], out_s.at[p])

    def rs_final(p):
        for o in range(C - 1, -1, -1):
            k = (c + o) % C
            u = z * C + k

            @pl.when(z > 0)
            def _():
                rs_copy(p, u, 0).wait_recv()
                rs_add(p, u, u + C)

            @pl.when(z < last)
            def _():
                rs_copy(p, u, 1).wait_recv()
                rs_add(p, u, u)

            if o:
                fin_copy(p, o).start()
            else:
                fin_own(p).start()

    def rs_end(p):
        for zs in range(Z):
            for cs in range(C):
                u = zs * C + cs
                pl.when(zs > z)(lambda: rs_copy(p, u, 0).wait_send())
                pl.when(zs < z)(lambda: rs_copy(p, u, 1).wait_send())
        for o in range(1, C):
            fin_copy(p, o).wait()
        fin_own(p).wait()

    def layer_norm():
        def rows_of(row):
            rows = pl.ds(row, 128)
            x = X[rows].astype(f32)
            mean = jnp.mean(x, axis=1, keepdims=True)
            centered = x - mean
            inv = lax.rsqrt(jnp.mean(centered * centered, axis=1, keepdims=True) + ln_eps)
            MI[rows, 0:1] = mean
            MI[rows, 1:2] = inv
            X[rows] = (centered * inv * gain[...] + bias[...]).astype(bf16)

        tiles(L, 128, rows_of)

    cf = min(BLOCK, fw)
    gelu_c = math.sqrt(2.0 / math.pi)

    def fc1_cols(col):
        cols = pl.ds(col, cf)

        def rows_of(row):
            rows = pl.ds(row, ROWS)
            v = fdot(X[rows], W1[:, cols]) + fc1b[:, cols]
            tanh = jnp.tanh(gelu_c * (v + 0.044715 * (v * v * v)))
            act = 0.5 * v * (1.0 + tanh)
            slope = gelu_c * (1.0 + 3.0 * 0.044715 * (v * v))
            DG[rows, cols] = (0.5 * (1.0 + tanh) + 0.5 * v * (1.0 - tanh * tanh) * slope).astype(bf16)
            ACT[rows, cols] = act.astype(bf16)
            TT[cols, rows] = act.T.astype(bf16)

        tiles(L, ROWS, rows_of)

    def unit_grads(p, base, source, units):
        G, _, k, _ = grads[p]
        size = next(s for s in (ROWS, 384, 256, 192, 64) if k % s == 0)
        for u in units:
            cols = slice(u * r, (u + 1) * r)

            def rows_of(row):
                G[u, pl.ds(row, size)] = fdot(TT[pl.ds(base + row, size)], source[:, cols]).astype(bf16)

            tiles(k, size, rows_of)

    def units_at(*ds):
        return [d * C + cs for d in ds for cs in range(C)]

    outer = units_at(last, 0)
    inner = units_at(*[d for d in range(last - 1, 0, -1)])

    def project():
        bn = BLOCK if (3 * hw) % BLOCK == 0 else 3 * hw
        for n in range(3 * hw // bn):
            cols = slice(n * bn, (n + 1) * bn)

            def rows_of(row):
                rows = pl.ds(row, ROWS)
                QV[rows, cols] = (fdot(X[rows], WQ[:, cols]) + qkvb[:, cols]).astype(bf16)

            tiles(L, ROWS, rows_of)

    def over_units(rows, weights):
        total = None
        for u in range(U):
            term = fdot(COT[rows, u * r : (u + 1) * r], weights(u), contract_cols)
            total = term if total is None else total + term
        return total

    def attended_grads():
        def rows_of(row):
            rows = pl.ds(row, ROWS)
            GA[rows] = over_units(rows, lambda u: WD[u]).astype(bf16)

        tiles(L, ROWS, rows_of)

    gw = min(hw, 128)
    in_group = gw // HD
    half = ROT // 2
    scale = 1.0 / math.sqrt(HD)

    def turn(values, rows, sign):
        turned = (
            pltpu.roll(values, gw - half, 1) * ahead[rows] + pltpu.roll(values, half, 1) * behind[rows]
        )
        return values * keep[rows] + (turned if sign > 0 else -turned)

    def attention(group, qs, ks, vs, gs, dq, dk, dv):
        lanes = [pl.ds(part * hw + group * gw, gw) for part in range(3)]
        own = pl.ds(group * gw, gw)

        def load(row):
            rows = pl.ds(row, BLOCK)
            query = turn(QV[rows, lanes[0]].astype(f32), rows, 1).astype(bf16)
            key = turn(QV[rows, lanes[1]].astype(f32), rows, 1).astype(bf16)
            value, grad = QV[rows, lanes[2]], GA[rows, own]
            for head in range(in_group):
                cols = slice(head * HD, (head + 1) * HD)
                qs[head, rows] = query[:, cols]
                ks[head, rows] = key[:, cols]
                vs[head, rows] = value[:, cols]
                gs[head, rows] = grad[:, cols]

        tiles(L, BLOCK, load)
        dk[...] = jnp.zeros_like(dk)
        dv[...] = jnp.zeros_like(dv)

        def one_head(head):
            for row in range(0, L, BLOCK):
                low = max(0, row - DOC_MAX)
                span = row + BLOCK - low
                rows, cols = pl.ds(row, BLOCK), pl.ds(low, span)
                query, key, value, grad = qs[head, rows], ks[head, cols], vs[head, cols], gs[head, rows]
                query_pos = row + lax.broadcasted_iota(jnp.int32, (BLOCK, span), 0)
                key_pos = low + lax.broadcasted_iota(jnp.int32, (BLOCK, span), 1)
                allowed = (key_pos >= starts[rows]) & (key_pos <= query_pos)
                scores = jnp.where(allowed, fdot(query, key, contract_cols) * scale, mask_fill)
                weights = jnp.exp(scores - jnp.max(scores, axis=1, keepdims=True))
                probs = weights * (1.0 / jnp.sum(weights, axis=1, keepdims=True))
                probs_b = probs.astype(bf16)
                attended = fdot(probs_b, value).astype(bf16)
                delta = jnp.sum(grad.astype(f32) * attended.astype(f32), axis=1, keepdims=True)
                grad_probs = fdot(grad, value, contract_cols)
                grad_scores = (probs * (grad_probs - delta)).astype(bf16)
                dv[head, cols] += fdot(probs_b, grad, contract_rows)
                dk[head, cols] += fdot(grad_scores, query, contract_rows)
                dq[head, rows] = fdot(grad_scores, key)
                gs[head, rows] = attended

        pl.loop(0, in_group)(one_head)

        def save(row):
            rows = pl.ds(row, BLOCK)

            def join(parts):
                return jnp.concatenate([parts[h, rows] for h in range(in_group)], axis=1)

            attended = join(gs)
            grad_q = turn(join(dq) * scale, rows, -1)
            grad_k = turn(join(dk) * scale, rows, -1)
            grad_v = join(dv)
            ATT[rows, own] = attended
            TT[pl.ds(3 * hw + group * gw, gw), rows] = attended.astype(f32).T.astype(bf16)
            for part, grad in enumerate((grad_q, grad_k, grad_v)):
                QV[rows, lanes[part]] = grad.astype(bf16)
                TT[lanes[part], rows] = grad.T.astype(bf16)
                rounded = grad.astype(bf16).astype(f32)
                SM[1:2, lanes[part]] += jnp.sum(rounded, axis=0, keepdims=True)

        tiles(L, BLOCK, save)

    def hidden_grads():
        for n in range(fw // cf):
            cols = slice(n * cf, (n + 1) * cf)

            def rows_of(row):
                rows = pl.ds(row, ROWS)
                grad = over_units(rows, lambda u: W2[u, cols]) * DG[rows, cols].astype(f32)
                SM[0:1, cols] += jnp.sum(grad, axis=0, keepdims=True)
                DG[rows, cols] = grad.astype(bf16)
                TT[cols, rows] = grad.T.astype(bf16)

            tiles(L, ROWS, rows_of)

    def halving(a, P_):
        plan, masks, slot = [], list(range(T)), 0
        for bit in bits_of(T):
            kept = [m for m in masks if not m & bit]
            plan.append((bit, kept, slot))
            slot += len(kept)
            masks = kept
        cplan, offset = [], 0
        for bit in reversed(bits_of(C)):
            cplan.append((bit, offset))
            offset += bit * piece

        def cols_of(m):
            return pl.ds(pl.multiple_of((t ^ m) * lw, lw), lw)

        def peer(stage):
            if stage < len(plan):
                return {"tensor": t ^ plan[stage][0]}
            return {"ctx": c ^ cplan[stage - len(plan)][0]}

        def copies(stage):
            if stage < len(plan):
                bit, kept, first = plan[stage]
                return [
                    remote(
                        P_.at[:, cols_of(m ^ bit)], RT.at[first + j],
                        ar_s.at[a, first + j], ar_r.at[a, first + j], **peer(stage),
                    )
                    for j, m in enumerate(kept)
                ]
            bit, first = cplan[stage - len(plan)]
            start = ((c ^ bit) // bit) * bit * piece
            sem = slot + stage - len(plan)
            return [
                remote(
                    P_.at[pl.ds(pl.multiple_of(start, piece), bit * piece), cols_of(0)],
                    RC.at[pl.ds(first, bit * piece)],
                    ar_s.at[a, sem], ar_r.at[a, sem], **peer(stage),
                )
            ]

        count = len(plan) + len(cplan)

        def begin(stage):
            if a:
                pl.semaphore_wait(ar_free.at[stage], 1)
            for copy in copies(stage):
                copy.start()

        def arrive(stage):
            for copy in copies(stage):
                copy.wait_recv()
            if stage < len(plan):
                _, kept, first = plan[stage]
                for j, m in enumerate(kept):

                    def add(row):
                        rows = pl.ds(row, 128)
                        total = P_[rows, cols_of(m)].astype(f32) + RT[first + j, rows].astype(f32)
                        P_[rows, cols_of(m)] = total.astype(bf16)

                    tiles(L, 128, add)
            elif stage < count - 1:
                bit, first = cplan[stage - len(plan)]
                start = (c // bit) * bit * piece

                def add(row):
                    rows = pl.ds(start + row, 128)
                    total = P_[rows, cols_of(0)].astype(f32) + RC[pl.ds(first + row, 128)].astype(f32)
                    P_[rows, cols_of(0)] = total.astype(bf16)

                tiles(bit * piece, 128, add)

        def total(row):
            rows = pl.ds(pl.multiple_of(c * piece + row, 128), 128)
            return P_[rows, cols_of(0)].astype(f32) + RC[pl.ds(cplan[-1][1] + row, 128)].astype(f32)

        def release():
            for stage in range(count):
                pl.semaphore_signal(
                    ar_free.at[stage], 1, device_id=peer(stage), device_id_type=MESH
                )

        def end():
            for stage in range(count):
                for copy in copies(stage):
                    copy.wait_send()

        return begin, arrive, total, release, end, count

    def out_units(P_):
        for u in range(U):
            cols = slice(u * r, (u + 1) * r)

            def rows_of(row):
                rows = pl.ds(row, ROWS)
                P_[rows, cols] = (fdot(ATT[rows], WD[u]) + fdot(ACT[rows], W2[u])).astype(bf16)

            tiles(L, ROWS, rows_of)

    def norm_units(P_):
        for u in range(U):
            cols = slice(u * r, (u + 1) * r)

            def rows_of(row):
                rows = pl.ds(row, ROWS)
                P_[rows, cols] = (
                    fdot(DG[rows], W1[cols], contract_cols) + fdot(QV[rows], WQ[cols], contract_cols)
                ).astype(bf16)

            tiles(L, ROWS, rows_of)

    def write_block(total):
        def rows_of(row):
            rows = pl.ds(row, 128)
            block_out[rows] = (hid[rows].astype(f32) + total(row) + out_bias[...]).astype(bf16)

        tiles(piece, 128, rows_of)

    def standard_of(row):
        rows = pl.ds(pl.multiple_of(c * piece + row, 128), 128)
        inv = MI[rows, 1:2]
        return (hid[pl.ds(row, 128)].astype(f32) - MI[rows, 0:1]) * inv, inv

    def norm_sums(total):
        for row in range(0, piece, 128):
            grad = total(row)
            standard, _ = standard_of(row)
            scaled = grad * gain_own[...]
            first = jnp.sum(scaled, axis=1, keepdims=True)
            second = jnp.sum(scaled * standard, axis=1, keepdims=True)
            lane = lax.broadcasted_iota(jnp.int32, (128, 128), 1)
            pair = jnp.where(lane == 0, first, jnp.where(lane == 1, second, 0.0))
            ST[:, row : row + 128] = pair.T[0:8]
            SM[3:4, :lw] += jnp.sum(grad * standard, axis=0, keepdims=True)
            SM[4:5, :lw] += jnp.sum(grad, axis=0, keepdims=True)

    def st_copy(o):
        return remote(ST, STR.at[o - 1], st_s.at[o - 1], st_r.at[o - 1], tensor=(t + o) % T)

    def write_input(total):
        for row in range(0, piece, 128):
            stats = ST[:, row : row + 128]
            for o in range(1, T):
                stats = stats + STR[o - 1, :, row : row + 128]
            stats = jnp.concatenate([stats, jnp.zeros((120, 128), f32)], axis=0).T * (1.0 / D)
            standard, inv = standard_of(row)
            scaled = total(row) * gain_own[...]
            rows = pl.ds(row, 128)
            grad_input[rows] = cot_in[rows].astype(f32) + inv * (
                scaled - stats[:, 0:1] - standard * stats[:, 1:2]
            )

    def sm_copy(dz, dc):
        o = dz * C + dc - 1
        return remote(
            SM, SMR.at[z * C + c], sm_s.at[o], sm_r.at[o], dp=(z + dz) % Z, ctx=(c + dc) % C
        )

    offsets = [(dz, dc) for dz in range(Z) for dc in range(C) if dz or dc]

    h_place(own_s.at[4]).start()
    c_place(own_s.at[5]).start()
    ag_y(FC1)
    c_begin(0)
    h_begin(0)
    ag_first(FC1)
    ag_y(QKV)
    ag_y(DENSE)
    SM[...] = jnp.zeros_like(SM)
    SM[2:3, :lw] = jnp.sum(cot_in[...].astype(f32), axis=0, keepdims=True)
    ag_second(FC1)
    c_arrive(0)
    c_place(own_s.at[5]).wait()
    c_begin(1)
    ag_y(FC2)
    h_arrive(0)
    h_place(own_s.at[4]).wait()
    h_begin(1)
    ag_step(FC1, 1)
    for stage in range(2, stages):
        h_arrive(stage - 1)
        h_begin(stage)
        if stage < Z - 1:
            ag_step(FC1, stage)
    for s in range(max(stages, 2), Z - 1):
        ag_step(FC1, s)
    ag_first(QKV)
    ag_second(QKV)
    for stage in range(2, stages):
        c_arrive(stage - 1)
        c_begin(stage)
    h_arrive(stages - 1)
    h_end()
    layer_norm()
    ag_step(FC1, last)
    ag_own(FC1)
    ag_first(DENSE)
    ag_second(DENSE)
    tiles(fw, cf, fc1_cols)
    c_arrive(stages - 1)
    unit_grads(FC2, 0, COT, outer)
    rs_step(FC2, 0)
    ag_step(QKV, 1)
    unit_grads(FC2, 0, COT, inner)
    ag_first(FC2)
    ag_second(FC2)
    for s in range(2, Z):
        ag_step(QKV, s)
        ag_step(DENSE, s - 1)
        rs_step(FC2, s - 1)
    ag_own(QKV)
    project()
    ag_step(DENSE, last)
    ag_own(DENSE)
    attended_grads()
    rs_final(FC2)
    ag_step(FC2, 1)

    def attend(*scratch):
        for group in range(hw // gw):
            attention(group, *scratch)
            if group + 2 < Z:
                ag_step(FC2, group + 2)
        for s in range(hw // gw + 2, Z):
            ag_step(FC2, s)

    heads_b = pltpu.VMEM((in_group, L, HD), bf16)
    heads_f = pltpu.VMEM((in_group, L, HD), f32)
    pl.run_scoped(attend, *[heads_b] * 4, *[heads_f] * 3)
    unit_grads(DENSE, 3 * hw, COT, outer)
    rs_step(DENSE, 0)
    unit_grads(QKV, 0, X, outer)
    rs_step(QKV, 0)
    unit_grads(DENSE, 3 * hw, COT, inner)
    unit_grads(QKV, 0, X, inner)
    rs_step(DENSE, 1)
    rs_step(QKV, 1)
    ag_own(FC2)
    hidden_grads()
    rs_end(FC2)
    pl.when(z < last)(
        lambda: pl.semaphore_signal(free.at[1], 1, device_id={"dp": z + 1}, device_id_type=MESH)
    )
    pl.when(z > 0)(
        lambda: pl.semaphore_signal(free.at[0], 1, device_id={"dp": z - 1}, device_id_type=MESH)
    )
    unit_grads(FC1, 0, X, outer)
    for s in range(2, Z - 1):
        rs_step(DENSE, s)
        rs_step(QKV, s)
    pl.when(z < last)(lambda: pl.semaphore_wait(free.at[0], 1))
    pl.when(z > 0)(lambda: pl.semaphore_wait(free.at[1], 1))
    rs_step(FC1, 0)
    unit_grads(FC1, 0, X, inner)
    rs_final(DENSE)
    rs_final(QKV)

    def sums(P_):
        begin, arrive, total, release, end, count = halving(0, P_)
        begin2, arrive2, total2, _, end2, _ = halving(1, P_)
        out_units(P_)
        rs_step(FC1, 1)
        begin(0)
        for stage in range(1, count):
            arrive(stage - 1)
            begin(stage)
        arrive(count - 1)
        write_block(total)
        end()
        release()
        norm_units(P_)
        begin2(0)
        for s in range(2, Z - 1):
            rs_step(FC1, s)
        for stage in range(1, count):
            arrive2(stage - 1)
            begin2(stage)
        arrive2(count - 1)
        norm_sums(total2)
        for o in range(1, T):
            st_copy(o).start()
        for dz, dc in offsets:
            sm_copy(dz, dc).start()
        for o in range(1, T):
            st_copy(o).wait()
        write_input(total2)
        end2()

    pl.run_scoped(sums, pltpu.VMEM((L, D), bf16))
    SMR[z * C + c] = SM[...]
    for dz, dc in offsets:
        sm_copy(dz, dc).wait()
    for k in range(C):
        fc1_sum, qkv_sum = SMR[k, 0:1, :fw], SMR[k, 1:2, : 3 * hw]
        for zs in range(1, Z):
            fc1_sum = fc1_sum + SMR[zs * C + k, 0:1, :fw]
            qkv_sum = qkv_sum + SMR[zs * C + k, 1:2, : 3 * hw]
        o_fc1b[k : k + 1] = fc1_sum
        o_qkvb[k : k + 1] = qkv_sum
    for row, out in ((2, o_outb), (3, o_gain), (4, o_bias)):
        all_sum = SMR[0, row : row + 1, :lw]
        for u in range(1, U):
            all_sum = all_sum + SMR[u, row : row + 1, :lw]
        out[...] = all_sum
    rs_final(FC1)
    for p in (FC1, QKV, DENSE, FC2):
        ag_end(p)
    c_end()
    for p in (DENSE, QKV, FC1):
        rs_end(p)


def body(
    hidden_in,
    segments,
    ln_gain,
    ln_bias,
    qkv_weight,
    qkv_bias,
    dense_weight,
    dense_bias,
    fc1_weight,
    fc1_bias,
    fc2_weight,
    fc2_bias,
    cotangent,
):
    _, piece, lw = hidden_in.shape
    C, T, Z = lax.axis_size("ctx"), lax.axis_size("tensor"), lax.axis_size("dp")
    L, D, U = piece * C, lw * T, Z * C
    r = qkv_weight.shape[0]
    hw, fw = lw // C, fc1_weight.shape[1] // C
    ctx = lax.axis_index("ctx")
    first = lax.axis_index("tensor") * lw
    gw = min(hw, 128)
    starts = doc_starts(segments)[0]
    tables = rope_lanes(starts, gw // HD)
    qkvw = qkv_weight.reshape(r, 3, C, hw).transpose(2, 0, 1, 3).reshape(C, r, 3 * hw)
    operands = [
        hidden_in[0],
        cotangent[0],
        fc1_weight,
        qkvw,
        dense_weight.reshape(C, hw, r),
        fc2_weight.reshape(C, fw, r),
        ln_gain[None],
        ln_bias[None],
        lax.dynamic_slice_in_dim(fc1_bias, ctx * fw, fw, 0)[None],
        lax.dynamic_slice_in_dim(qkv_bias, ctx * hw, hw, 1).reshape(1, 3 * hw),
        lax.dynamic_slice_in_dim(ln_gain, first, lw, 0)[None],
        (dense_bias + fc2_bias)[None],
        starts[:, None],
        *tables,
    ]
    vmem, anywhere = pl.BlockSpec(memory_space=pltpu.VMEM), pl.BlockSpec(memory_space=pl.ANY)
    in_specs = [vmem] * 2 + [anywhere] * 4 + [vmem] * 10

    def out(shape, dtype=f32):
        return jax.ShapeDtypeStruct(shape, dtype)

    outs = [
        out((piece, lw), bf16),
        out((piece, lw)),
        out((C, fw, r), bf16),
        out((C, 3 * hw, r), bf16),
        out((C, hw, r), bf16),
        out((C, fw, r), bf16),
        out((C, fw)),
        out((C, 3 * hw)),
        out((1, lw)),
        out((1, lw)),
        out((1, lw)),
    ]
    out_specs = [vmem] * 2 + [anywhere] * 4 + [vmem] * 5
    most = max(fw, 3 * hw, lw)
    V = pltpu.VMEM
    stages = len(bits_of(C)) + len(bits_of(T))
    blocks = C * T
    dma = pltpu.SemaphoreType.DMA
    scratch = [
        V((L, D), bf16), V((L, D), bf16),
        V((D, fw), bf16), V((D, 3 * hw), bf16), V((U, hw, r), bf16), V((U, fw, r), bf16),
        V((L, fw), bf16), V((L, fw), bf16), V((max(fw, 4 * hw), L), bf16),
        V((L, 3 * hw), bf16), V((L, hw), bf16), V((L, hw), bf16), V((L, 2), f32),
        V((U, fw, r), bf16), V((U + C, fw, r), bf16),
        V((U, 3 * hw, r), bf16), V((U + C, 3 * hw, r), bf16),
        V((U, hw, r), bf16), V((U + C, hw, r), bf16),
        V((T - 1, L, lw), bf16), V(((C - 1) * piece, lw), bf16),
        V((8, most), f32), V((U, 8, most), f32), V((8, piece), f32), V((T - 1, 8, piece), f32),
        dma((4, C)), dma((4, C)), dma((6,)), dma((4, 2, U)), dma((4, U)),
        dma((4, 2, U)), dma((4, 2, U)), dma((4, C)), dma((4, C)), dma((4,)),
        dma((2, blocks)), dma((2, blocks)), dma((2, blocks)), dma((2, blocks)),
        dma((U - 1,)), dma((U - 1,)), dma((T - 1,)), dma((T - 1,)),
        pltpu.SemaphoreType.REGULAR((2,)), pltpu.SemaphoreType.REGULAR((stages,)),
    ]
    (
        block_out, grad_input, g_fc1, g_qkv, g_dense, g_fc2, fc1b_sum, qkvb_sum, outb_sum, gain_sum, bias_sum
    ) = pl.pallas_call(
        partial(block_kernel, (Z, C, T, r, fw, hw, lw, piece)),
        in_specs=in_specs,
        out_specs=out_specs,
        out_shape=outs,
        scratch_shapes=scratch,
        compiler_params=pltpu.CompilerParams(
            collective_id=0, has_side_effects=True, vmem_limit_bytes=67043328
        ),
        name="transformer_block",
    )(*operands)
    grad_fc1 = g_fc1.astype(f32).transpose(2, 0, 1).reshape(r, C * fw)
    grad_qkv = g_qkv.astype(f32).reshape(C, 3, hw, r).transpose(3, 1, 0, 2).reshape(r, 3, lw)
    qkv_bias_grad = qkvb_sum.reshape(C, 3, hw).transpose(1, 0, 2).reshape(3, lw)
    return (
        block_out[None],
        grad_input[None],
        grad_qkv,
        qkv_bias_grad,
        g_dense.astype(f32).reshape(lw, r),
        outb_sum[0],
        grad_fc1,
        fc1b_sum.reshape(-1),
        g_fc2.astype(f32).reshape(C * fw, r),
        outb_sum[0],
        gain_sum[0],
        bias_sum[0],
    )


def solution(mesh):
    in_specs = (
        P("dp", "ctx", "tensor"),
        P("dp", None),
        P(),
        P(),
        P(("dp", "ctx"), None, "tensor"),
        P(None, "tensor"),
        P("tensor", ("dp", "ctx")),
        P("tensor"),
        P(("dp", "ctx"), "tensor"),
        P("tensor"),
        P("tensor", ("dp", "ctx")),
        P("tensor"),
        P("dp", "ctx", "tensor"),
    )
    out_specs = (
        P("dp", "ctx", "tensor"),
        P("dp", "ctx", "tensor"),
        P(("dp", "ctx"), None, "tensor"),
        P(None, "tensor"),
        P("tensor", ("dp", "ctx")),
        P("tensor"),
        P(("dp", "ctx"), "tensor"),
        P("tensor"),
        P("tensor", ("dp", "ctx")),
        P("tensor"),
        P("tensor"),
        P("tensor"),
    )
    return jax.shard_map(body, mesh=mesh, in_specs=in_specs, out_specs=out_specs, check_vma=False)
```

```python
from functools import partial
import math

import jax
import jax.numpy as jnp
import numpy as np
from jax import lax
from jax.experimental import pallas as pl
from jax.experimental.pallas import tpu as pltpu
from jax.sharding import PartitionSpec as P

HD = 64
ROT = 32
DOC_MAX = 512
BLOCK = 256
ROWS = 512

ln_eps = 1e-05
rope_base = 10000.0
mask_fill = -1e30
contract_rows = (((0,), (0,)), ((), ()))
contract_cols = (((1,), (1,)), ((), ()))
contract_in = (((1,), (0,)), ((), ()))
f32, bf16 = jnp.float32, jnp.bfloat16
MESH = pl.DeviceIdType.MESH

WEIGHTS = ("F1a", "F1b", "Qa", "Qb", "Da", "Db", "F2a", "F2b")
GRADS = ("f2a", "f2b", "qda", "qdb", "f1a", "f1b")
NEEDS = {
    "F1a": "F1a", "F1b": "F1b", "PRa": "Qa", "PRb": "Qb",
    "GAa": "Da", "GAb": "Db", "HGa": "F2a", "HGb": "F2b",
}
ATa0_, ATa1_, ATb0_, ATb1_, C_, Da_, Db_, END_ = "ATa0", "ATa1", "ATb0", "ATb1", "C", "Da", "Db", "END"
F1a_, F1b_, F2a_, F2b_, GAa_, GAb_, HGa_, HGb_ = "F1a", "F1b", "F2a", "F2b", "GAa", "GAb", "HGa", "HGb"
LN_, NORM_, NS_, OUT_, PRa_, PRb_, Qa_, Qb_ = "LN", "NORM", "NS", "OUT", "PRa", "PRb", "Qa", "Qb"
TAB_, U1a_, U1b_, U2a_, U2b_, UQa_, UQb_, WB_ = "TAB", "U1a", "U1b", "U2a", "U2b", "UQa", "UQb", "WB"
WI_, a_, act_, actw_, af1_, af2_, an_, b_ = "WI", "a", "act", "actw", "af1", "af2", "an", "b"
c3_, cA1_, cA2_, cB1_, cB2_, f1a_, f1b_, f2a_ = "c3", "cA1", "cA2", "cB1", "cB2", "f1a", "f1b", "f2a"
f2b_, fin_, finw_, fr_, fw_, h3_, hA1_, hA2_ = "f2b", "fin", "finw", "fr", "fw", "h3", "hA1", "hA2"
hB1_, hB2_, n1_, n2_, n3_, o0_, o0i_, o0o_ = "hB1", "hB2", "n1", "n2", "n3", "o0", "o0i", "o0o"
o1_, o1i_, o1o_, qda_, qdb_, rf_, rn_, rsend_ = "o1", "o1i", "o1o", "qda", "qdb", "rf", "rn", "rsend"
st_, u1_, u2_, u3_, y_ = "st", "u1", "u2", "u3", "y"
SCHEDULE = (
    (
        LN_,
        (
            (y_, Db_), (y_, F1a_), (o0_, F2a_), (y_, Da_),
            (act_, cA1_), (act_, hB1_), (act_, hA1_), (o0_, Da_),
            (o0_, F1a_), (o0_, F1b_), (o0_, Qa_), (y_, Qa_),
            (act_, cA2_), (o0_, Qb_), (o1_, Da_), (o1_, F1a_),
            (y_, F1b_), (o1_, F1b_), (o0_, F2b_), (act_, hA2_),
            (o1_, Qa_), (y_, F2b_), (act_, hB2_), (y_, F2a_),
            (o1_, F2b_), (act_, cB1_), (act_, cB2_), (act_, h3_),
            (act_, c3_), (o0_, Db_), (y_, Qb_), (o1_, F2a_),
            (o1_, Qb_), (o1_, Db_), (actw_, h3_),
        ),
        (
            (o0i_, Qb_), (o0o_, Qa_), (o0i_, F1b_), (o0i_, Da_),
            (y_, Da_), (o0o_, F1a_), (y_, Qa_), (act_, hB1_),
            (o0o_, F1b_), (y_, F1a_), (y_, F2b_), (act_, cA1_),
            (o0i_, F1a_), (o0o_, F2a_), (act_, hA1_), (o0i_, Db_),
            (y_, F2a_), (o1i_, Qa_), (o1i_, F1a_), (af1_, Qb_, 0),
            (o1i_, Da_), (af1_, F1a_, 0), (act_, cB1_), (y_, Qb_),
            (af1_, F1a_, 1), (o1o_, F1a_), (af1_, F1b_, 0), (an_, F1b_, 0),
            (o0o_, Db_), (an_, F1a_, 1), (act_, cB2_), (y_, F1b_),
            (act_, cA2_), (af1_, Da_, 0), (an_, F1b_, 1), (an_, Qb_, 0),
            (af2_, F1a_, 1), (an_, Da_, 1), (act_, hA2_), (an_, F1a_, 0),
            (an_, Qa_, 1), (an_, Da_, 0), (af1_, Qa_, 1), (o1o_, Da_),
            (act_, hB2_), (o0o_, Da_), (an_, Qa_, 0), (o1o_, F1b_),
            (o0i_, F2a_), (o0i_, Qa_), (af2_, Da_, 0), (af2_, F1a_, 0),
            (af2_, Da_, 1), (o1i_, F2b_), (act_, c3_), (af2_, Qb_, 0),
            (actw_, c3_), (af2_, F1b_, 0), (af2_, Qa_, 1), (act_, h3_),
            (actw_, h3_), (an_, Db_, 0), (o1i_, F1b_), (an_, F2a_, 0),
            (an_, Qb_, 1), (o0o_, Qb_),
        ),
    ),
    (
        F1a_,
        (),
        (
            (an_, Db_, 1), (af1_, F1b_, 1), (af2_, F1b_, 1),
        ),
    ),
    (
        U2a_,
        (
            (actw_, c3_),
        ),
        (),
    ),
    (
        F1b_,
        (
            (rsend_, f2a_),
        ),
        (),
    ),
    (
        U2b_,
        (),
        (
            (af1_, Qa_, 0), (o1o_, Qa_),
        ),
    ),
    (
        TAB_,
        (
            (rsend_, f2b_),
        ),
        (
            (rn_, f2a_, 2, 0),
        ),
    ),
    (
        PRa_,
        (),
        (
            (af1_, Da_, 1), (o1i_, F2a_), (af2_, Qa_, 0), (rn_, f2a_, 3, 1),
            (o1i_, Qb_), (af2_, Qb_, 1), (rn_, f2a_, 3, 0), (af1_, Db_, 0),
            (an_, F2b_, 0), (o1o_, F2a_), (af1_, F2b_, 1), (rn_, f2a_, 2, 1),
            (o0i_, F2b_), (an_, F2a_, 1), (af1_, F2a_, 1),
        ),
    ),
    (
        GAa_,
        (),
        (
            (af1_, Qb_, 1), (af2_, Db_, 0),
        ),
    ),
    (
        ATa0_,
        (),
        (
            (af2_, F2a_, 0), (y_, Db_), (o1o_, Db_), (rf_, f2a_, 1),
        ),
    ),
    (
        ATa1_,
        (),
        (),
    ),
    (
        UQa_,
        (),
        (
            (o1i_, Db_), (rf_, f2a_, 0),
        ),
    ),
    (
        HGa_,
        (
            (rsend_, qda_), (fin_, f2a_, 0), (fin_, f2a_, 1), (fr_, a_),
            (fw_, a_),
        ),
        (
            (af1_, Db_, 1), (af1_, F2a_, 0), (an_, F2b_, 1), (af2_, F2a_, 1),
        ),
    ),
    (
        U1a_,
        (),
        (
            (rn_, f2b_, 2, 1), (rn_, qda_, 3, 0), (rn_, f2b_, 3, 0), (o1o_, Qb_),
            (fin_, f2a_, 0), (af2_, Db_, 1), (af1_, F2b_, 0), (rn_, f2b_, 3, 1),
            (rn_, qda_, 2, 1), (af2_, F2b_, 1), (fin_, f2a_, 1), (o1o_, F2b_),
            (fr_, a_),
        ),
    ),
    (
        GAb_,
        (),
        (),
    ),
    (
        PRb_,
        (
            (rsend_, f1a_),
        ),
        (
            (o0o_, F2b_),
        ),
    ),
    (
        ATb0_,
        (),
        (),
    ),
    (
        ATb1_,
        (),
        (
            (rn_, f2b_, 2, 0),
        ),
    ),
    (
        UQb_,
        (),
        (),
    ),
    (
        HGb_,
        (
            (rsend_, qdb_),
        ),
        (
            (af2_, F2b_, 0), (fw_, a_), (rn_, f1a_, 3, 0),
        ),
    ),
    (
        OUT_,
        (
            (finw_, f2a_),
        ),
        (
            (rf_, f2b_, 0), (rn_, qda_, 3, 1),
        ),
    ),
    (
        U1b_,
        (
            (act_, u1_), (fin_, f2b_, 0), (fin_, f2b_, 1), (act_, u2_),
            (fr_, b_), (fw_, b_),
        ),
        (
            (act_, u1_), (rf_, f2b_, 1), (rn_, f1a_, 3, 1), (rf_, f1a_, 0),
            (fin_, f2b_, 1), (fin_, f2b_, 0), (rn_, f1a_, 2, 0), (act_, u2_),
            (fr_, b_),
        ),
    ),
    (
        NORM_,
        (
            (rsend_, f1b_),
        ),
        (
            (rf_, qda_, 0), (rn_, qdb_, 3, 0),
        ),
    ),
    (
        WB_,
        (
            (act_, n1_), (fin_, f1a_, 0), (fin_, qdb_, 0), (act_, n2_),
            (act_, u3_), (actw_, u3_), (fin_, qda_, 1), (fin_, qda_, 0),
            (act_, n3_), (fin_, f1b_, 0),
        ),
        (
            (act_, n1_), (rf_, qdb_, 0), (rn_, qda_, 2, 0), (rn_, qdb_, 2, 0),
            (rf_, qda_, 1), (fin_, f1a_, 0), (fin_, qda_, 0), (act_, u3_),
            (act_, n2_), (finw_, f2b_), (rn_, qdb_, 3, 1), (rn_, f1a_, 2, 1),
            (fw_, b_), (fin_, qdb_, 0), (rn_, f1b_, 3, 0), (rn_, qdb_, 2, 1),
            (actw_, u3_), (rf_, f1a_, 1), (rf_, qdb_, 1), (act_, n3_),
            (rf_, f1b_, 0), (rn_, f1b_, 3, 1), (fin_, qdb_, 1), (rn_, f1b_, 2, 0),
        ),
    ),
    (
        NS_,
        (
            (actw_, n3_),
        ),
        (
            (rf_, f1b_, 1), (rn_, f1b_, 2, 1), (actw_, n3_), (fin_, f1a_, 1),
        ),
    ),
    (
        WI_,
        (
            (fin_, f1a_, 1), (fin_, f1b_, 1), (finw_, f1a_), (act_, st_),
            (actw_, st_),
        ),
        (
            (fin_, f1b_, 0), (act_, st_), (actw_, st_),
        ),
    ),
    (
        END_,
        (
            (finw_, qda_), (fin_, qdb_, 1), (finw_, qdb_), (finw_, f2b_),
            (finw_, f1b_),
        ),
        (
            (fin_, f1b_, 1), (finw_, f1b_), (finw_, qdb_), (finw_, f1a_),
            (finw_, f2a_), (fin_, qda_, 1), (finw_, qda_),
        ),
    ),
)


def fdot(a, b, dims=contract_in):
    return lax.dot_general(a, b, dims, preferred_element_type=f32)


def tiles(total, size, step):
    if total == size:
        step(0)
    else:
        pl.loop(0, total // size)(lambda i: step(pl.multiple_of(i * size, size)))


def bits_of(count):
    return [1 << i for i in range(count.bit_length() - 1)]


def block_kernel(dims, *refs):
    Z, C, T, r, fw, hw, lw, piece = dims
    (
        hid, cot_in, fc1w, qkvw, densew, fc2w, gain, bias, fc1b, qkvb, dense_b, fc2_b, segs, freqs,
        block_out, grad_input, g_fc1, g_qd, g_fc2, o_fc1b, o_qkvb, o_outb, o_gain, o_bias,
        X, COT, W1, WQ, WD, W2, ACT, DG, TT, QV, GA, ATT, MI, COS, SIN,
        G2, R2, GQ, RQ, RT, RC, SM, SMR, ST, STR, qs, ks, dq, dk, dv,
        y_s, y_r, own_s, ag_s, ag_r, rs_s, rs_r, fin_s, fin_r, out_s,
        aa_s, aa_r, ar_s, ar_r, sm_s, sm_r, st_s, st_r, free,
    ) = refs
    L, D, U, last = piece * C, T * lw, Z * C, Z - 1
    fh, gw = fw // 2, min(hw, 128)
    groups, in_group, aligned = hw // gw, gw // HD, gw % 128 == 0
    z, c, t = lax.axis_index("dp"), lax.axis_index("ctx"), lax.axis_index("tensor")
    end_side, mid_side = z // last, z - 1
    end_in, mid_in, mid_out = z + 1 - 2 * end_side, last - z, last * mid_side
    is_end, is_mid = (z == 0) | (z == last), (z > 0) & (z < last)

    def remote(src, dst, send, recv, **where):
        return pltpu.make_async_remote_copy(
            src_ref=src, dst_ref=dst, send_sem=send, recv_sem=recv,
            device_id=where, device_id_type=MESH,
        )

    def exists(name):
        return groups == 2 or name[:2] not in ("Qb", "Db") and name != "qdb"

    def sub_offsets(own):
        return [0] if own else list(range(1, C))

    def weight(p, u):
        half = "ab".index(p[-1])
        if p[:2] == "F1":
            return W1.at[pl.ds(pl.multiple_of(u * r, r), r), half * fh : (half + 1) * fh]
        if p[0] == "Q":
            return WQ.at[half, :, pl.ds(pl.multiple_of(u * r, r), r)]
        if p[0] == "D":
            return WD.at[u, half * gw : (half + 1) * gw]
        return W2.at[u, half * fh : (half + 1) * fh]

    def shard(p, k):
        half = "ab".index(p[-1])
        if p[:2] == "F1":
            return fc1w.at[:, pl.ds(pl.multiple_of(k * fw + half * fh, fh), fh)]
        if p[0] == "Q":
            if not aligned:
                return qkvw.at[k, half]
            return qkvw.at[:, :, pl.ds(pl.multiple_of(k * hw + half * gw, gw), gw)]
        if p[0] == "D":
            return densew.at[k, half * gw : (half + 1) * gw]
        return fc2w.at[k, half * fh : (half + 1) * fh]

    def y_copy(p, o):
        i, k = WEIGHTS.index(p), (c + o) % C
        return remote(shard(p, k), weight(p, z * C + c), y_s.at[i, o], y_r.at[i, o], ctx=k)

    def own_copy(p):
        i = WEIGHTS.index(p)
        return pltpu.make_async_copy(shard(p, c), weight(p, z * C + c), own_s.at[i])

    def ag_copy(p, u, way, to, src=None):
        i = WEIGHTS.index(p)
        src = weight(p, u) if src is None else src
        return remote(src, weight(p, u), ag_s.at[i, way, u], ag_r.at[i, u], dp=to)

    def ag_wait(p, u):
        ag_copy(p, u, 0, end_in).wait_recv()

    def y_start(p):
        for o in range(1, C):
            y_copy(p, o).start()
        own_copy(p).start()

    def send_own(p, second, way, to):
        if not second:
            ag_copy(p, z * C + c, way, to, shard(p, c)).start()
        for o in range(1, C) if second else ():
            ag_copy(p, z * C + (c - o) % C, way, to).start()

    def y_wait(p):
        for o in range(1, C):
            i, u, k = WEIGHTS.index(p), z * C + (c - o) % C, (c + o) % C
            remote(shard(p, k), weight(p, u), y_s.at[i, o], y_r.at[i, o], ctx=k).wait_recv()

    def forward(p, chunk, sub, way, to):
        for o in sub_offsets(sub == 0):
            u = chunk * C + (c - o) % C
            ag_wait(p, u)
            ag_copy(p, u, way, to).start()

    def weights_end(p):
        for o in range(1, C):
            y_copy(p, o).wait_send()
        for cs in range(C):

            @pl.when(is_end)
            def _():
                ag_copy(p, z * C + cs, 0, end_in).wait_send()

            @pl.when(is_mid)
            def _():
                for way, chunk in ((0, z), (1, z), (0, mid_out), (1, mid_in), (1, last - mid_out)):
                    ag_copy(p, chunk * C + cs, way, mid_in).wait_send()

    def doubling(index, array, own, part, order):
        rows_half = piece // 2
        masks, blocks, at, plan = [0], 1, 0, []
        for axis, bit in order:
            plan.append((axis, bit, blocks, tuple(masks), at))
            at += len(masks) * blocks
            if axis == "c":
                blocks *= 2
            else:
                masks = masks + [m ^ bit for m in masks]

        def copies(stage):
            axis, bit, count, sent, first = plan[stage]
            where = {"ctx": c ^ bit} if axis == "c" else {"tensor": t ^ bit}
            found = []
            for b in range(count):
                start = ((c // count) * count + b) * piece + part * rows_half
                for j, m in enumerate(sent):
                    dst = array.at[
                        pl.ds(pl.multiple_of(start, rows_half), rows_half),
                        pl.ds(pl.multiple_of((t ^ m) * lw, lw), lw),
                    ]
                    src = own.at[part * rows_half : (part + 1) * rows_half] if stage == 0 else dst
                    sem = first + b * len(sent) + j
                    found.append(remote(src, dst, aa_s.at[index, sem], aa_r.at[index, sem], **where))
            return found

        def begin(stage):
            for copy in copies(stage):
                copy.start()

        def arrive(stage):
            for copy in copies(stage):
                copy.wait_recv()

        def end():
            for stage in range(len(plan)):
                for copy in copies(stage):
                    copy.wait_send()

        return begin, arrive, end

    cbits = [("c", b) for b in bits_of(C)]
    tbits = [("t", b) for b in reversed(bits_of(T))]
    routes = (cbits + tbits, tbits[:-1] + cbits + tbits[-1:])
    doubles = {
        name + "AB"[part]: doubling(2 * i + part, array, own, part, routes[part])
        for i, (name, array, own) in enumerate((("h", X, hid), ("c", COT, cot_in)))
        for part in range(2)
    }
    doubling_stages = len(cbits) + len(tbits)

    def place(array, own, sem):
        return pltpu.make_async_copy(
            own,
            array.at[
                pl.ds(pl.multiple_of(c * piece, piece), piece), pl.ds(pl.multiple_of(t * lw, lw), lw)
            ],
            sem,
        )

    def double(name, step):
        if step == "3":
            for part in "AB":
                begin, arrive, _ = doubles[name + part]
                arrive(doubling_stages - 2)
                begin(doubling_stages - 1)
        else:
            begin, arrive, _ = doubles[name]
            stages = [0] if step == "1" else range(1, doubling_stages - 1)
            for stage in stages:
                if stage:
                    arrive(stage - 1)
                begin(stage)

    def double_wait(name):
        for part in "AB":
            doubles[name + part][1](doubling_stages - 1)

    def double_end(name):
        for part in "AB":
            doubles[name + part][2]()

    def grad_rows(q):
        return 4 * gw if q[0] == "q" else fh

    def grad_at(q, u, row, size, slots=False):
        half = "ab".index(q[-1])
        if q[0] == "q":
            return (RQ if slots else GQ).at[half, u, pl.ds(row, size)]
        return (R2 if slots else G2).at[u, pl.ds(half * fh + row, size)]

    def whole_at(q, u, slots=False):
        return grad_at(q, u, 0, grad_rows(q), slots)

    def grad_out(q):
        half = "ab".index(q[-1])
        if q[0] == "q":
            return g_qd.at[c, half]
        return (g_fc2 if q[1] == "2" else g_fc1).at[c, half * fh : (half + 1) * fh]

    def rs_copy(q, u, slot, kind, to):
        i = GRADS.index(q)
        return remote(
            whole_at(q, u), whole_at(q, slot, True), rs_s.at[i, u], rs_r.at[i, kind, u], dp=to
        )

    def rs_add(q, u, slots):
        size = min(128, grad_rows(q))

        def add(row):
            ref = grad_at(q, u, row, size)
            total = ref[...].astype(f32)
            for slot in slots:
                total = total + grad_at(q, slot, row, size, True)[...].astype(f32)
            ref[...] = total.astype(bf16)

        tiles(grad_rows(q), size, add)

    def rs_send(q):
        for k in range(last):
            d = end_side * k + (1 - end_side) * (last - k)
            for own in (False, True):
                for o in sub_offsets(own):
                    u = d * C + (c + o) % C
                    rs_copy(q, u, u + C * (1 - end_side), 0, end_in).start()

    def rs_near(q, dist, sub):
        d = last * (1 - mid_side) if dist == last else last - z
        for o in sub_offsets(sub == 1):
            u = d * C + (c + o) % C
            slot = u + C * (1 - mid_side)
            rs_copy(q, u, slot, 0, mid_in).wait_recv()
            rs_add(q, u, [slot])
            rs_copy(q, u, slot, 1, mid_in).start()

    def rs_far(q, sub):
        for o in sub_offsets(sub == 1):
            u = last * mid_side * C + (c + o) % C
            slot = u + C * mid_side
            rs_copy(q, u, slot, 1, mid_out).wait_recv()
            rs_add(q, u, [slot])
            rs_copy(q, u, slot, 1, mid_out).start()

    def fin_copy(q, o):
        i, k = GRADS.index(q), (c + o) % C
        return remote(whole_at(q, z * C + k), grad_out(q), fin_s.at[i, o], fin_r.at[i, o], ctx=k)

    def fin_own(q):
        return pltpu.make_async_copy(
            whole_at(q, z * C + c), grad_out(q), out_s.at[GRADS.index(q)]
        )

    def finish(q, sub, at_end):
        for o in sub_offsets(sub == 1):
            u = z * C + (c + o) % C
            if at_end:
                slots = [u + C * end_side]
                rs_copy(q, u, slots[0], 1, end_in).wait_recv()
            else:
                slots = [u + C * (1 - mid_side), u + C * mid_side]
                for kind in range(2):
                    rs_copy(q, u, slots[kind], kind, mid_in).wait_recv()
            rs_add(q, u, slots)
            if o:
                fin_copy(q, o).start()
            else:
                fin_own(q).start()

    def grads_sent(q):
        for dz in range(1, Z):
            for cs in range(C):
                u = ((z + dz) % Z) * C + cs
                rs_copy(q, u, u, 0, (z + dz) % Z).wait_send()
        for o in range(1, C):
            fin_copy(q, o).wait_send()
        fin_own(q).wait()

    def grads_arrived(q):
        for o in range(1, C):
            fin_copy(q, o).wait_recv()

    def tables():
        lane = lax.broadcasted_iota(jnp.int32, (128, gw), 1) % HD

        def rows_of(row):
            rows = pl.ds(row, 128)
            every = segs[...].astype(f32)
            own = jnp.broadcast_to(segs[:, rows].astype(f32), (128, 128)).T[:, 0:1]
            start = jnp.sum((every < own).astype(f32), axis=1, keepdims=True)
            at = (lax.broadcasted_iota(jnp.int32, (128, 1), 0) + row).astype(f32)
            angle = (at - start) * freqs[...]
            MI[rows, 2:3] = start
            COS[rows] = jnp.cos(angle)
            sine = jnp.sin(angle)
            SIN[rows] = jnp.where(lane < ROT // 2, -sine, sine)

        tiles(L, 128, rows_of)
        SM[...] = jnp.zeros_like(SM)
        SM[2:3, :lw] = jnp.sum(cot_in[...].astype(f32), axis=0, keepdims=True)

    def layer_norm():
        double_end("h")

        def rows_of(row):
            rows = pl.ds(row, 128)
            x = X[rows].astype(f32)
            mean = jnp.mean(x, axis=1, keepdims=True)
            centered = x - mean
            inv = lax.rsqrt(jnp.mean(centered * centered, axis=1, keepdims=True) + ln_eps)
            MI[rows, 0:1] = mean
            MI[rows, 1:2] = inv
            X[rows] = (centered * inv * gain[...] + bias[...]).astype(bf16)

        tiles(L, 128, rows_of)

    cf = min(BLOCK, fh)
    gelu_c = math.sqrt(2.0 / math.pi)

    def hidden(half):
        def cols_of(col):
            cols = pl.ds(half * fh + col, cf)
            shift = fc1b[:, pl.ds(pl.multiple_of(c * fw + half * fh + col, cf), cf)]

            def rows_of(row):
                rows = pl.ds(row, ROWS)
                v = fdot(X[rows], W1[:, cols]) + shift
                tanh = jnp.tanh(gelu_c * (v + 0.044715 * (v * v * v)))
                act = 0.5 * v * (1.0 + tanh)
                slope = gelu_c * (1.0 + 3.0 * 0.044715 * (v * v))
                DG[rows, cols] = (0.5 * (1.0 + tanh) + 0.5 * v * (1.0 - tanh * tanh) * slope).astype(bf16)
                ACT[rows, cols] = act.astype(bf16)
                TT[cols, rows] = act.T.astype(bf16)

            tiles(L, ROWS, rows_of)

        tiles(fh, cf, cols_of)

    def over_each_unit(step):
        if r % 128 == 0:
            pl.loop(0, U)(lambda u: step(u, pl.ds(pl.multiple_of(u * r, r), r)))
        else:
            for u in range(U):
                step(u, slice(u * r, (u + 1) * r))

    def unit_grads(q):
        half = "ab".index(q[-1])

        def step(u, cols):
            if q[0] == "q":
                first = half * 4 * gw
                GQ[half, u, : 3 * gw] = fdot(TT[first : first + 3 * gw], X[:, cols]).astype(bf16)
                GQ[half, u, 3 * gw :] = fdot(TT[first + 3 * gw : first + 4 * gw], COT[:, cols]).astype(bf16)
            else:
                rows = slice(half * fh, (half + 1) * fh)
                source = COT if q[1] == "2" else X
                G2[u, rows] = fdot(TT[rows], source[:, cols]).astype(bf16)

        over_each_unit(step)

    def side_by_side(rows, group):
        return jnp.concatenate([WQ[group, part, rows] for part in range(3)], axis=1)

    def project(group):
        def shift(part):
            if not aligned:
                return qkvb[part : part + 1]
            return qkvb[part : part + 1, pl.ds(pl.multiple_of(c * hw + group * gw, gw), gw)]

        shifts = jnp.concatenate([shift(part) for part in range(3)], axis=1)

        def rows_of(row):
            rows = pl.ds(row, ROWS)
            QV[group, rows] = (fdot(X[rows], side_by_side(pl.ds(0, D), group)) + shifts).astype(bf16)

        tiles(L, ROWS, rows_of)

    def over_units(rows, weights):
        total = None
        for u in range(U):
            term = fdot(COT[rows, u * r : (u + 1) * r], weights(u), contract_cols)
            total = term if total is None else total + term
        return total

    def attended_grads(group):
        def rows_of(row):
            rows = pl.ds(row, ROWS)
            lanes = slice(group * gw, (group + 1) * gw)
            GA[rows] = over_units(rows, lambda u: WD[u, lanes]).astype(bf16)

        tiles(L, ROWS, rows_of)

    half_rot = ROT // 2
    scale = 1.0 / math.sqrt(HD)

    def turn(values, rows, sign):
        lane = lax.broadcasted_iota(jnp.int32, values.shape, 1) % HD
        other = jnp.where(
            lane < half_rot, pltpu.roll(values, gw - half_rot, 1), pltpu.roll(values, half_rot, 1)
        )
        turned = other * SIN[rows]
        return values * COS[rows] + (turned if sign > 0 else -turned)

    def attention_load(group):
        def load(row):
            rows = pl.ds(row, BLOCK)
            qs[rows] = turn(QV[group, rows, :gw].astype(f32), rows, 1).astype(bf16)
            ks[rows] = turn(QV[group, rows, gw : 2 * gw].astype(f32), rows, 1).astype(bf16)

        tiles(L, BLOCK, load)
        for ref in (dq, dk, dv):
            ref[...] = jnp.zeros_like(ref)
        ATT[:, group * gw : (group + 1) * gw] = jnp.zeros((L, gw), bf16)

    def attention_head(group, head):
        own = slice(group * gw, (group + 1) * gw)
        for row in range(0, L, BLOCK):
            low = max(0, row - DOC_MAX)
            span = row + BLOCK - low
            rows, cols = pl.ds(row, BLOCK), pl.ds(low, span)
            mine = lax.broadcasted_iota(jnp.int32, (BLOCK, gw), 1) // HD == head
            query = jnp.where(mine, qs[rows].astype(f32), 0.0).astype(bf16)
            grad = jnp.where(mine, GA[rows].astype(f32), 0.0)
            grad_b, key, value = grad.astype(bf16), ks[cols], QV[group, cols, 2 * gw :]
            query_pos = row + lax.broadcasted_iota(jnp.int32, (BLOCK, span), 0)
            key_pos = low + lax.broadcasted_iota(jnp.int32, (BLOCK, span), 1)
            allowed = (key_pos >= MI[rows, 2:3].astype(jnp.int32)) & (key_pos <= query_pos)
            scores = jnp.where(allowed, fdot(query, key, contract_cols) * scale, mask_fill)
            weights = jnp.exp(scores - jnp.max(scores, axis=1, keepdims=True))
            probs = weights * (1.0 / jnp.sum(weights, axis=1, keepdims=True))
            probs_b = probs.astype(bf16)
            attended = jnp.where(mine, fdot(probs_b, value), 0.0).astype(bf16)
            delta = jnp.sum(grad * attended.astype(f32), axis=1, keepdims=True)
            grad_probs = fdot(grad_b, value, contract_cols)
            grad_scores = (probs * (grad_probs - delta)).astype(bf16)
            dv[cols] += fdot(probs_b, grad_b, contract_rows)
            dk[cols] += fdot(grad_scores, query, contract_rows)
            dq[rows] += jnp.where(mine, fdot(grad_scores, key), 0.0)
            ATT[rows, own] += attended

    def attention_save(group):
        first = group * 4 * gw

        def save(row):
            rows = pl.ds(row, BLOCK)
            attended = ATT[rows, group * gw : (group + 1) * gw].astype(f32)
            TT[first + 3 * gw : first + 4 * gw, rows] = attended.T.astype(bf16)
            grads = turn(dq[rows] * scale, rows, -1), turn(dk[rows] * scale, rows, -1), dv[rows]
            for part, grad in enumerate(grads):
                lanes = slice(part * gw, (part + 1) * gw)
                QV[group, rows, lanes] = grad.astype(bf16)
                TT[first + part * gw : first + (part + 1) * gw, rows] = grad.T.astype(bf16)
                sums = jnp.sum(grad.astype(bf16).astype(f32), axis=0, keepdims=True)
                SM[5 + group : 6 + group, lanes] += sums

        tiles(L, BLOCK, save)

    def attention_heads(group, second):
        mine = range(in_group // 2, in_group) if second else range(in_group // 2)
        if in_group == 1:
            mine = [] if second else [0]
        if not second:
            attention_load(group)
        for head in mine:
            attention_head(group, head)
        if second:
            attention_save(group)

    def hidden_grads(half):
        for n in range(fh // cf):
            cols = slice(half * fh + n * cf, half * fh + (n + 1) * cf)

            def rows_of(row):
                rows = pl.ds(row, ROWS)
                grad = over_units(rows, lambda u: W2[u, cols]) * DG[rows, cols].astype(f32)
                SM[0:1, cols] += jnp.sum(grad, axis=0, keepdims=True)
                DG[rows, cols] = grad.astype(bf16)
                TT[cols, rows] = grad.T.astype(bf16)

            tiles(L, ROWS, rows_of)

    def halving(a, part):
        plan, masks, slot = [], list(range(T)), 0
        for bit in bits_of(T):
            kept = [m for m in masks if not m & bit]
            plan.append((bit, kept, slot))
            slot += len(kept)
            masks = kept
        cplan, offset = [], 0
        for bit in reversed(bits_of(C)):
            cplan.append((bit, offset))
            offset += bit * piece
        count = len(plan) + len(cplan)

        def cols_of(m):
            return pl.ds(pl.multiple_of((t ^ m) * lw, lw), lw)

        def copies(stage):
            if stage < len(plan):
                bit, kept, first = plan[stage]
                return [
                    remote(
                        part.at[:, cols_of(m ^ bit)], RT.at[a, first + j],
                        ar_s.at[a, first + j], ar_r.at[a, first + j], tensor=t ^ bit,
                    )
                    for j, m in enumerate(kept)
                ]
            bit, first = cplan[stage - len(plan)]
            start = ((c ^ bit) // bit) * bit * piece
            sem = slot + stage - len(plan)
            return [
                remote(
                    part.at[pl.ds(pl.multiple_of(start, piece), bit * piece), cols_of(0)],
                    RC.at[a, pl.ds(first, bit * piece)],
                    ar_s.at[a, sem], ar_r.at[a, sem], ctx=c ^ bit,
                )
            ]

        def begin(stage):
            for copy in copies(stage):
                copy.start()

        def arrive(stage):
            for copy in copies(stage):
                copy.wait_recv()
            if stage < len(plan):
                _, kept, first = plan[stage]
                for j, m in enumerate(kept):

                    def add(row):
                        rows = pl.ds(row, 128)
                        total = part[rows, cols_of(m)].astype(f32) + RT[a, first + j, rows].astype(f32)
                        part[rows, cols_of(m)] = total.astype(bf16)

                    tiles(L, 128, add)
            elif stage < count - 1:
                bit, first = cplan[stage - len(plan)]
                start = (c // bit) * bit * piece

                def add(row):
                    rows = pl.ds(pl.multiple_of(start + row, 128), 128)
                    total = part[rows, cols_of(0)].astype(f32) + RC[a, pl.ds(first + row, 128)].astype(f32)
                    part[rows, cols_of(0)] = total.astype(bf16)

                tiles(bit * piece, 128, add)

        def run(step):
            stages = {"1": [0], "2": range(1, count - 1), "3": [count - 1]}[step]
            for stage in stages:
                if stage:
                    arrive(stage - 1)
                begin(stage)

        def total(row):
            rows = pl.ds(pl.multiple_of(c * piece + row, 128), 128)
            return part[rows, cols_of(0)].astype(f32) + RC[a, pl.ds(cplan[-1][1] + row, 128)].astype(f32)

        def end():
            for stage in range(count):
                for copy in copies(stage):
                    copy.wait_send()

        return run, lambda: arrive(count - 1), total, end

    n_run, n_wait, n_total, n_end = halving(0, X)
    u_run, u_wait, u_total, u_end = halving(1, COT)

    def norm_units():
        def step(u, cols):
            w1 = W1[pl.ds(pl.multiple_of(u * r, r), r)]
            wq = [side_by_side(pl.ds(pl.multiple_of(u * r, r), r), g) for g in range(groups)]

            def rows_of(row):
                rows = pl.ds(row, ROWS)
                total = fdot(DG[rows], w1, contract_cols)
                for g in range(groups):
                    total = total + fdot(QV[g, rows], wq[g], contract_cols)
                X[rows, cols] = total.astype(bf16)

            tiles(L, ROWS, rows_of)

        over_each_unit(step)

    def out_units():
        double_end("c")

        def step(u, cols):
            def rows_of(row):
                rows = pl.ds(row, ROWS)
                COT[rows, cols] = (fdot(ATT[rows], WD[u]) + fdot(ACT[rows], W2[u])).astype(bf16)

            tiles(L, ROWS, rows_of)

        over_each_unit(step)

    def write_block():
        def rows_of(row):
            rows = pl.ds(row, 128)
            shift = dense_b[...] + fc2_b[...]
            block_out[rows] = (hid[rows].astype(f32) + u_total(row) + shift).astype(bf16)

        tiles(piece, 128, rows_of)

    def gain_own():
        return gain[:, pl.ds(pl.multiple_of(t * lw, lw), lw)]

    def standard_of(row):
        rows = pl.ds(pl.multiple_of(c * piece + row, 128), 128)
        inv = MI[rows, 1:2]
        return (hid[pl.ds(row, 128)].astype(f32) - MI[rows, 0:1]) * inv, inv

    def norm_sums():
        for row in range(0, piece, 128):
            grad = n_total(row)
            standard, _ = standard_of(row)
            scaled = grad * gain_own()
            first = jnp.sum(scaled, axis=1, keepdims=True)
            second = jnp.sum(scaled * standard, axis=1, keepdims=True)
            lane = lax.broadcasted_iota(jnp.int32, (128, 128), 1)
            pair = jnp.where(lane == 0, first, jnp.where(lane == 1, second, 0.0))
            ST[:, row : row + 128] = pair.T[0:8]
            SM[3:4, :lw] += jnp.sum(grad * standard, axis=0, keepdims=True)
            SM[4:5, :lw] += jnp.sum(grad, axis=0, keepdims=True)

    def st_copy(o):
        return remote(ST, STR.at[o - 1], st_s.at[o - 1], st_r.at[o - 1], tensor=(t + o) % T)

    def sm_copy(dz, dc):
        o = dz * C + dc - 1
        return remote(
            SM, SMR.at[z * C + c], sm_s.at[o], sm_r.at[o], dp=(z + dz) % Z, ctx=(c + dc) % C
        )

    offsets = [(dz, dc) for dz in range(Z) for dc in range(C) if dz or dc]

    def stats_start():
        for o in range(1, T):
            st_copy(o).start()
        for dz, dc in offsets:
            sm_copy(dz, dc).start()

    def stats_wait():
        for o in range(1, T):
            st_copy(o).wait()

    def write_input():
        for row in range(0, piece, 128):
            stats = ST[:, row : row + 128]
            for o in range(1, T):
                stats = stats + STR[o - 1, :, row : row + 128]
            stats = jnp.concatenate([stats, jnp.zeros((120, 128), f32)], axis=0).T * (1.0 / D)
            standard, inv = standard_of(row)
            scaled = n_total(row) * gain_own()
            rows = pl.ds(row, 128)
            grad_input[rows] = cot_in[rows].astype(f32) + inv * (
                scaled - stats[:, 0:1] - standard * stats[:, 1:2]
            )

    def small_sums():
        SMR[z * C + c] = SM[...]
        for dz, dc in offsets:
            sm_copy(dz, dc).wait()

        def summed(row, size, units):
            total = SMR[units[0], row : row + 1, :size]
            for u in units[1:]:
                total = total + SMR[u, row : row + 1, :size]
            return total

        for k in range(C):
            units = [zs * C + k for zs in range(Z)]
            o_fc1b[:, k * fw : (k + 1) * fw] = summed(0, fw, units)
            for g in range(groups):
                sums = summed(5 + g, 3 * gw, units)
                for part in range(3):
                    lanes = slice(k * hw + g * gw, k * hw + (g + 1) * gw)
                    o_qkvb[part : part + 1, lanes] = sums[:, part * gw : (part + 1) * gw]
        for i, out in enumerate((o_outb, o_gain, o_bias)):
            out[...] = summed(2 + i, lw, list(range(U)))

    computes = {"TAB": tables, "LN": layer_norm, "NORM": norm_units, "OUT": out_units}
    computes.update({"NS": norm_sums, "WI": write_input, "WB": write_block})
    for i, half in enumerate("ab"):
        computes["F1" + half] = partial(hidden, i)
        computes["U2" + half] = partial(unit_grads, "f2" + half)
        computes["U1" + half] = partial(unit_grads, "f1" + half)
        computes["HG" + half] = partial(hidden_grads, i)
        if i < groups:
            computes["PR" + half] = partial(project, i)
            computes["GA" + half] = partial(attended_grads, i)
            computes["AT" + half + "0"] = partial(attention_heads, i, False)
            computes["AT" + half + "1"] = partial(attention_heads, i, True)
            computes["UQ" + half] = partial(unit_grads, "qd" + half)

    def action(kind, name, *rest, at_end):
        if kind == "act" or kind == "actw":
            if name == "st":
                (stats_start if kind == "act" else stats_wait)()
            elif name[0] in "hc":
                if kind == "actw":
                    double_wait(name[0])
                elif name[1:] == "3":
                    double(name[0], "3")
                else:
                    double(name[:2], name[2])
            elif kind == "actw":
                (n_wait if name[0] == "n" else u_wait)()
            else:
                (n_run if name[0] == "n" else u_run)(name[1])
        elif kind == "fr":
            grads_sent("f2" + name)
            half = "ab".index(name)

            def tell(to, way):
                pl.semaphore_signal(free.at[half, way], 1, device_id={"dp": to}, device_id_type=MESH)

            if at_end:
                tell(end_in, 0)
            else:
                tell(mid_in, 1)
                tell(mid_out, 1)
        elif kind == "fw":
            half = "ab".index(name)
            if not at_end:
                pl.semaphore_wait(free.at[half, 0], 1)
            pl.semaphore_wait(free.at[half, 1], 1)
        elif not exists(name):
            return
        elif kind == "y":
            y_start(name)
        elif kind == "o0":
            send_own(name, False, 0, end_in)
        elif kind == "o1":
            y_wait(name)
            send_own(name, True, 0, end_in)
        elif kind in ("o0i", "o0o", "o1i", "o1o"):
            if kind[1] == "1" and (name, "seen") not in seen:
                y_wait(name)
                seen.add((name, "seen"))
            way = "io".index(kind[2])
            send_own(name, kind[1] == "1", way, (mid_in, mid_out)[way])
        elif kind == "an":
            forward(name, mid_out, rest[0], 0, mid_in)
        elif kind == "af1":
            forward(name, mid_in, rest[0], 1, mid_out)
        elif kind == "af2":
            forward(name, last - mid_out, rest[0], 1, mid_out)
        elif kind == "rsend":
            rs_send(name)
        elif kind == "rn":
            rs_near(name, *rest)
        elif kind == "rf":
            rs_far(name, *rest)
        elif kind == "fin":
            finish(name, rest[0], at_end)
        elif kind == "finw":
            grads_arrived(name)

    seen = set()

    barrier = pltpu.get_barrier_semaphore()
    for dz, dc in offsets:
        pl.semaphore_signal(
            barrier, 1, device_id={"dp": (z + dz) % Z, "ctx": (c + dc) % C}, device_id_type=MESH
        )
    for dt in range(1, T):
        pl.semaphore_signal(barrier, 1, device_id={"tensor": (t + dt) % T}, device_id_type=MESH)
    pl.semaphore_wait(barrier, U - 1 + T - 1)
    for i, (array, own) in enumerate(((X, hid), (COT, cot_in))):
        place(array, own, own_s.at[8 + i]).start()
    for i, (array, own) in enumerate(((X, hid), (COT, cot_in))):
        place(array, own, own_s.at[8 + i]).wait()

    for name, at_ends, inside in SCHEDULE:

        @pl.when(is_end)
        def _():
            for step in at_ends:
                action(*step, at_end=True)

        @pl.when(is_mid)
        def _():
            for step in inside:
                action(*step, at_end=False)

        if name not in computes:
            continue
        needed = NEEDS.get(name)
        if needed is not None:

            @pl.when(is_end)
            def _():
                for dz in range(1, Z):
                    for cs in range(C):
                        ag_wait(needed, ((z + dz) % Z) * C + cs)

            own_copy(needed).wait()
        computes[name]()

    small_sums()
    n_end()
    u_end()
    for p in WEIGHTS:
        if exists(p):
            weights_end(p)
    for q in GRADS[2:]:
        if exists(q):
            grads_sent(q)


def body(
    hidden_in,
    segments,
    ln_gain,
    ln_bias,
    qkv_weight,
    qkv_bias,
    dense_weight,
    dense_bias,
    fc1_weight,
    fc1_bias,
    fc2_weight,
    fc2_bias,
    cotangent,
):
    _, piece, lw = hidden_in.shape
    C, T, Z = lax.axis_size("ctx"), lax.axis_size("tensor"), lax.axis_size("dp")
    L, D, U = piece * C, lw * T, Z * C
    r = qkv_weight.shape[0]
    hw, fw = lw // C, fc1_weight.shape[1] // C
    gw = min(hw, 128)
    groups, aligned = hw // gw, gw % 128 == 0
    lane = np.arange(gw) % HD
    freqs = rope_base ** (-((lane % (ROT // 2)) * 2.0) / ROT)
    freqs = jnp.asarray(np.where(lane < ROT, freqs, 0.0)[None], f32)
    if aligned:
        qkvw, own_bias = qkv_weight.transpose(1, 0, 2), qkv_bias
    else:
        qkvw = qkv_weight.reshape(r, 3, C, groups, gw).transpose(2, 3, 1, 0, 4)
        own_bias = lax.dynamic_slice_in_dim(qkv_bias, lax.axis_index("ctx") * hw, hw, 1)
    operands = [
        hidden_in[0],
        cotangent[0],
        fc1_weight,
        qkvw,
        dense_weight.reshape(C, hw, r),
        fc2_weight.reshape(C, fw, r),
        ln_gain[None],
        ln_bias[None],
        fc1_bias[None],
        own_bias,
        dense_bias[None],
        fc2_bias[None],
        segments,
        freqs,
    ]
    vmem, anywhere = pl.BlockSpec(memory_space=pltpu.VMEM), pl.BlockSpec(memory_space=pl.ANY)
    in_specs = [vmem] * 2 + [anywhere] * 4 + [vmem] * 8

    def out(shape, dtype=f32):
        return jax.ShapeDtypeStruct(shape, dtype)

    outs = [
        out((piece, lw), bf16),
        out((piece, lw)),
        out((C, fw, r), bf16),
        out((C, groups, 4 * gw, r), bf16),
        out((C, fw, r), bf16),
        out((1, C * fw)),
        out((3, lw)),
        out((1, lw)),
        out((1, lw)),
        out((1, lw)),
    ]
    out_specs = [vmem] * 2 + [anywhere] * 3 + [vmem] * 5
    most = max(fw, 3 * gw, lw)
    V = pltpu.VMEM
    dma = pltpu.SemaphoreType.DMA
    blocks = C * T
    scratch = [
        V((L, D), bf16), V((L, D), bf16),
        V((D, fw), bf16), V((groups, 3, D, gw), bf16), V((U, hw, r), bf16), V((U, fw, r), bf16),
        V((L, fw), bf16), V((L, fw), bf16), V((max(fw, 4 * hw), L), bf16),
        V((groups, L, 3 * gw), bf16), V((L, gw), bf16), V((L, hw), bf16), V((L, 4), f32),
        V((L, gw), f32), V((L, gw), f32),
        V((U, fw, r), bf16), V((U + C, fw, r), bf16),
        V((groups, U, 4 * gw, r), bf16), V((groups, U + C, 4 * gw, r), bf16),
        V((2, T - 1, L, lw), bf16), V((2, (C - 1) * piece, lw), bf16),
        V((8, most), f32), V((U, 8, most), f32), V((8, piece), f32), V((T - 1, 8, piece), f32),
        *[V((L, gw), bf16)] * 2, *[V((L, gw), f32)] * 3,
        dma((8, C)), dma((8, C)), dma((10,)), dma((8, 2, U)), dma((8, U)),
        dma((6, U)), dma((6, 2, U)), dma((6, C)), dma((6, C)), dma((6,)),
        dma((4, blocks)), dma((4, blocks)), dma((2, blocks)), dma((2, blocks)),
        dma((U - 1,)), dma((U - 1,)), dma((T - 1,)), dma((T - 1,)),
        pltpu.SemaphoreType.REGULAR((2, 2)),
    ]
    results = pl.pallas_call(
        partial(block_kernel, (Z, C, T, r, fw, hw, lw, piece)),
        in_specs=in_specs,
        out_specs=out_specs,
        out_shape=outs,
        scratch_shapes=scratch,
        compiler_params=pltpu.CompilerParams(
            collective_id=0, has_side_effects=True, vmem_limit_bytes=67043328
        ),
        name="transformer_block",
    )(*operands)
    block_out, grad_input, g_fc1, g_qd, g_fc2, *sums = results
    if aligned and r % 128 == 0:
        block_out, grad_input, grad_fc1, grad_qkv, grad_dense, grad_fc2, *sums = unpack(results)
        grad_qkv = grad_qkv.transpose(1, 0, 2)
    else:
        sums.append(sums[2])
        grad_fc1 = g_fc1.astype(f32).transpose(2, 0, 1).reshape(r, C * fw)
        grad_qkv = g_qd[:, :, : 3 * gw].astype(f32).reshape(C, groups, 3, gw, r)
        grad_qkv = grad_qkv.transpose(4, 2, 0, 1, 3).reshape(r, 3, lw)
        grad_dense = g_qd[:, :, 3 * gw :].astype(f32).reshape(lw, r)
        grad_fc2 = g_fc2.astype(f32).reshape(C * fw, r)
    return (
        block_out[None],
        grad_input[None],
        grad_qkv,
        sums[1],
        grad_dense,
        sums[2][0],
        grad_fc1,
        sums[0][0],
        grad_fc2,
        sums[5][0],
        sums[3][0],
        sums[4][0],
    )


def unpack_kernel(gw, *refs):
    (block, input_grad, fc1, qd, fc2), sums, outs = refs[:5], refs[5:10], refs[10:]
    o_block, o_input, o_fc1, o_qkv, o_dense, o_fc2 = outs[:6]
    o_block[...] = block[...]
    o_input[...] = input_grad[...]
    o_fc1[...] = fc1[...].astype(f32).T
    o_fc2[...] = fc2[...].astype(f32)
    o_dense[...] = qd[0, 3 * gw :].astype(f32)
    for part in range(3):
        o_qkv[part] = qd[0, part * gw : (part + 1) * gw].astype(f32).T

    @pl.when(pl.program_id(0) == 0)
    def _():
        for src, dst in zip((*sums, sums[2]), outs[6:]):
            dst[...] = src[...]


def unpack(results):
    block_out, grad_input, g_fc1, g_qd, g_fc2, *sums = results
    (piece, lw), (C, fw, r), (_, groups, quad, _) = block_out.shape, g_fc1.shape, g_qd.shape
    gw, steps = quad // 4, C * groups
    part = C * fw // steps

    def rows(size, width):
        return pl.BlockSpec((size, width), lambda i: (i, 0))

    def cols(shape):
        return pl.BlockSpec(shape, lambda i: (0,) * (len(shape) - 1) + (i,))

    small = [pl.BlockSpec(s.shape, lambda i: (0, 0)) for s in sums]
    return pl.pallas_call(
        partial(unpack_kernel, gw),
        grid=(steps,),
        in_specs=[
            rows(piece // steps, lw), rows(piece // steps, lw), rows(part, r),
            pl.BlockSpec((1, quad, r), lambda i: (i, 0, 0)), rows(part, r), *small,
        ],
        out_specs=[
            rows(piece // steps, lw), rows(piece // steps, lw), cols((r, part)),
            cols((3, r, gw)), rows(gw, r), rows(part, r), *small, small[2],
        ],
        out_shape=[
            jax.ShapeDtypeStruct((piece, lw), bf16),
            *[
                jax.ShapeDtypeStruct(shape, f32)
                for shape in (
                    (piece, lw), (r, C * fw), (3, r, lw), (lw, r), (C * fw, r),
                    *[s.shape for s in sums], sums[2].shape,
                )
            ],
        ],
        name="unpack_results",
    )(
        block_out, grad_input, g_fc1.reshape(C * fw, r), g_qd.reshape(steps, quad, r),
        g_fc2.reshape(C * fw, r), *sums,
    )


def solution(mesh):
    in_specs = (
        P("dp", "ctx", "tensor"),
        P("dp", None),
        P(),
        P(),
        P(("dp", "ctx"), None, "tensor"),
        P(None, "tensor"),
        P("tensor", ("dp", "ctx")),
        P("tensor"),
        P(("dp", "ctx"), "tensor"),
        P("tensor"),
        P("tensor", ("dp", "ctx")),
        P("tensor"),
        P("dp", "ctx", "tensor"),
    )
    out_specs = (
        P("dp", "ctx", "tensor"),
        P("dp", "ctx", "tensor"),
        P(("dp", "ctx"), None, "tensor"),
        P(None, "tensor"),
        P("tensor", ("dp", "ctx")),
        P("tensor"),
        P(("dp", "ctx"), "tensor"),
        P("tensor"),
        P("tensor", ("dp", "ctx")),
        P("tensor"),
        P("tensor"),
        P("tensor"),
    )
    return jax.shard_map(body, mesh=mesh, in_specs=in_specs, out_specs=out_specs, check_vma=False)
```

```python
from functools import partial
import math

import jax
import jax.numpy as jnp
import numpy as np
from jax import lax
from jax.experimental import pallas as pl
from jax.experimental.pallas import tpu as pltpu
from jax.sharding import PartitionSpec as P

HD = 64
ROT = 32
DOC_MAX = 512
BLOCK = 256
ROWS = 512

ln_eps = 1e-05
rope_base = 10000.0
mask_fill = -1e30
contract_rows = (((0,), (0,)), ((), ()))
contract_cols = (((1,), (1,)), ((), ()))
contract_in = (((1,), (0,)), ((), ()))
f32, bf16 = jnp.float32, jnp.bfloat16
MESH = pl.DeviceIdType.MESH

WEIGHTS = ("F1a", "F1b", "Qa", "Qb", "Da", "Db", "F2a", "F2b")
GRADS = ("f2a", "f2b", "qda", "qdb", "f1a", "f1b")
NEEDS = {
    "F1a": "F1a", "F1b": "F1b", "PRa": "Qa", "PRb": "Qb",
    "GAa": "Da", "GAb": "Db", "HGa": "F2a", "HGb": "F2b",
}
ATa0_, ATa1_, ATb0_, ATb1_, C_, Da_, Db_, END_ = "ATa0", "ATa1", "ATb0", "ATb1", "C", "Da", "Db", "END"
F1a_, F1b_, F2a_, F2b_, GAa_, GAb_, HGa_, HGb_ = "F1a", "F1b", "F2a", "F2b", "GAa", "GAb", "HGa", "HGb"
LN_, NORM_, NS_, OUT_, PRa_, PRb_, Qa_, Qb_ = "LN", "NORM", "NS", "OUT", "PRa", "PRb", "Qa", "Qb"
TAB_, U1a_, U1b_, U2a_, U2b_, UQa_, UQb_, WB_ = "TAB", "U1a", "U1b", "U2a", "U2b", "UQa", "UQb", "WB"
WI_, a_, act_, actw_, af1_, af2_, an_, b_ = "WI", "a", "act", "actw", "af1", "af2", "an", "b"
c3_, cA1_, cA2_, cB1_, cB2_, f1a_, f1b_, f2a_ = "c3", "cA1", "cA2", "cB1", "cB2", "f1a", "f1b", "f2a"
f2b_, fin_, finw_, fr_, fw_, h3_, hA1_, hA2_ = "f2b", "fin", "finw", "fr", "fw", "h3", "hA1", "hA2"
hB1_, hB2_, n_, n1_, nA2_, nA3_, nB2_, nB3_ = "hB1", "hB2", "n", "n1", "nA2", "nA3", "nB2", "nB3"
o0_, o0i_, o0o_, o1_, o1i_, o1o_, qda_, qdb_ = "o0", "o0i", "o0o", "o1", "o1i", "o1o", "qda", "qdb"
rf_, rn_, rsend_, st_, u_, u1_, uA2_, uA3_ = "rf", "rn", "rsend", "st", "u", "u1", "uA2", "uA3"
uB2_, uB3_, y_ = "uB2", "uB3", "y"
SCHEDULE = (
    (
        TAB_,
        (
            (y_, F1a_), (y_, Db_), (o0_, F2a_), (act_, hB1_),
            (act_, cB1_), (y_, F1b_), (act_, cA1_), (y_, Da_),
            (y_, Qa_), (o0_, Qb_), (o1_, F1a_), (o0_, F1a_),
            (o0_, Qa_), (o1_, Da_), (act_, cA2_), (act_, hA1_),
            (act_, hB2_), (y_, Qb_), (o0_, Da_), (o0_, F1b_),
            (o1_, F1b_), (act_, cB2_),
        ),
        (
            (o0o_, F1a_), (act_, cB1_), (o0i_, Da_), (y_, F1b_),
            (y_, F1a_), (y_, Da_), (o0i_, F1a_), (o0o_, F2a_),
            (act_, hA1_), (o0i_, Qb_), (af1_, F1a_, 0), (o0i_, Qa_),
            (o1i_, F1a_), (act_, hB1_), (o0i_, F1b_), (o1o_, F1a_),
            (act_, cA1_), (act_, hB2_), (o1o_, F1b_), (o1o_, Da_),
            (an_, F1a_, 1), (o0o_, F1b_), (act_, hA2_), (af1_, F1a_, 1),
            (o0i_, Db_), (o1i_, Da_), (act_, cB2_), (o0o_, Qb_),
            (an_, F1a_, 0), (an_, Da_, 0), (af2_, F1a_, 1), (act_, cA2_),
            (act_, h3_),
        ),
    ),
    (
        LN_,
        (
            (act_, hA2_), (act_, h3_), (o1_, Qa_), (o0_, F2b_),
            (o1_, Qb_), (o0_, Db_), (o1_, Db_), (y_, F2a_),
            (actw_, h3_),
        ),
        (
            (an_, F1b_, 0), (y_, Qb_), (actw_, h3_), (o1i_, F1b_),
            (af2_, F1a_, 0),
        ),
    ),
    (
        F1a_,
        (
            (act_, c3_),
        ),
        (
            (y_, Qa_), (an_, F1b_, 1), (act_, c3_), (an_, Qa_, 0),
            (af2_, F1b_, 0),
        ),
    ),
    (
        U2a_,
        (
            (o1_, F2a_), (actw_, c3_),
        ),
        (
            (af1_, F1b_, 0), (af1_, F1b_, 1), (actw_, c3_),
        ),
    ),
    (
        F1b_,
        (
            (rsend_, f2a_), (y_, F2b_),
        ),
        (
            (af2_, F1b_, 1), (af1_, Da_, 1), (an_, Da_, 1), (an_, Qa_, 1),
            (o1i_, Qa_), (y_, Db_),
        ),
    ),
    (
        U2b_,
        (),
        (),
    ),
    (
        GAa_,
        (
            (rsend_, f2b_),
        ),
        (
            (af2_, Qa_, 1), (af2_, Da_, 1), (o0o_, Da_), (o1i_, Qb_),
            (an_, Qb_, 1), (o1o_, Qa_), (af2_, Da_, 0), (af1_, Da_, 0),
        ),
    ),
    (
        PRa_,
        (),
        (
            (af1_, Qa_, 0), (af2_, Qa_, 0), (an_, Db_, 0), (an_, Qb_, 0),
            (y_, F2b_), (af1_, Qa_, 1), (an_, Db_, 1), (y_, F2a_),
            (o1i_, Db_),
        ),
    ),
    (
        ATa0_,
        (),
        (),
    ),
    (
        ATa1_,
        (
            (o1_, F2b_),
        ),
        (
            (o0i_, F2b_), (rn_, f2a_, 3, 0), (o0i_, F2a_),
        ),
    ),
    (
        UQa_,
        (),
        (
            (o0o_, Qa_), (af2_, Db_, 0), (o1o_, Qb_),
        ),
    ),
    (
        GAb_,
        (
            (rsend_, qda_),
        ),
        (
            (af2_, Db_, 1), (af1_, Db_, 0), (af1_, Db_, 1), (af1_, Qb_, 1),
            (af2_, Qb_, 1), (rn_, f2a_, 3, 1), (o1o_, Db_),
        ),
    ),
    (
        PRb_,
        (),
        (
            (o0o_, Db_), (o1i_, F2a_), (af2_, Qb_, 0), (af1_, Qb_, 0),
        ),
    ),
    (
        ATb0_,
        (),
        (
            (an_, F2a_, 0),
        ),
    ),
    (
        ATb1_,
        (),
        (),
    ),
    (
        UQb_,
        (),
        (),
    ),
    (
        HGa_,
        (
            (rsend_, qdb_), (fin_, f2a_, 0), (fin_, f2a_, 1), (fr_, a_),
            (fw_, a_),
        ),
        (
            (rf_, f2a_, 1), (rn_, f2a_, 2, 0), (rf_, f2a_, 0), (af1_, F2a_, 0),
            (an_, F2a_, 1), (rn_, f2a_, 2, 1), (af2_, F2a_, 0), (af1_, F2a_, 1),
            (af2_, F2a_, 1), (fin_, f2a_, 0), (o1o_, F2a_), (rn_, f2b_, 2, 0),
            (o1i_, F2b_),
        ),
    ),
    (
        U1a_,
        (),
        (
            (an_, F2b_, 1), (rn_, f2b_, 3, 0), (fin_, f2a_, 1), (fr_, a_),
            (af1_, F2b_, 0), (o1o_, F2b_),
        ),
    ),
    (
        HGb_,
        (
            (rsend_, f1a_),
        ),
        (
            (o0o_, F2b_), (rn_, qda_, 2, 0), (rn_, qda_, 2, 1), (an_, F2b_, 0),
            (rn_, qda_, 3, 0), (af2_, F2b_, 0), (af2_, F2b_, 1), (rn_, f2b_, 2, 1),
            (fw_, a_), (af1_, F2b_, 1),
        ),
    ),
    (
        OUT_,
        (
            (fin_, f2b_, 0),
        ),
        (),
    ),
    (
        U1b_,
        (
            (fin_, f2b_, 1), (fr_, b_), (fw_, b_), (act_, u1_),
            (fin_, qdb_, 0),
        ),
        (
            (act_, u1_), (rn_, qdb_, 3, 0), (fin_, qda_, 0), (fin_, f2b_, 0),
            (act_, uA2_), (rn_, qda_, 3, 1), (rn_, f2b_, 3, 1), (rn_, qdb_, 2, 0),
            (rf_, f2b_, 0), (rn_, qdb_, 2, 1), (act_, uB2_), (act_, uA3_),
            (rn_, qdb_, 3, 1), (rf_, f2b_, 1), (fin_, f2b_, 1), (rn_, f1a_, 3, 0),
            (rf_, qdb_, 0), (rn_, f1a_, 3, 1), (rf_, qda_, 0), (fr_, b_),
        ),
    ),
    (
        NORM_,
        (
            (rsend_, f1b_), (act_, uA2_), (act_, uB2_),
        ),
        (),
    ),
    (
        NS_,
        (
            (act_, n1_), (fin_, qda_, 0), (fin_, qdb_, 1), (act_, uA3_),
            (act_, uB3_), (act_, nA2_), (act_, nB2_), (fin_, f1a_, 0),
            (act_, nA3_), (finw_, f2a_), (act_, nB3_), (fin_, qda_, 1),
            (finw_, qdb_), (fin_, f1b_, 0), (actw_, n_),
        ),
        (
            (rn_, f1a_, 2, 0), (fw_, b_), (act_, n1_), (rf_, qdb_, 1),
            (act_, nA2_), (finw_, f2b_), (act_, nB2_), (rn_, f1a_, 2, 1),
            (act_, uB3_), (rf_, f1a_, 1), (rf_, f1a_, 0), (fin_, f1a_, 1),
            (rf_, qda_, 1), (fin_, qda_, 1), (rn_, f1b_, 3, 1), (fin_, f1a_, 0),
            (rn_, f1b_, 3, 0), (act_, nA3_), (rn_, f1b_, 2, 0), (finw_, f1a_),
            (act_, nB3_), (actw_, n_),
        ),
    ),
    (
        WI_,
        (
            (act_, st_), (actw_, st_), (fin_, f1a_, 1),
        ),
        (
            (rf_, f1b_, 0), (fin_, qdb_, 1), (fin_, qdb_, 0), (rn_, f1b_, 2, 1),
            (act_, st_), (actw_, st_), (fin_, f1b_, 0), (actw_, u_),
        ),
    ),
    (
        WB_,
        (
            (actw_, u_),
        ),
        (
            (rf_, f1b_, 1),
        ),
    ),
    (
        END_,
        (
            (finw_, f1a_), (finw_, qda_), (fin_, f1b_, 1), (finw_, f2b_),
            (finw_, f1b_),
        ),
        (
            (fin_, f1b_, 1), (finw_, f1b_), (finw_, qdb_), (finw_, f2a_),
            (finw_, qda_),
        ),
    ),
)


def fdot(a, b, dims=contract_in):
    return lax.dot_general(a, b, dims, preferred_element_type=f32)


def tiles(total, size, step):
    if total == size:
        step(0)
    else:
        pl.loop(0, total // size)(lambda i: step(pl.multiple_of(i * size, size)))


def bits_of(count):
    return [1 << i for i in range(count.bit_length() - 1)]


def halving_slots(C, T):
    return max(C * (T // 2 - 1) + C - 1, (T // 2) * (C - 1) + T // 2 - 1)


def block_kernel(dims, *refs):
    Z, C, T, r, fw, hw, lw, piece = dims
    (
        hid_hbm, cot_hbm, fc1w, qkvw, densew, fc2w, gain, bias, fc1b, qkvb, dense_b, fc2_b, segs, freqs,
        r_block, r_input, g_fc1, g_qd, g_fc2, r_fc1b, r_qkvb, r_outb, r_gain, r_bias,
        X, COT, W1, WQ, WD, W2, ACT, DG, TT, QV, GA, ATT, MI, COS, SIN, hid, cot_in,
        G2, R2, GQ, RQ, RT, RC, SM, SMR, ST, STR, qs, ks, dq, dk, dv,
        block_out, grad_input, o_fc1b, o_qkvb, o_outb, o_gain, o_bias,
        y_s, y_r, own_s, ag_s, ag_r, rs_s, rs_r, fin_s, fin_r, out_s,
        aa_s, aa_r, ar_s, ar_r, sm_s, sm_r, st_s, st_r, res_s, free,
    ) = refs
    L, D, U, last = piece * C, T * lw, Z * C, Z - 1
    fh, gw = fw // 2, min(hw, 128)
    groups, in_group, aligned = hw // gw, gw // HD, gw % 128 == 0
    z, c, t = lax.axis_index("dp"), lax.axis_index("ctx"), lax.axis_index("tensor")
    end_side, mid_side = z // last, z - 1
    end_in, mid_in, mid_out = z + 1 - 2 * end_side, last - z, last * mid_side
    is_end, is_mid = (z == 0) | (z == last), (z > 0) & (z < last)

    def remote(src, dst, send, recv, **where):
        return pltpu.make_async_remote_copy(
            src_ref=src, dst_ref=dst, send_sem=send, recv_sem=recv,
            device_id=where, device_id_type=MESH,
        )

    def exists(name):
        return groups == 2 or name[:2] not in ("Qb", "Db") and name != "qdb"

    def sub_offsets(own):
        return [0] if own else list(range(1, C))

    def weight(p, u, count=1):
        half = "ab".index(p[-1])
        units = u if count == 1 else pl.ds(u, count)
        rows = pl.ds(pl.multiple_of(u * r, r), count * r)
        if p[:2] == "F1":
            return W1.at[rows, half * fh : (half + 1) * fh]
        if p[0] == "Q":
            return WQ.at[half, :, rows]
        if p[0] == "D":
            return WD.at[units, half * gw : (half + 1) * gw]
        return W2.at[units, half * fh : (half + 1) * fh]

    def shard(p, k):
        half = "ab".index(p[-1])
        if p[:2] == "F1":
            return fc1w.at[:, pl.ds(pl.multiple_of(k * fw + half * fh, fh), fh)]
        if p[0] == "Q":
            if not aligned:
                return qkvw.at[k, half]
            return qkvw.at[:, :, pl.ds(pl.multiple_of(k * hw + half * gw, gw), gw)]
        if p[0] == "D":
            return densew.at[k, half * gw : (half + 1) * gw]
        return fc2w.at[k, half * fh : (half + 1) * fh]

    def y_copy(p, o):
        i, k = WEIGHTS.index(p), (c + o) % C
        return remote(shard(p, k), weight(p, z * C + c), y_s.at[i, o - 1], y_r.at[i, o - 1], ctx=k)

    def own_copy(p):
        i = WEIGHTS.index(p)
        return pltpu.make_async_copy(shard(p, c), weight(p, z * C + c), own_s.at[i])

    def ag_copy(p, u, way, to, src=None):
        i = WEIGHTS.index(p)
        src = weight(p, u) if src is None else src
        return remote(src, weight(p, u), ag_s.at[i, way], ag_r.at[i, u], dp=to)

    def ag_wait(p, u):
        ag_copy(p, u, 0, end_in).wait_recv()

    def y_start(p):
        for o in range(1, C):
            y_copy(p, o).start()
        own_copy(p).start()

    def send_own(p, second, way, to):
        if not second:
            ag_copy(p, z * C + c, way, to, shard(p, c)).start()
        for o in range(1, C) if second else ():
            ag_copy(p, z * C + (c - o) % C, way, to).start()

    def y_wait(p):
        for o in range(1, C):
            i, u, k = WEIGHTS.index(p), z * C + (c - o) % C, (c + o) % C
            remote(shard(p, k), weight(p, u), y_s.at[i, o - 1], y_r.at[i, o - 1], ctx=k).wait_recv()

    def forward(p, chunk, sub, way, to):
        for o in sub_offsets(sub == 0):
            u = chunk * C + (c - o) % C
            ag_wait(p, u)
            ag_copy(p, u, way, to).start()

    def weights_end(p):
        i = WEIGHTS.index(p)
        for o in range(1, C):
            y_copy(p, o).wait_send()

        def sent(way, chunk, chunks):
            region = weight(p, chunk * C, chunks * C)
            remote(region, region, ag_s.at[i, way], ag_r.at[i, 0], dp=mid_in).wait_send()

        pl.when(is_end)(lambda: sent(0, z, 1))

        @pl.when(is_mid)
        def _():
            sent(0, 2 * mid_side, 2)
            sent(1, 1 - mid_side, 3)

    def doubling(index, array, own, part, order):
        rows_half = piece // 2
        masks, blocks, at, plan = [0], 1, 0, []
        for axis, bit in order:
            plan.append((axis, bit, blocks, tuple(masks), at))
            at += len(masks) * blocks
            if axis == "c":
                blocks *= 2
            else:
                masks = masks + [m ^ bit for m in masks]

        def copies(stage):
            axis, bit, count, sent, first = plan[stage]
            where = {"ctx": c ^ bit} if axis == "c" else {"tensor": t ^ bit}
            found = []
            for b in range(count):
                start = ((c // count) * count + b) * piece + part * rows_half
                for j, m in enumerate(sent):
                    dst = array.at[
                        pl.ds(pl.multiple_of(start, rows_half), rows_half),
                        pl.ds(pl.multiple_of((t ^ m) * lw, lw), lw),
                    ]
                    src = own.at[part * rows_half : (part + 1) * rows_half] if stage == 0 else dst
                    sem = first + b * len(sent) + j
                    found.append(remote(src, dst, aa_s.at[index, sem], aa_r.at[index, sem], **where))
            return found

        def begin(stage):
            for copy in copies(stage):
                copy.start()

        def arrive(stage):
            for copy in copies(stage):
                copy.wait_recv()

        def end():
            for stage in range(len(plan)):
                for copy in copies(stage):
                    copy.wait_send()

        return begin, arrive, end

    cbits = [("c", b) for b in bits_of(C)]
    tbits = [("t", b) for b in reversed(bits_of(T))]
    routes = (cbits + tbits, tbits[:-1] + cbits + tbits[-1:])
    doubles = {
        name + "AB"[part]: doubling(2 * i + part, array, own, part, routes[part])
        for i, (name, array, own) in enumerate((("h", X, hid_hbm), ("c", COT, cot_hbm)))
        for part in range(2)
    }
    doubling_stages = len(cbits) + len(tbits)

    def place(array, own, sem):
        return pltpu.make_async_copy(
            own,
            array.at[
                pl.ds(pl.multiple_of(c * piece, piece), piece), pl.ds(pl.multiple_of(t * lw, lw), lw)
            ],
            sem,
        )

    def load(i):
        return pltpu.make_async_copy((hid_hbm, cot_hbm)[i], (hid, cot_in)[i], own_s.at[10 + i])

    def double(name, step):
        if step == "3":
            for part in "AB":
                begin, arrive, _ = doubles[name + part]
                arrive(doubling_stages - 2)
                begin(doubling_stages - 1)
        else:
            begin, arrive, _ = doubles[name]
            stages = [0] if step == "1" else range(1, doubling_stages - 1)
            for stage in stages:
                if stage:
                    arrive(stage - 1)
                begin(stage)

    def double_wait(name):
        for part in "AB":
            doubles[name + part][1](doubling_stages - 1)

    def double_end(name):
        for part in "AB":
            doubles[name + part][2]()

    def grad_rows(q):
        return 4 * gw if q[0] == "q" else fh

    def grad_at(q, u, row, size, slots=False):
        half = "ab".index(q[-1])
        if q[0] == "q":
            return (RQ if slots else GQ).at[half, u, pl.ds(row, size)]
        return (R2 if slots else G2).at[u, pl.ds(half * fh + row, size)]

    def whole_at(q, u, slots=False):
        return grad_at(q, u, 0, grad_rows(q), slots)

    def grad_out(q):
        half = "ab".index(q[-1])
        if q[0] == "q":
            return g_qd.at[c, half]
        return (g_fc2 if q[1] == "2" else g_fc1).at[c, half * fh : (half + 1) * fh]

    def rs_copy(q, u, slot, way, number, to):
        i = GRADS.index(q)
        return remote(
            whole_at(q, u), whole_at(q, slot, True), rs_s.at[i, way],
            rs_r.at[i, number * C + u % C], dp=to,
        )

    def rs_add(q, u, slots):
        size = min(128, grad_rows(q))

        def add(row):
            ref = grad_at(q, u, row, size)
            total = ref[...].astype(f32)
            for slot in slots:
                total = total + grad_at(q, slot, row, size, True)[...].astype(f32)
            ref[...] = total.astype(bf16)

        tiles(grad_rows(q), size, add)

    def rs_send(q):
        for k in range(last):
            d = end_side * k + (1 - end_side) * (last - k)
            for own in (False, True):
                for o in sub_offsets(own):
                    u = d * C + (c + o) % C
                    rs_copy(q, u, u + C * (1 - end_side), 0, k, end_in).start()

    def rs_near(q, dist, sub):
        d = last * (1 - mid_side) if dist == last else last - z
        for o in sub_offsets(sub == 1):
            u = d * C + (c + o) % C
            slot = u + C * (1 - mid_side)
            near = 0 if dist == last else 1
            rs_copy(q, u, slot, 0, near, mid_in).wait_recv()
            rs_add(q, u, [slot])
            rs_copy(q, u, slot, 0, last + near, mid_in).start()

    def rs_far(q, sub):
        for o in sub_offsets(sub == 1):
            u = last * mid_side * C + (c + o) % C
            slot = u + C * mid_side
            rs_copy(q, u, slot, 1, last, mid_out).wait_recv()
            rs_add(q, u, [slot])
            rs_copy(q, u, slot, 1, last, mid_out).start()

    def fin_copy(q, o):
        i, k = GRADS.index(q), (c + o) % C
        return remote(whole_at(q, z * C + k), grad_out(q), fin_s.at[i, o - 1], fin_r.at[i, o - 1], ctx=k)

    def fin_own(q):
        return pltpu.make_async_copy(
            whole_at(q, z * C + c), grad_out(q), out_s.at[GRADS.index(q)]
        )

    def finish(q, sub, at_end):
        for o in sub_offsets(sub == 1):
            u = z * C + (c + o) % C
            if at_end:
                slots = [u + C * end_side]
                rs_copy(q, u, slots[0], 1, last, end_in).wait_recv()
            else:
                slots = [u + C * (1 - mid_side), u + C * mid_side]
                for slot, number in zip(slots, (last - 1, last + 1)):
                    rs_copy(q, u, slot, 0, number, mid_in).wait_recv()
            rs_add(q, u, slots)
            if o:
                fin_copy(q, o).start()
            else:
                fin_own(q).start()

    def grads_sent(q):
        i, half = GRADS.index(q), "ab".index(q[-1])

        def sent(way, chunk, chunks):
            units = pl.ds(chunk * C, chunks * C)
            if q[0] == "q":
                region = GQ.at[half, units]
            else:
                region = G2.at[units, half * fh : (half + 1) * fh]
            remote(region, region, rs_s.at[i, way], rs_r.at[i, 0], dp=mid_in).wait_send()

        pl.when(is_end)(lambda: sent(0, 1 - end_side, last))

        @pl.when(is_mid)
        def _():
            sent(0, 2 - 2 * mid_side, 2)
            sent(1, last * mid_side, 1)

        for o in range(1, C):
            fin_copy(q, o).wait_send()
        fin_own(q).wait()

    def grads_arrived(q):
        for o in range(1, C):
            fin_copy(q, o).wait_recv()

    def tables():
        lane = lax.broadcasted_iota(jnp.int32, (128, gw), 1) % HD

        def rows_of(row):
            rows = pl.ds(row, 128)
            every = segs[...].astype(f32)
            own = jnp.broadcast_to(segs[:, rows].astype(f32), (128, 128)).T[:, 0:1]
            start = jnp.sum((every < own).astype(f32), axis=1, keepdims=True)
            at = (lax.broadcasted_iota(jnp.int32, (128, 1), 0) + row).astype(f32)
            angle = (at - start) * freqs[...]
            MI[rows, 2:3] = start
            COS[rows] = jnp.cos(angle)
            sine = jnp.sin(angle)
            SIN[rows] = jnp.where(lane < ROT // 2, -sine, sine)

        tiles(L, 128, rows_of)
        SM[...] = jnp.zeros_like(SM)
        for i in range(2):
            load(i).wait()
        SM[2:3, :lw] = jnp.sum(cot_in[...].astype(f32), axis=0, keepdims=True)

    def layer_norm():
        double_end("h")

        def rows_of(row):
            rows = pl.ds(row, 128)
            x = X[rows].astype(f32)
            mean = jnp.mean(x, axis=1, keepdims=True)
            centered = x - mean
            inv = lax.rsqrt(jnp.mean(centered * centered, axis=1, keepdims=True) + ln_eps)
            MI[rows, 0:1] = mean
            MI[rows, 1:2] = inv
            X[rows] = (centered * inv * gain[...] + bias[...]).astype(bf16)

        tiles(L, 128, rows_of)

    cf = min(BLOCK, fh)
    gelu_c = math.sqrt(2.0 / math.pi)

    def hidden(half):
        def cols_of(col):
            cols = pl.ds(half * fh + col, cf)
            shift = fc1b[:, pl.ds(pl.multiple_of(c * fw + half * fh + col, cf), cf)]

            def rows_of(row):
                rows = pl.ds(row, ROWS)
                v = fdot(X[rows], W1[:, cols]) + shift
                tanh = jnp.tanh(gelu_c * (v + 0.044715 * (v * v * v)))
                act = 0.5 * v * (1.0 + tanh)
                slope = gelu_c * (1.0 + 3.0 * 0.044715 * (v * v))
                DG[rows, cols] = (0.5 * (1.0 + tanh) + 0.5 * v * (1.0 - tanh * tanh) * slope).astype(bf16)
                ACT[rows, cols] = act.astype(bf16)
                TT[cols, rows] = act.T.astype(bf16)

            tiles(L, ROWS, rows_of)

        tiles(fh, cf, cols_of)

    def over_each_unit(step):
        if r % 128 == 0:
            pl.loop(0, U)(lambda u: step(u, pl.ds(pl.multiple_of(u * r, r), r)))
        else:
            for u in range(U):
                step(u, slice(u * r, (u + 1) * r))

    def unit_grads(q):
        half = "ab".index(q[-1])

        def step(u, cols):
            if q[0] == "q":
                first = half * 4 * gw
                GQ[half, u, : 3 * gw] = fdot(TT[first : first + 3 * gw], X[:, cols]).astype(bf16)
                GQ[half, u, 3 * gw :] = fdot(TT[first + 3 * gw : first + 4 * gw], COT[:, cols]).astype(bf16)
            else:
                rows = slice(half * fh, (half + 1) * fh)
                source = COT if q[1] == "2" else X
                G2[u, rows] = fdot(TT[rows], source[:, cols]).astype(bf16)

        over_each_unit(step)

    def side_by_side(rows, group):
        return jnp.concatenate([WQ[group, part, rows] for part in range(3)], axis=1)

    def project(group):
        def shift(part):
            if not aligned:
                return qkvb[part : part + 1]
            return qkvb[part : part + 1, pl.ds(pl.multiple_of(c * hw + group * gw, gw), gw)]

        shifts = jnp.concatenate([shift(part) for part in range(3)], axis=1)

        def rows_of(row):
            rows = pl.ds(row, ROWS)
            QV[group, rows] = (fdot(X[rows], side_by_side(pl.ds(0, D), group)) + shifts).astype(bf16)

        tiles(L, ROWS, rows_of)

    def over_units(rows, weights):
        total = None
        for u in range(U):
            term = fdot(COT[rows, u * r : (u + 1) * r], weights(u), contract_cols)
            total = term if total is None else total + term
        return total

    def attended_grads(group):
        def rows_of(row):
            rows = pl.ds(row, ROWS)
            lanes = slice(group * gw, (group + 1) * gw)
            GA[rows] = over_units(rows, lambda u: WD[u, lanes]).astype(bf16)

        tiles(L, ROWS, rows_of)

    half_rot = ROT // 2
    scale = 1.0 / math.sqrt(HD)

    def turn(values, rows, sign):
        lane = lax.broadcasted_iota(jnp.int32, values.shape, 1) % HD
        other = jnp.where(
            lane < half_rot, pltpu.roll(values, gw - half_rot, 1), pltpu.roll(values, half_rot, 1)
        )
        turned = other * SIN[rows]
        return values * COS[rows] + (turned if sign > 0 else -turned)

    def attention_load(group):
        def load(row):
            rows = pl.ds(row, BLOCK)
            qs[rows] = turn(QV[group, rows, :gw].astype(f32), rows, 1).astype(bf16)
            ks[rows] = turn(QV[group, rows, gw : 2 * gw].astype(f32), rows, 1).astype(bf16)

        tiles(L, BLOCK, load)
        for ref in (dq, dk, dv):
            ref[...] = jnp.zeros_like(ref)
        ATT[:, group * gw : (group + 1) * gw] = jnp.zeros((L, gw), bf16)

    def attention_head(group, head):
        own = slice(group * gw, (group + 1) * gw)
        for row in range(0, L, BLOCK):
            low = max(0, row - DOC_MAX)
            span = row + BLOCK - low
            rows, cols = pl.ds(row, BLOCK), pl.ds(low, span)
            mine = lax.broadcasted_iota(jnp.int32, (BLOCK, gw), 1) // HD == head
            query = jnp.where(mine, qs[rows].astype(f32), 0.0).astype(bf16)
            grad = jnp.where(mine, GA[rows].astype(f32), 0.0)
            grad_b, key, value = grad.astype(bf16), ks[cols], QV[group, cols, 2 * gw :]
            query_pos = row + lax.broadcasted_iota(jnp.int32, (BLOCK, span), 0)
            key_pos = low + lax.broadcasted_iota(jnp.int32, (BLOCK, span), 1)
            allowed = (key_pos >= MI[rows, 2:3].astype(jnp.int32)) & (key_pos <= query_pos)
            scores = jnp.where(allowed, fdot(query, key, contract_cols) * scale, mask_fill)
            weights = jnp.exp(scores - jnp.max(scores, axis=1, keepdims=True))
            probs = weights * (1.0 / jnp.sum(weights, axis=1, keepdims=True))
            probs_b = probs.astype(bf16)
            attended = jnp.where(mine, fdot(probs_b, value), 0.0).astype(bf16)
            delta = jnp.sum(grad * attended.astype(f32), axis=1, keepdims=True)
            grad_probs = fdot(grad_b, value, contract_cols)
            grad_scores = (probs * (grad_probs - delta)).astype(bf16)
            dv[cols] += fdot(probs_b, grad_b, contract_rows)
            dk[cols] += fdot(grad_scores, query, contract_rows)
            dq[rows] += jnp.where(mine, fdot(grad_scores, key), 0.0)
            ATT[rows, own] += attended

    def attention_save(group):
        first = group * 4 * gw

        def save(row):
            rows = pl.ds(row, BLOCK)
            attended = ATT[rows, group * gw : (group + 1) * gw].astype(f32)
            TT[first + 3 * gw : first + 4 * gw, rows] = attended.T.astype(bf16)
            grads = turn(dq[rows] * scale, rows, -1), turn(dk[rows] * scale, rows, -1), dv[rows]
            for part, grad in enumerate(grads):
                lanes = slice(part * gw, (part + 1) * gw)
                QV[group, rows, lanes] = grad.astype(bf16)
                TT[first + part * gw : first + (part + 1) * gw, rows] = grad.T.astype(bf16)
                sums = jnp.sum(grad.astype(bf16).astype(f32), axis=0, keepdims=True)
                SM[5 + group : 6 + group, lanes] += sums

        tiles(L, BLOCK, save)

    def attention_heads(group, second):
        mine = range(in_group // 2, in_group) if second else range(in_group // 2)
        if in_group == 1:
            mine = [] if second else [0]
        if not second:
            attention_load(group)
        for head in mine:
            attention_head(group, head)
        if second:
            attention_save(group)

    def hidden_grads(half):
        for n in range(fh // cf):
            cols = slice(half * fh + n * cf, half * fh + (n + 1) * cf)

            def rows_of(row):
                rows = pl.ds(row, ROWS)
                grad = over_units(rows, lambda u: W2[u, cols]) * DG[rows, cols].astype(f32)
                SM[0:1, cols] += jnp.sum(grad, axis=0, keepdims=True)
                DG[rows, cols] = grad.astype(bf16)
                TT[cols, rows] = grad.T.astype(bf16)

            tiles(L, ROWS, rows_of)

    rows_half = piece // 2

    def halving(a, part):
        first_bit, later_bits = bits_of(T)[0], [("t", b) for b in bits_of(T)[1:]]
        first_kept = [m for m in range(T) if not m & first_bit]
        c_bits = [("c", b) for b in reversed(bits_of(C))]

        def cols_of(m):
            return pl.ds(pl.multiple_of((t ^ m) * lw, lw), lw)

        def rows_at(block, which):
            return pl.ds(pl.multiple_of(block * piece + which * rows_half, rows_half), rows_half)

        def plan_of(order):
            plan, masks, blocks, slot = [], first_kept, C, 0
            for axis, bit in order:
                if axis == "t":
                    masks = [m for m in masks if not m & bit]
                else:
                    blocks = bit
                plan.append((axis, bit, masks, blocks, slot))
                slot += blocks * len(masks)
            return plan

        plans = plan_of(later_bits + c_bits), plan_of(c_bits + later_bits)

        def add(target, source, size):
            def rows_of(row):
                rows = pl.ds(row, 128)
                total = target.at[rows][...].astype(f32) + source.at[rows][...].astype(f32)
                target.at[rows][...] = total.astype(bf16)

            tiles(size, min(128, size), rows_of) if size % 128 == 0 else add_whole(target, source)

        def add_whole(target, source):
            target[...] = (target[...].astype(f32) + source[...].astype(f32)).astype(bf16)

        def first_copies():
            return [
                remote(
                    part.at[:, cols_of(m ^ first_bit)], RT.at[a, j],
                    ar_s.at[a, 0, j], ar_r.at[a, 0, j], tensor=t ^ first_bit,
                )
                for j, m in enumerate(first_kept)
            ]

        def copies(which, stage):
            axis, bit, masks, blocks, slot = plans[which][stage]
            where = {"ctx": c ^ bit} if axis == "c" else {"tensor": t ^ bit}
            start = (c ^ bit) // blocks * blocks if axis == "c" else c // blocks * blocks
            flip = 0 if axis == "c" else bit
            return [
                remote(
                    part.at[rows_at(start + b, which), cols_of(m ^ flip)],
                    RC.at[a, which, slot + b * len(masks) + j],
                    ar_s.at[a, 1 + which, slot + b * len(masks) + j],
                    ar_r.at[a, 1 + which, slot + b * len(masks) + j],
                    **where,
                )
                for b in range(blocks)
                for j, m in enumerate(masks)
            ]

        def arrive(which, stage):
            for copy in copies(which, stage):
                copy.wait_recv()
            axis, bit, masks, blocks, slot = plans[which][stage]
            if stage == len(plans[which]) - 1:
                return
            for b in range(blocks):
                for j, m in enumerate(masks):
                    add(
                        part.at[rows_at(c // blocks * blocks + b, which), cols_of(m)],
                        RC.at[a, which, slot + b * len(masks) + j],
                        rows_half,
                    )

        def begin(which, stage):
            for copy in copies(which, stage):
                copy.start()

        def run(step):
            if step == "1":
                for copy in first_copies():
                    copy.start()
                return
            which = "AB".index(step[0])
            if step[1] == "3":
                for stage in range(1, len(plans[which])):
                    arrive(which, stage - 1)
                    begin(which, stage)
                return
            if which == 0:
                for copy in first_copies():
                    copy.wait_recv()
                for j, m in enumerate(first_kept):
                    add(part.at[:, cols_of(m)], RT.at[a, j], L)
            begin(which, 0)

        def wait():
            for which in range(2):
                arrive(which, len(plans[which]) - 1)

        def total(row, size):
            which, slot = row // rows_half, None
            slot = plans[which][-1][4]
            rows = pl.ds(pl.multiple_of(c * piece + row, size), size)
            received = RC[a, which, slot, row % rows_half : row % rows_half + size]
            return part[rows, cols_of(0)].astype(f32) + received.astype(f32)

        def end():
            for copy in first_copies():
                copy.wait_send()
            for which in range(2):
                for stage in range(len(plans[which])):
                    for copy in copies(which, stage):
                        copy.wait_send()

        return run, wait, total, end

    n_run, n_wait, n_total, n_end = halving(0, X)
    u_run, u_wait, u_total, u_end = halving(1, COT)

    def norm_units():
        def step(u, cols):
            w1 = W1[pl.ds(pl.multiple_of(u * r, r), r)]
            wq = [side_by_side(pl.ds(pl.multiple_of(u * r, r), r), g) for g in range(groups)]

            def rows_of(row):
                rows = pl.ds(row, ROWS)
                total = fdot(DG[rows], w1, contract_cols)
                for g in range(groups):
                    total = total + fdot(QV[g, rows], wq[g], contract_cols)
                X[rows, cols] = total.astype(bf16)

            tiles(L, ROWS, rows_of)

        over_each_unit(step)

    def out_units():
        double_end("c")

        def step(u, cols):
            def rows_of(row):
                rows = pl.ds(row, ROWS)
                COT[rows, cols] = (fdot(ATT[rows], WD[u]) + fdot(ACT[rows], W2[u])).astype(bf16)

            tiles(L, ROWS, rows_of)

        over_each_unit(step)

    size = min(128, rows_half)

    def write_block():
        shift = dense_b[...] + fc2_b[...]
        for row in range(0, piece, size):
            rows = pl.ds(row, size)
            block_out[rows] = (hid[rows].astype(f32) + u_total(row, size) + shift).astype(bf16)
        final(0).start()

    def gain_own():
        return gain[:, pl.ds(pl.multiple_of(t * lw, lw), lw)]

    def standard_of(row):
        rows = pl.ds(pl.multiple_of(c * piece + row, size), size)
        inv = MI[rows, 1:2]
        return (hid[pl.ds(row, size)].astype(f32) - MI[rows, 0:1]) * inv, inv

    def norm_sums():
        for row in range(0, piece, size):
            grad = n_total(row, size)
            standard, _ = standard_of(row)
            scaled = grad * gain_own()
            first = jnp.sum(scaled, axis=1, keepdims=True)
            second = jnp.sum(scaled * standard, axis=1, keepdims=True)
            lane = lax.broadcasted_iota(jnp.int32, (size, 128), 1)
            pair = jnp.where(lane == 0, first, jnp.where(lane == 1, second, 0.0))
            ST[:, row : row + size] = pair.T[0:8]
            SM[3:4, :lw] += jnp.sum(grad * standard, axis=0, keepdims=True)
            SM[4:5, :lw] += jnp.sum(grad, axis=0, keepdims=True)

    def st_copy(o):
        return remote(ST, STR.at[o - 1], st_s.at[o - 1], st_r.at[o - 1], tensor=(t + o) % T)

    def sm_copy(dz, dc):
        o = dz * C + dc - 1
        return remote(
            SM, SMR.at[z * C + c], sm_s.at[o], sm_r.at[o], dp=(z + dz) % Z, ctx=(c + dc) % C
        )

    finals = (
        (block_out, r_block), (grad_input, r_input), (o_fc1b, r_fc1b), (o_qkvb, r_qkvb),
        (o_outb, r_outb), (o_gain, r_gain), (o_bias, r_bias),
    )

    def final(i):
        return pltpu.make_async_copy(*finals[i], res_s.at[i])

    offsets = [(dz, dc) for dz in range(Z) for dc in range(C) if dz or dc]

    def stats_start():
        for o in range(1, T):
            st_copy(o).start()
        for dz, dc in offsets:
            sm_copy(dz, dc).start()

    def stats_wait():
        for o in range(1, T):
            st_copy(o).wait()

    def write_input():
        for row in range(0, piece, size):
            stats = ST[:, row : row + size]
            for o in range(1, T):
                stats = stats + STR[o - 1, :, row : row + size]
            stats = jnp.concatenate([stats, jnp.zeros((120, size), f32)], axis=0).T * (1.0 / D)
            standard, inv = standard_of(row)
            scaled = n_total(row, size) * gain_own()
            rows = pl.ds(row, size)
            grad_input[rows] = cot_in[rows].astype(f32) + inv * (
                scaled - stats[:, 0:1] - standard * stats[:, 1:2]
            )
        final(1).start()

    def small_sums():
        SMR[z * C + c] = SM[...]
        for dz, dc in offsets:
            sm_copy(dz, dc).wait()

        def summed(row, size, units):
            total = SMR[units[0], row : row + 1, :size]
            for u in units[1:]:
                total = total + SMR[u, row : row + 1, :size]
            return total

        for k in range(C):
            units = [zs * C + k for zs in range(Z)]
            o_fc1b[:, k * fw : (k + 1) * fw] = summed(0, fw, units)
            for g in range(groups):
                sums = summed(5 + g, 3 * gw, units)
                for part in range(3):
                    lanes = slice(k * hw + g * gw, k * hw + (g + 1) * gw)
                    o_qkvb[part : part + 1, lanes] = sums[:, part * gw : (part + 1) * gw]
        for i, out in enumerate((o_outb, o_gain, o_bias)):
            out[...] = summed(2 + i, lw, list(range(U)))
        for i in range(2, len(finals)):
            final(i).start()

    computes = {"TAB": tables, "LN": layer_norm, "NORM": norm_units, "OUT": out_units}
    computes.update({"NS": norm_sums, "WI": write_input, "WB": write_block})
    for i, half in enumerate("ab"):
        computes["F1" + half] = partial(hidden, i)
        computes["U2" + half] = partial(unit_grads, "f2" + half)
        computes["U1" + half] = partial(unit_grads, "f1" + half)
        computes["HG" + half] = partial(hidden_grads, i)
        if i < groups:
            computes["PR" + half] = partial(project, i)
            computes["GA" + half] = partial(attended_grads, i)
            computes["AT" + half + "0"] = partial(attention_heads, i, False)
            computes["AT" + half + "1"] = partial(attention_heads, i, True)
            computes["UQ" + half] = partial(unit_grads, "qd" + half)

    def action(kind, name, *rest, at_end):
        if kind == "act" or kind == "actw":
            if name == "st":
                (stats_start if kind == "act" else stats_wait)()
            elif name[0] in "hc":
                if kind == "actw":
                    double_wait(name[0])
                elif name[1:] == "3":
                    double(name[0], "3")
                else:
                    double(name[:2], name[2])
            elif kind == "actw":
                (n_wait if name[0] == "n" else u_wait)()
            else:
                (n_run if name[0] == "n" else u_run)(name[1:])
        elif kind == "fr":
            grads_sent("f2" + name)
            half = "ab".index(name)

            def tell(to, way):
                pl.semaphore_signal(free.at[half, way], 1, device_id={"dp": to}, device_id_type=MESH)

            if at_end:
                tell(end_in, 0)
            else:
                tell(mid_in, 1)
                tell(mid_out, 1)
        elif kind == "fw":
            half = "ab".index(name)
            if not at_end:
                pl.semaphore_wait(free.at[half, 0], 1)
            pl.semaphore_wait(free.at[half, 1], 1)
        elif not exists(name):
            return
        elif kind == "y":
            y_start(name)
        elif kind == "o0":
            send_own(name, False, 0, end_in)
        elif kind == "o1":
            y_wait(name)
            send_own(name, True, 0, end_in)
        elif kind in ("o0i", "o0o", "o1i", "o1o"):
            if kind[1] == "1" and (name, "seen") not in seen:
                y_wait(name)
                seen.add((name, "seen"))
            way = "io".index(kind[2])
            send_own(name, kind[1] == "1", way, (mid_in, mid_out)[way])
        elif kind == "an":
            forward(name, mid_out, rest[0], 0, mid_in)
        elif kind == "af1":
            forward(name, mid_in, rest[0], 1, mid_out)
        elif kind == "af2":
            forward(name, last - mid_out, rest[0], 1, mid_out)
        elif kind == "rsend":
            rs_send(name)
        elif kind == "rn":
            rs_near(name, *rest)
        elif kind == "rf":
            rs_far(name, *rest)
        elif kind == "fin":
            finish(name, rest[0], at_end)

    seen = set()

    barrier = pltpu.get_barrier_semaphore()

    def greet(**where):
        pl.semaphore_signal(barrier, 1, device_id=where, device_id_type=MESH)

    @pl.when(is_end)
    def _():
        greet(dp=end_in)

    @pl.when(is_mid)
    def _():
        greet(dp=mid_in)
        greet(dp=mid_out)

    for o in range(1, C):
        greet(ctx=(c + o) % C)
    for o in range(1, T):
        greet(tensor=(t + o) % T)
    pl.when(is_end)(lambda: pl.semaphore_wait(barrier, C + T - 1))
    pl.when(is_mid)(lambda: pl.semaphore_wait(barrier, C + T))
    owns = (X, hid_hbm), (COT, cot_hbm)
    for i, (array, own) in enumerate(owns):
        place(array, own, own_s.at[8 + i]).start()
        load(i).start()
    for i, (array, own) in enumerate(owns):
        place(array, own, own_s.at[8 + i]).wait()

    for name, at_ends, inside in SCHEDULE:

        @pl.when(is_end)
        def _():
            for step in at_ends:
                action(*step, at_end=True)

        @pl.when(is_mid)
        def _():
            for step in inside:
                action(*step, at_end=False)

        if name not in computes:
            continue
        needed = NEEDS.get(name)
        if needed is not None:

            @pl.when(is_end)
            def _():
                for dz in range(1, Z):
                    for cs in range(C):
                        ag_wait(needed, ((z + dz) % Z) * C + cs)

            own_copy(needed).wait()
        computes[name]()

    small_sums()
    for q in GRADS:
        if exists(q):
            grads_arrived(q)
    n_end()
    u_end()
    for p in WEIGHTS:
        if exists(p):
            weights_end(p)
    for q in GRADS[2:]:
        if exists(q):
            grads_sent(q)
    for i in range(len(finals)):
        final(i).wait()


def body(
    hidden_in,
    segments,
    ln_gain,
    ln_bias,
    qkv_weight,
    qkv_bias,
    dense_weight,
    dense_bias,
    fc1_weight,
    fc1_bias,
    fc2_weight,
    fc2_bias,
    cotangent,
):
    _, piece, lw = hidden_in.shape
    C, T, Z = lax.axis_size("ctx"), lax.axis_size("tensor"), lax.axis_size("dp")
    L, D, U = piece * C, lw * T, Z * C
    r = qkv_weight.shape[0]
    hw, fw = lw // C, fc1_weight.shape[1] // C
    gw = min(hw, 128)
    groups, aligned = hw // gw, gw % 128 == 0
    lane = np.arange(gw) % HD
    freqs = rope_base ** (-((lane % (ROT // 2)) * 2.0) / ROT)
    freqs = jnp.asarray(np.where(lane < ROT, freqs, 0.0)[None], f32)
    if aligned:
        qkvw, own_bias = qkv_weight.transpose(1, 0, 2), qkv_bias
    else:
        qkvw = qkv_weight.reshape(r, 3, C, groups, gw).transpose(2, 3, 1, 0, 4)
        own_bias = lax.dynamic_slice_in_dim(qkv_bias, lax.axis_index("ctx") * hw, hw, 1)
    operands = [
        hidden_in[0],
        cotangent[0],
        fc1_weight,
        qkvw,
        dense_weight.reshape(C, hw, r),
        fc2_weight.reshape(C, fw, r),
        ln_gain[None],
        ln_bias[None],
        fc1_bias[None],
        own_bias,
        dense_bias[None],
        fc2_bias[None],
        segments,
        freqs,
    ]
    vmem, anywhere = pl.BlockSpec(memory_space=pltpu.VMEM), pl.BlockSpec(memory_space=pl.ANY)
    in_specs = [anywhere] * 6 + [vmem] * 8

    def out(shape, dtype=f32):
        return jax.ShapeDtypeStruct(shape, dtype)

    outs = [
        out((piece, lw), bf16),
        out((piece, lw)),
        out((C, fw, r), bf16),
        out((C, groups, 4 * gw, r), bf16),
        out((C, fw, r), bf16),
        out((1, C * fw)),
        out((3, lw)),
        out((1, lw)),
        out((1, lw)),
        out((1, lw)),
    ]
    out_specs = [anywhere] * 10
    most = max(fw, 3 * gw, lw)
    V = pltpu.VMEM
    dma = pltpu.SemaphoreType.DMA
    blocks, slots = C * T, max(halving_slots(C, T), T // 2)
    scratch = [
        V((L, D), bf16), V((L, D), bf16),
        V((D, fw), bf16), V((groups, 3, D, gw), bf16), V((U, hw, r), bf16), V((U, fw, r), bf16),
        V((L, fw), bf16), V((L, fw), bf16), V((max(fw, 4 * hw), L), bf16),
        V((groups, L, 3 * gw), bf16), V((L, gw), bf16), V((L, hw), bf16), V((L, 4), f32),
        V((L, gw), f32), V((L, gw), f32), V((piece, lw), bf16), V((piece, lw), bf16),
        V((U, fw, r), bf16), V((U + C, fw, r), bf16),
        V((groups, U, 4 * gw, r), bf16), V((groups, U + C, 4 * gw, r), bf16),
        V((2, T // 2, L, lw), bf16), V((2, 2, halving_slots(C, T), piece // 2, lw), bf16),
        V((8, most), f32), V((U, 8, most), f32), V((8, piece), f32), V((T - 1, 8, piece), f32),
        *[V((L, gw), bf16)] * 2, *[V((L, gw), f32)] * 3,
        *[V(o.shape, o.dtype) for o in outs[:2] + outs[5:]],
        dma((8, C - 1)), dma((8, C - 1)), dma((12,)), dma((8, 2)), dma((8, U)),
        dma((6, 2)), dma((6, 5 * C)), dma((6, C - 1)), dma((6, C - 1)), dma((6,)),
        dma((4, blocks)), dma((4, blocks)), dma((2, 3, slots)), dma((2, 3, slots)),
        dma((U - 1,)), dma((U - 1,)), dma((T - 1,)), dma((T - 1,)), dma((7,)),
        pltpu.SemaphoreType.REGULAR((2, 2)),
    ]
    results = pl.pallas_call(
        partial(block_kernel, (Z, C, T, r, fw, hw, lw, piece)),
        in_specs=in_specs,
        out_specs=out_specs,
        out_shape=outs,
        scratch_shapes=scratch,
        compiler_params=pltpu.CompilerParams(
            collective_id=0, has_side_effects=True, vmem_limit_bytes=67043328
        ),
        name="transformer_block",
    )(*operands)
    block_out, grad_input, g_fc1, g_qd, g_fc2, *sums = results
    if aligned and r % 128 == 0:
        block_out, grad_input, grad_fc1, grad_qkv, grad_dense, grad_fc2, *sums = unpack(results)
        grad_qkv = grad_qkv.transpose(1, 0, 2)
    else:
        sums.append(sums[2])
        grad_fc1 = g_fc1.astype(f32).transpose(2, 0, 1).reshape(r, C * fw)
        grad_qkv = g_qd[:, :, : 3 * gw].astype(f32).reshape(C, groups, 3, gw, r)
        grad_qkv = grad_qkv.transpose(4, 2, 0, 1, 3).reshape(r, 3, lw)
        grad_dense = g_qd[:, :, 3 * gw :].astype(f32).reshape(lw, r)
        grad_fc2 = g_fc2.astype(f32).reshape(C * fw, r)
    return (
        block_out[None],
        grad_input[None],
        grad_qkv,
        sums[1],
        grad_dense,
        sums[2][0],
        grad_fc1,
        sums[0][0],
        grad_fc2,
        sums[5][0],
        sums[3][0],
        sums[4][0],
    )


def unpack_kernel(gw, count, *refs):
    ins, outs, refs = refs[:count], refs[count : 2 * count + 2], refs[2 * count + 2 :]
    held, made, in_sem, out_sem = refs[:count], refs[count:-2], refs[-2], refs[-1]
    order = [4, 3, 2, 1, 0, *range(5, count)]
    reads = [pltpu.make_async_copy(ins[i], held[i], in_sem.at[i]) for i in range(count)]
    for i in order:
        reads[i].start()
    writes = []

    def write(src, out):
        copy = pltpu.make_async_copy(src, outs[out], out_sem.at[out])
        copy.start()
        writes.append(copy)

    blocks, quad = held[3].shape[:2]
    fc1, dense, qkv, fc2 = made
    for i in order:
        reads[i].wait()
        if i == 4:
            fc2[...] = held[4][...].astype(f32)
            write(fc2, 5)
        elif i == 3:
            for b in range(blocks):
                dense[b * gw : (b + 1) * gw] = held[3][b, 3 * gw :].astype(f32)
                for part in range(3):
                    source = held[3][b, part * gw : (part + 1) * gw].astype(f32)
                    qkv[part, :, b * gw : (b + 1) * gw] = source.T
            write(dense, 4)
            write(qkv, 3)
        elif i == 2:
            fc1[...] = held[2][...].astype(f32).T
            write(fc1, 2)
        elif i < 2:
            write(held[i], i)
        else:
            write(held[i], i + 1)
            if i == 7:
                write(held[i], count + 1)
    for copy in writes:
        copy.wait()


def unpack(results):
    block_out, grad_input, g_fc1, g_qd, g_fc2, *sums = results
    (piece, lw), (C, fw, r), (_, groups, quad, _) = block_out.shape, g_fc1.shape, g_qd.shape
    gw = quad // 4
    operands = [
        block_out, grad_input, g_fc1.reshape(C * fw, r), g_qd.reshape(C * groups, quad, r),
        g_fc2.reshape(C * fw, r), *sums,
    ]
    shapes = (r, C * fw), (3, r, lw), (lw, r), (C * fw, r)
    made = shapes[0], shapes[2], shapes[1], shapes[3]
    outs = [jax.ShapeDtypeStruct(a.shape, a.dtype) for a in operands[:2]]
    outs += [jax.ShapeDtypeStruct(s, f32) for s in (*shapes, *[s.shape for s in sums], sums[2].shape)]
    dma, count = pltpu.SemaphoreType.DMA, len(operands)
    anywhere = pl.BlockSpec(memory_space=pl.ANY)
    return pl.pallas_call(
        partial(unpack_kernel, gw, count),
        in_specs=[anywhere] * count,
        out_specs=[anywhere] * len(outs),
        out_shape=outs,
        scratch_shapes=[
            *[pltpu.VMEM(a.shape, a.dtype) for a in operands],
            *[pltpu.VMEM(s, f32) for s in made],
            dma((count,)), dma((len(outs),)),
        ],
        name="unpack_results",
    )(*operands)


def solution(mesh):
    in_specs = (
        P("dp", "ctx", "tensor"),
        P("dp", None),
        P(),
        P(),
        P(("dp", "ctx"), None, "tensor"),
        P(None, "tensor"),
        P("tensor", ("dp", "ctx")),
        P("tensor"),
        P(("dp", "ctx"), "tensor"),
        P("tensor"),
        P("tensor", ("dp", "ctx")),
        P("tensor"),
        P("dp", "ctx", "tensor"),
    )
    out_specs = (
        P("dp", "ctx", "tensor"),
        P("dp", "ctx", "tensor"),
        P(("dp", "ctx"), None, "tensor"),
        P(None, "tensor"),
        P("tensor", ("dp", "ctx")),
        P("tensor"),
        P(("dp", "ctx"), "tensor"),
        P("tensor"),
        P("tensor", ("dp", "ctx")),
        P("tensor"),
        P("tensor"),
        P("tensor"),
    )
    return jax.shard_map(body, mesh=mesh, in_specs=in_specs, out_specs=out_specs, check_vma=False)
```

```python
from functools import partial
import math

import jax
import jax.numpy as jnp
import numpy as np
from jax import lax
from jax.experimental import pallas as pl
from jax.experimental.pallas import tpu as pltpu
from jax.sharding import PartitionSpec as P

HD = 64
ROT = 32
DOC_MAX = 512
BLOCK = 256
ROWS = 512

ln_eps = 1e-05
rope_base = 10000.0
mask_fill = -1e30
contract_rows = (((0,), (0,)), ((), ()))
contract_cols = (((1,), (1,)), ((), ()))
contract_in = (((1,), (0,)), ((), ()))
f32, bf16 = jnp.float32, jnp.bfloat16
MESH = pl.DeviceIdType.MESH

WEIGHTS = ("F1a", "F1b", "Qa", "Qb", "Da", "Db", "F2a", "F2b")
GRADS = ("f2a", "f2b", "qda", "qdb", "f1a", "f1b")
NEEDS = {
    "F1a": "F1a", "F1b": "F1b", "PRa": "Qa", "PRb": "Qb",
    "GAa": "Da", "GAb": "Db", "HGa": "F2a", "HGb": "F2b",
}
ATa0_, ATa1_, ATb0_, ATb1_, C_, Da_, Db_, END_ = "ATa0", "ATa1", "ATb0", "ATb1", "C", "Da", "Db", "END"
F1a_, F1b_, F2a_, F2b_, GAa_, GAb_, HGa_, HGb_ = "F1a", "F1b", "F2a", "F2b", "GAa", "GAb", "HGa", "HGb"
LN_, NORM_, NS_, OUT_, PRa_, PRb_, Qa_, Qb_ = "LN", "NORM", "NS", "OUT", "PRa", "PRb", "Qa", "Qb"
TAB_, U1a_, U1b_, U2a_, U2b_, UQa_, UQb_, WB_ = "TAB", "U1a", "U1b", "U2a", "U2b", "UQa", "UQb", "WB"
WI_, a_, act_, actw_, af1_, af2_, an_, b_ = "WI", "a", "act", "actw", "af1", "af2", "an", "b"
c3_, cA1_, cA2_, cB1_, cB2_, f1a_, f1b_, f2a_ = "c3", "cA1", "cA2", "cB1", "cB2", "f1a", "f1b", "f2a"
f2b_, fin_, finw_, fr_, fw_, h3_, hA1_, hA2_ = "f2b", "fin", "finw", "fr", "fw", "h3", "hA1", "hA2"
hB1_, hB2_, n_, n1_, nA2_, nA3_, nB2_, nB3_ = "hB1", "hB2", "n", "n1", "nA2", "nA3", "nB2", "nB3"
o0_, o0i_, o0o_, o1_, o1i_, o1o_, qda_, qdb_ = "o0", "o0i", "o0o", "o1", "o1i", "o1o", "qda", "qdb"
rf_, rn_, rsend_, st_, u_, u1_, uA2_, uA3_ = "rf", "rn", "rsend", "st", "u", "u1", "uA2", "uA3"
uB2_, uB3_, y_ = "uB2", "uB3", "y"
SCHEDULE = (
    (
        LN_,
        (
            (o0_, Qa_), (o0_, F1b_), (y_, Da_), (act_, cA1_),
            (act_, cB1_), (act_, hB1_), (y_, Db_), (act_, hA1_),
            (act_, cB2_), (o0_, F1a_), (o0_, F2b_), (y_, F1b_),
            (o0_, Db_), (o0_, Qb_), (o0_, F2a_), (act_, cA2_),
            (y_, F1a_), (act_, hB2_), (act_, hA2_), (o0_, Da_),
            (o1_, F1b_), (act_, c3_), (o1_, F1a_), (o1_, Da_),
            (y_, F2b_), (o1_, Db_), (y_, F2a_), (actw_, c3_),
            (y_, Qb_), (act_, h3_), (y_, Qa_), (o1_, F2b_),
            (o1_, F2a_), (actw_, h3_),
        ),
        (
            (o0o_, F1b_), (o0o_, Qb_), (y_, F1b_), (act_, cA1_),
            (y_, Qa_), (o0i_, F1b_), (o0i_, F1a_), (y_, F1a_),
            (act_, hB1_), (o1i_, F1b_), (o1o_, F1b_), (o0i_, Db_),
            (o0i_, Qb_), (an_, F1b_, 0), (act_, hA1_), (an_, Qa_, 0),
            (af1_, F1b_, 0), (o0o_, F2a_), (act_, cB1_), (act_, cA2_),
            (y_, Qb_), (o1i_, F1a_), (af1_, F1a_, 0), (an_, F1a_, 0),
            (act_, cB2_), (af2_, F1b_, 0), (af1_, F1b_, 1), (act_, hA2_),
            (af2_, Qa_, 0), (act_, hB2_), (o1o_, Qb_), (an_, F1b_, 1),
            (an_, F1a_, 1), (af2_, F1b_, 1), (an_, Da_, 0), (an_, Qb_, 0),
            (o1o_, F1a_), (act_, h3_), (an_, Da_, 1), (o0o_, F1a_),
            (y_, Da_), (o0i_, Da_), (act_, c3_), (af1_, F1a_, 1),
            (af2_, F1a_, 0), (o1i_, Da_), (y_, Db_), (o1i_, Db_),
            (af2_, F1a_, 1), (an_, Db_, 0), (actw_, h3_), (af2_, Da_, 0),
            (o0i_, Qa_), (o0o_, Da_),
        ),
    ),
    (
        F1b_,
        (
            (o1_, Qb_),
        ),
        (
            (actw_, c3_), (o1i_, Qa_),
        ),
    ),
    (
        U2b_,
        (
            (o1_, Qa_),
        ),
        (
            (y_, F2b_), (af2_, Da_, 1), (o1o_, Da_),
        ),
    ),
    (
        F1a_,
        (
            (rsend_, f2b_),
        ),
        (
            (af1_, Da_, 1),
        ),
    ),
    (
        U2a_,
        (),
        (
            (o0i_, F2a_), (y_, F2a_), (an_, Qb_, 1), (an_, Qa_, 1),
            (o0o_, Qa_), (af1_, Da_, 0), (an_, F2b_, 1),
        ),
    ),
    (
        TAB_,
        (
            (rsend_, f2a_),
        ),
        (),
    ),
    (
        GAa_,
        (),
        (),
    ),
    (
        PRa_,
        (),
        (
            (o0i_, F2b_), (rn_, f2b_, 3, 0), (o1i_, Qb_), (an_, Db_, 1),
            (af2_, Qa_, 1), (af1_, Qa_, 0), (o1o_, Qa_), (rn_, f2b_, 3, 1),
            (af1_, Qa_, 1),
        ),
    ),
    (
        ATa0_,
        (),
        (
            (af1_, Qb_, 0), (o0o_, Db_), (rn_, f2b_, 2, 1),
        ),
    ),
    (
        ATa1_,
        (),
        (
            (af1_, Db_, 0),
        ),
    ),
    (
        UQa_,
        (),
        (
            (rn_, f2b_, 2, 0), (af2_, Db_, 0), (o1o_, Db_),
        ),
    ),
    (
        PRb_,
        (
            (rsend_, qda_),
        ),
        (
            (an_, F2a_, 0), (an_, F2b_, 0), (af1_, Qb_, 1), (af2_, Qb_, 0),
            (o1i_, F2a_), (af2_, Qb_, 1), (af1_, Db_, 1),
        ),
    ),
    (
        GAb_,
        (),
        (
            (af2_, Db_, 1), (rf_, f2b_, 0),
        ),
    ),
    (
        ATb0_,
        (),
        (),
    ),
    (
        ATb1_,
        (),
        (),
    ),
    (
        UQb_,
        (),
        (
            (o1i_, F2b_),
        ),
    ),
    (
        HGb_,
        (
            (rsend_, qdb_), (fin_, f2b_, 0), (fin_, f2b_, 1), (fr_, b_),
        ),
        (
            (rf_, f2b_, 1), (o1o_, F2b_), (af1_, F2b_, 0), (af2_, F2b_, 1),
            (rn_, f2a_, 3, 0), (an_, F2a_, 1), (o0o_, F2b_), (fin_, f2b_, 0),
            (fin_, f2b_, 1), (rn_, f2a_, 2, 0), (af1_, F2b_, 1), (af2_, F2b_, 0),
        ),
    ),
    (
        U1b_,
        (),
        (
            (fr_, b_),
        ),
    ),
    (
        HGa_,
        (
            (fw_, b_), (rsend_, f1b_), (finw_, f2b_),
        ),
        (
            (af1_, F2a_, 0), (fin_, f2a_, 0), (af2_, F2a_, 0), (rn_, f2a_, 2, 1),
            (o1o_, F2a_), (rn_, qda_, 3, 0), (finw_, f2b_), (rn_, qda_, 2, 0),
            (af1_, F2a_, 1), (af2_, F2a_, 1),
        ),
    ),
    (
        NORM_,
        (
            (fin_, f2a_, 0),
        ),
        (
            (rn_, f2a_, 3, 1), (rn_, qda_, 2, 1),
        ),
    ),
    (
        U1a_,
        (
            (act_, n1_), (fin_, qda_, 0), (fin_, f2a_, 1), (fr_, a_),
            (fw_, a_),
        ),
        (
            (rf_, f2a_, 0), (fw_, b_), (act_, n1_), (act_, nA2_),
            (fin_, qda_, 1), (rn_, qda_, 3, 1), (rn_, qdb_, 3, 0), (rf_, f2a_, 1),
            (act_, nB2_), (rn_, f1b_, 3, 0), (fin_, f2a_, 1), (rn_, qdb_, 2, 0),
            (rf_, qda_, 0), (act_, nA3_), (rn_, qdb_, 3, 1), (act_, nB3_),
            (finw_, f2a_), (rn_, f1b_, 3, 1), (fr_, a_),
        ),
    ),
    (
        OUT_,
        (
            (rsend_, f1a_), (fin_, qdb_, 0), (act_, nA2_), (act_, nB2_),
        ),
        (
            (rn_, f1b_, 2, 0), (actw_, n_), (rf_, qdb_, 0), (rn_, qdb_, 2, 1),
            (fin_, qda_, 0),
        ),
    ),
    (
        NS_,
        (
            (act_, u1_), (fin_, f1b_, 0), (act_, nB3_), (act_, nA3_),
            (act_, uA2_), (act_, uB2_), (act_, uA3_), (fin_, f1a_, 0),
            (act_, uB3_), (actw_, n_),
        ),
        (
            (act_, u1_), (fin_, qdb_, 0), (rf_, qdb_, 1), (act_, uA2_),
            (rf_, f1b_, 0), (act_, uB2_), (fin_, f1b_, 0), (fw_, a_),
            (rf_, qda_, 1), (rn_, f1a_, 3, 0), (rn_, f1b_, 2, 1), (rn_, f1a_, 2, 0),
            (rf_, f1b_, 1), (act_, uB3_), (fin_, f1b_, 1), (rn_, f1a_, 2, 1),
            (act_, uA3_), (rn_, f1a_, 3, 1), (finw_, f1b_), (rf_, f1a_, 0),
            (fin_, qdb_, 1), (fin_, f1a_, 0),
        ),
    ),
    (
        WI_,
        (
            (act_, st_), (fin_, f1b_, 1), (finw_, f1b_), (actw_, u_),
            (fin_, f1a_, 1), (actw_, st_),
        ),
        (
            (act_, st_), (fin_, f1a_, 1), (finw_, qda_), (actw_, st_),
            (actw_, u_),
        ),
    ),
    (
        WB_,
        (),
        (),
    ),
    (
        END_,
        (
            (fin_, qdb_, 1), (finw_, f2a_), (fin_, qda_, 1), (finw_, qdb_),
            (finw_, qda_), (finw_, f1a_),
        ),
        (
            (rf_, f1a_, 1), (finw_, qdb_), (finw_, f1a_),
        ),
    ),
)


def fdot(a, b, dims=contract_in):
    return lax.dot_general(a, b, dims, preferred_element_type=f32)


def tiles(total, size, step):
    if total == size:
        step(0)
    else:
        pl.loop(0, total // size)(lambda i: step(pl.multiple_of(i * size, size)))


def bits_of(count):
    return [1 << i for i in range(count.bit_length() - 1)]


def halving_slots(C, T):
    return max(C * (T // 2 - 1) + C - 1, (T // 2) * (C - 1) + T // 2 - 1)


def block_kernel(dims, *refs):
    Z, C, T, r, fw, hw, lw, piece = dims
    (
        hid_hbm, cot_hbm, fc1w, qkvw, densew, fc2w, gain, bias, fc1b, qkvb, dense_b, fc2_b, segs, freqs,
        r_block, r_input, g_fc1, g_qd, g_fc2, r_fc1b, r_qkvb, r_outb, r_gain, r_bias,
        X, COT, W1, WQ, WD, W2, ACT, DG, TT, QV, GA, ATT, MI, COS, SIN, hid, cot_in,
        G2, R2, GQ, RQ, RT, RC, SM, SMR, ST, STR, qs, ks, dq, dk, dv,
        block_out, grad_input, o_fc1b, o_qkvb, o_outb, o_gain, o_bias,
        y_s, y_r, own_s, ag_s, ag_r, rs_s, rs_r, fin_s, fin_r, out_s,
        aa_s, aa_r, ar_s, ar_r, sm_s, sm_r, st_s, st_r, res_s, free,
    ) = refs
    L, D, U, last = piece * C, T * lw, Z * C, Z - 1
    fh, gw = fw // 2, min(hw, 128)
    groups, in_group, aligned = hw // gw, gw // HD, gw % 128 == 0
    z, c, t = lax.axis_index("dp"), lax.axis_index("ctx"), lax.axis_index("tensor")
    end_side, mid_side = z // last, z - 1
    end_in, mid_in, mid_out = z + 1 - 2 * end_side, last - z, last * mid_side
    is_end, is_mid = (z == 0) | (z == last), (z > 0) & (z < last)

    def remote(src, dst, send, recv, **where):
        return pltpu.make_async_remote_copy(
            src_ref=src, dst_ref=dst, send_sem=send, recv_sem=recv,
            device_id=where, device_id_type=MESH,
        )

    def exists(name):
        return groups == 2 or name[:2] not in ("Qb", "Db") and name != "qdb"

    def sub_offsets(own):
        return [0] if own else list(range(1, C))

    def weight(p, u, count=1):
        half = "ab".index(p[-1])
        units = u if count == 1 else pl.ds(u, count)
        rows = pl.ds(pl.multiple_of(u * r, r), count * r)
        if p[:2] == "F1":
            return W1.at[rows, half * fh : (half + 1) * fh]
        if p[0] == "Q":
            return WQ.at[half, :, rows]
        if p[0] == "D":
            return WD.at[units, half * gw : (half + 1) * gw]
        return W2.at[units, half * fh : (half + 1) * fh]

    def shard(p, k):
        half = "ab".index(p[-1])
        if p[:2] == "F1":
            return fc1w.at[:, pl.ds(pl.multiple_of(k * fw + half * fh, fh), fh)]
        if p[0] == "Q":
            if not aligned:
                return qkvw.at[k, half]
            return qkvw.at[:, :, pl.ds(pl.multiple_of(k * hw + half * gw, gw), gw)]
        if p[0] == "D":
            return densew.at[k, half * gw : (half + 1) * gw]
        return fc2w.at[k, half * fh : (half + 1) * fh]

    def y_copy(p, o):
        i, k = WEIGHTS.index(p), (c + o) % C
        return remote(shard(p, k), weight(p, z * C + c), y_s.at[i, o - 1], y_r.at[i, o - 1], ctx=k)

    def own_copy(p):
        i = WEIGHTS.index(p)
        return pltpu.make_async_copy(shard(p, c), weight(p, z * C + c), own_s.at[i])

    def ag_copy(p, u, way, to, src=None):
        i = WEIGHTS.index(p)
        src = weight(p, u) if src is None else src
        return remote(src, weight(p, u), ag_s.at[i, way], ag_r.at[i, u], dp=to)

    def ag_wait(p, u):
        ag_copy(p, u, 0, end_in).wait_recv()

    def y_start(p):
        for o in range(1, C):
            y_copy(p, o).start()
        own_copy(p).start()

    def send_own(p, second, way, to):
        if not second:
            ag_copy(p, z * C + c, way, to, shard(p, c)).start()
        for o in range(1, C) if second else ():
            ag_copy(p, z * C + (c - o) % C, way, to).start()

    def y_wait(p):
        for o in range(1, C):
            i, u, k = WEIGHTS.index(p), z * C + (c - o) % C, (c + o) % C
            remote(shard(p, k), weight(p, u), y_s.at[i, o - 1], y_r.at[i, o - 1], ctx=k).wait_recv()

    def forward(p, chunk, sub, way, to):
        for o in sub_offsets(sub == 0):
            u = chunk * C + (c - o) % C
            ag_wait(p, u)
            ag_copy(p, u, way, to).start()

    def weights_end(p):
        i = WEIGHTS.index(p)
        for o in range(1, C):
            y_copy(p, o).wait_send()

        def sent(way, chunk, chunks):
            region = weight(p, chunk * C, chunks * C)
            remote(region, region, ag_s.at[i, way], ag_r.at[i, 0], dp=mid_in).wait_send()

        pl.when(is_end)(lambda: sent(0, z, 1))

        @pl.when(is_mid)
        def _():
            sent(0, 2 * mid_side, 2)
            sent(1, 1 - mid_side, 3)

    def doubling(index, array, own, part, order):
        quarter = piece // 4
        skip, count_rows = ((0, 3 * quarter), (3 * quarter, quarter))[part]
        masks, blocks, at, plan = [0], 1, 0, []
        for axis, bit in order:
            plan.append((axis, bit, blocks, tuple(masks), at))
            at += len(masks) * blocks
            if axis == "c":
                blocks *= 2
            else:
                masks = masks + [m ^ bit for m in masks]

        def copies(stage):
            axis, bit, count, sent, first = plan[stage]
            where = {"ctx": c ^ bit} if axis == "c" else {"tensor": t ^ bit}
            found = []
            for b in range(count):
                start = ((c // count) * count + b) * piece + skip
                for j, m in enumerate(sent):
                    dst = array.at[
                        pl.ds(pl.multiple_of(start, quarter), count_rows),
                        pl.ds(pl.multiple_of((t ^ m) * lw, lw), lw),
                    ]
                    src = own.at[skip : skip + count_rows] if stage == 0 else dst
                    sem = first + b * len(sent) + j
                    found.append(remote(src, dst, aa_s.at[index, sem], aa_r.at[index, sem], **where))
            return found

        def begin(stage):
            for copy in copies(stage):
                copy.start()

        def arrive(stage):
            for copy in copies(stage):
                copy.wait_recv()

        def end():
            for stage in range(len(plan)):
                for copy in copies(stage):
                    copy.wait_send()

        return begin, arrive, end

    cbits = [("c", b) for b in bits_of(C)]
    tbits = [("t", b) for b in reversed(bits_of(T))]
    routes = (cbits + tbits, tbits[:-1] + cbits + tbits[-1:])
    doubles = {
        name + "AB"[part]: doubling(2 * i + part, array, own, part, routes[part])
        for i, (name, array, own) in enumerate((("h", X, hid_hbm), ("c", COT, cot_hbm)))
        for part in range(2)
    }
    doubling_stages = len(cbits) + len(tbits)

    def place(array, own, sem):
        return pltpu.make_async_copy(
            own,
            array.at[
                pl.ds(pl.multiple_of(c * piece, piece), piece), pl.ds(pl.multiple_of(t * lw, lw), lw)
            ],
            sem,
        )

    def load(i):
        return pltpu.make_async_copy((hid_hbm, cot_hbm)[i], (hid, cot_in)[i], own_s.at[10 + i])

    def double(name, step):
        if step == "3":
            for part in "AB":
                begin, arrive, _ = doubles[name + part]
                arrive(doubling_stages - 2)
                begin(doubling_stages - 1)
        else:
            begin, arrive, _ = doubles[name]
            stages = [0] if step == "1" else range(1, doubling_stages - 1)
            for stage in stages:
                if stage:
                    arrive(stage - 1)
                begin(stage)

    def double_wait(name):
        for part in "AB":
            doubles[name + part][1](doubling_stages - 1)

    def double_end(name):
        for part in "AB":
            doubles[name + part][2]()

    def grad_rows(q):
        return 4 * gw if q[0] == "q" else fh

    def grad_at(q, u, row, size, slots=False):
        half = "ab".index(q[-1])
        if q[0] == "q":
            return (RQ if slots else GQ).at[half, u, pl.ds(row, size)]
        return (R2 if slots else G2).at[u, pl.ds(half * fh + row, size)]

    def whole_at(q, u, slots=False):
        return grad_at(q, u, 0, grad_rows(q), slots)

    def grad_out(q):
        half = "ab".index(q[-1])
        if q[0] == "q":
            return g_qd.at[c, half]
        return (g_fc2 if q[1] == "2" else g_fc1).at[c, half * fh : (half + 1) * fh]

    def rs_copy(q, u, slot, way, number, to):
        i = GRADS.index(q)
        return remote(
            whole_at(q, u), whole_at(q, slot, True), rs_s.at[i, way],
            rs_r.at[i, number * C + u % C], dp=to,
        )

    def rs_add(q, u, slots):
        size = min(128, grad_rows(q))

        def add(row):
            ref = grad_at(q, u, row, size)
            total = ref[...].astype(f32)
            for slot in slots:
                total = total + grad_at(q, slot, row, size, True)[...].astype(f32)
            ref[...] = total.astype(bf16)

        tiles(grad_rows(q), size, add)

    def rs_send(q):
        for k in range(last):
            d = end_side * k + (1 - end_side) * (last - k)
            for own in (False, True):
                for o in sub_offsets(own):
                    u = d * C + (c + o) % C
                    rs_copy(q, u, u + C * (1 - end_side), 0, k, end_in).start()

    def rs_near(q, dist, sub):
        d = last * (1 - mid_side) if dist == last else last - z
        for o in sub_offsets(sub == 1):
            u = d * C + (c + o) % C
            slot = u + C * (1 - mid_side)
            near = 0 if dist == last else 1
            rs_copy(q, u, slot, 0, near, mid_in).wait_recv()
            rs_add(q, u, [slot])
            rs_copy(q, u, slot, 0, last + near, mid_in).start()

    def rs_far(q, sub):
        for o in sub_offsets(sub == 1):
            u = last * mid_side * C + (c + o) % C
            slot = u + C * mid_side
            rs_copy(q, u, slot, 1, last, mid_out).wait_recv()
            rs_add(q, u, [slot])
            rs_copy(q, u, slot, 1, last, mid_out).start()

    def fin_copy(q, o):
        i, k = GRADS.index(q), (c + o) % C
        return remote(whole_at(q, z * C + k), grad_out(q), fin_s.at[i, o - 1], fin_r.at[i, o - 1], ctx=k)

    def fin_own(q):
        return pltpu.make_async_copy(
            whole_at(q, z * C + c), grad_out(q), out_s.at[GRADS.index(q)]
        )

    def finish(q, sub, at_end):
        for o in sub_offsets(sub == 1):
            u = z * C + (c + o) % C
            if at_end:
                slots = [u + C * end_side]
                rs_copy(q, u, slots[0], 1, last, end_in).wait_recv()
            else:
                slots = [u + C * (1 - mid_side), u + C * mid_side]
                for slot, number in zip(slots, (last - 1, last + 1)):
                    rs_copy(q, u, slot, 0, number, mid_in).wait_recv()
            rs_add(q, u, slots)
            if o:
                fin_copy(q, o).start()
            else:
                fin_own(q).start()

    def grads_sent(q):
        i, half = GRADS.index(q), "ab".index(q[-1])

        def sent(way, chunk, chunks):
            units = pl.ds(chunk * C, chunks * C)
            if q[0] == "q":
                region = GQ.at[half, units]
            else:
                region = G2.at[units, half * fh : (half + 1) * fh]
            remote(region, region, rs_s.at[i, way], rs_r.at[i, 0], dp=mid_in).wait_send()

        pl.when(is_end)(lambda: sent(0, 1 - end_side, last))

        @pl.when(is_mid)
        def _():
            sent(0, 2 - 2 * mid_side, 2)
            sent(1, last * mid_side, 1)

        for o in range(1, C):
            fin_copy(q, o).wait_send()
        fin_own(q).wait()

    def grads_arrived(q):
        for o in range(1, C):
            fin_copy(q, o).wait_recv()

    def tables():
        lane = lax.broadcasted_iota(jnp.int32, (128, gw), 1) % HD

        def rows_of(row):
            rows = pl.ds(row, 128)
            every = segs[...].astype(f32)
            own = jnp.broadcast_to(segs[:, rows].astype(f32), (128, 128)).T[:, 0:1]
            start = jnp.sum((every < own).astype(f32), axis=1, keepdims=True)
            at = (lax.broadcasted_iota(jnp.int32, (128, 1), 0) + row).astype(f32)
            angle = (at - start) * freqs[...]
            MI[rows, 2:3] = start
            COS[rows] = jnp.cos(angle)
            sine = jnp.sin(angle)
            SIN[rows] = jnp.where(lane < ROT // 2, -sine, sine)

        tiles(L, 128, rows_of)
        SM[...] = jnp.zeros_like(SM)
        for i in range(2):
            load(i).wait()
        SM[2:3, :lw] = jnp.sum(cot_in[...].astype(f32), axis=0, keepdims=True)

    def layer_norm():
        double_end("h")

        def rows_of(row):
            rows = pl.ds(row, 128)
            x = X[rows].astype(f32)
            mean = jnp.mean(x, axis=1, keepdims=True)
            centered = x - mean
            inv = lax.rsqrt(jnp.mean(centered * centered, axis=1, keepdims=True) + ln_eps)
            MI[rows, 0:1] = mean
            MI[rows, 1:2] = inv
            X[rows] = (centered * inv * gain[...] + bias[...]).astype(bf16)

        tiles(L, 128, rows_of)

    cf = min(BLOCK, fh)
    gelu_c = math.sqrt(2.0 / math.pi)

    def hidden(half):
        def cols_of(col):
            cols = pl.ds(half * fh + col, cf)
            shift = fc1b[:, pl.ds(pl.multiple_of(c * fw + half * fh + col, cf), cf)]

            def rows_of(row):
                rows = pl.ds(row, ROWS)
                v = fdot(X[rows], W1[:, cols]) + shift
                tanh = jnp.tanh(gelu_c * (v + 0.044715 * (v * v * v)))
                act = 0.5 * v * (1.0 + tanh)
                slope = gelu_c * (1.0 + 3.0 * 0.044715 * (v * v))
                DG[rows, cols] = (0.5 * (1.0 + tanh) + 0.5 * v * (1.0 - tanh * tanh) * slope).astype(bf16)
                ACT[rows, cols] = act.astype(bf16)
                TT[cols, rows] = act.T.astype(bf16)

            tiles(L, ROWS, rows_of)

        tiles(fh, cf, cols_of)

    def over_each_unit(step):
        if r % 128 == 0:
            pl.loop(0, U)(lambda u: step(u, pl.ds(pl.multiple_of(u * r, r), r)))
        else:
            for u in range(U):
                step(u, slice(u * r, (u + 1) * r))

    def unit_grads(q):
        half = "ab".index(q[-1])

        def step(u, cols):
            if q[0] == "q":
                first = half * 4 * gw
                GQ[half, u, : 3 * gw] = fdot(TT[first : first + 3 * gw], X[:, cols]).astype(bf16)
                GQ[half, u, 3 * gw :] = fdot(TT[first + 3 * gw : first + 4 * gw], COT[:, cols]).astype(bf16)
            else:
                rows = slice(half * fh, (half + 1) * fh)
                source = COT if q[1] == "2" else X
                G2[u, rows] = fdot(TT[rows], source[:, cols]).astype(bf16)

        over_each_unit(step)

    def side_by_side(rows, group):
        return jnp.concatenate([WQ[group, part, rows] for part in range(3)], axis=1)

    def project(group):
        def shift(part):
            if not aligned:
                return qkvb[part : part + 1]
            return qkvb[part : part + 1, pl.ds(pl.multiple_of(c * hw + group * gw, gw), gw)]

        shifts = jnp.concatenate([shift(part) for part in range(3)], axis=1)

        def rows_of(row):
            rows = pl.ds(row, ROWS)
            QV[group, rows] = (fdot(X[rows], side_by_side(pl.ds(0, D), group)) + shifts).astype(bf16)

        tiles(L, ROWS, rows_of)

    def over_units(rows, weights):
        total = None
        for u in range(U):
            term = fdot(COT[rows, u * r : (u + 1) * r], weights(u), contract_cols)
            total = term if total is None else total + term
        return total

    def attended_grads(group):
        def rows_of(row):
            rows = pl.ds(row, ROWS)
            lanes = slice(group * gw, (group + 1) * gw)
            GA[rows] = over_units(rows, lambda u: WD[u, lanes]).astype(bf16)

        tiles(L, ROWS, rows_of)

    half_rot = ROT // 2
    scale = 1.0 / math.sqrt(HD)

    def turn(values, rows, sign):
        lane = lax.broadcasted_iota(jnp.int32, values.shape, 1) % HD
        other = jnp.where(
            lane < half_rot, pltpu.roll(values, gw - half_rot, 1), pltpu.roll(values, half_rot, 1)
        )
        turned = other * SIN[rows]
        return values * COS[rows] + (turned if sign > 0 else -turned)

    def attention_load(group):
        def load(row):
            rows = pl.ds(row, BLOCK)
            qs[rows] = turn(QV[group, rows, :gw].astype(f32), rows, 1).astype(bf16)
            ks[rows] = turn(QV[group, rows, gw : 2 * gw].astype(f32), rows, 1).astype(bf16)

        tiles(L, BLOCK, load)
        for ref in (dq, dk, dv):
            ref[...] = jnp.zeros_like(ref)
        ATT[:, group * gw : (group + 1) * gw] = jnp.zeros((L, gw), bf16)

    def attention_head(group, head):
        own = slice(group * gw, (group + 1) * gw)
        for row in range(0, L, BLOCK):
            low = max(0, row - DOC_MAX)
            span = row + BLOCK - low
            rows, cols = pl.ds(row, BLOCK), pl.ds(low, span)
            mine = lax.broadcasted_iota(jnp.int32, (BLOCK, gw), 1) // HD == head
            query = jnp.where(mine, qs[rows].astype(f32), 0.0).astype(bf16)
            grad = jnp.where(mine, GA[rows].astype(f32), 0.0)
            grad_b, key, value = grad.astype(bf16), ks[cols], QV[group, cols, 2 * gw :]
            query_pos = row + lax.broadcasted_iota(jnp.int32, (BLOCK, span), 0)
            key_pos = low + lax.broadcasted_iota(jnp.int32, (BLOCK, span), 1)
            allowed = (key_pos >= MI[rows, 2:3].astype(jnp.int32)) & (key_pos <= query_pos)
            scores = jnp.where(allowed, fdot(query, key, contract_cols) * scale, mask_fill)
            weights = jnp.exp(scores - jnp.max(scores, axis=1, keepdims=True))
            probs = weights * (1.0 / jnp.sum(weights, axis=1, keepdims=True))
            probs_b = probs.astype(bf16)
            attended = jnp.where(mine, fdot(probs_b, value), 0.0).astype(bf16)
            delta = jnp.sum(grad * attended.astype(f32), axis=1, keepdims=True)
            grad_probs = fdot(grad_b, value, contract_cols)
            grad_scores = (probs * (grad_probs - delta)).astype(bf16)
            dv[cols] += fdot(probs_b, grad_b, contract_rows)
            dk[cols] += fdot(grad_scores, query, contract_rows)
            dq[rows] += jnp.where(mine, fdot(grad_scores, key), 0.0)
            ATT[rows, own] += attended

    def attention_save(group):
        first = group * 4 * gw

        def save(row):
            rows = pl.ds(row, BLOCK)
            attended = ATT[rows, group * gw : (group + 1) * gw].astype(f32)
            TT[first + 3 * gw : first + 4 * gw, rows] = attended.T.astype(bf16)
            grads = turn(dq[rows] * scale, rows, -1), turn(dk[rows] * scale, rows, -1), dv[rows]
            for part, grad in enumerate(grads):
                lanes = slice(part * gw, (part + 1) * gw)
                QV[group, rows, lanes] = grad.astype(bf16)
                TT[first + part * gw : first + (part + 1) * gw, rows] = grad.T.astype(bf16)
                sums = jnp.sum(grad.astype(bf16).astype(f32), axis=0, keepdims=True)
                SM[5 + group : 6 + group, lanes] += sums

        tiles(L, BLOCK, save)

    def attention_heads(group, second):
        mine = range(in_group // 2, in_group) if second else range(in_group // 2)
        if in_group == 1:
            mine = [] if second else [0]
        if not second:
            attention_load(group)
        for head in mine:
            attention_head(group, head)
        if second:
            attention_save(group)

    def hidden_grads(half):
        for n in range(fh // cf):
            cols = slice(half * fh + n * cf, half * fh + (n + 1) * cf)

            def rows_of(row):
                rows = pl.ds(row, ROWS)
                grad = over_units(rows, lambda u: W2[u, cols]) * DG[rows, cols].astype(f32)
                SM[0:1, cols] += jnp.sum(grad, axis=0, keepdims=True)
                DG[rows, cols] = grad.astype(bf16)
                TT[cols, rows] = grad.T.astype(bf16)

            tiles(L, ROWS, rows_of)

    rows_half = piece // 2

    def halving(a, part):
        first_bit, later_bits = bits_of(T)[0], [("t", b) for b in bits_of(T)[1:]]
        first_kept = [m for m in range(T) if not m & first_bit]
        c_bits = [("c", b) for b in reversed(bits_of(C))]

        def cols_of(m):
            return pl.ds(pl.multiple_of((t ^ m) * lw, lw), lw)

        def rows_at(block, which):
            return pl.ds(pl.multiple_of(block * piece + which * rows_half, rows_half), rows_half)

        def plan_of(order):
            plan, masks, blocks, slot = [], first_kept, C, 0
            for axis, bit in order:
                if axis == "t":
                    masks = [m for m in masks if not m & bit]
                else:
                    blocks = bit
                plan.append((axis, bit, masks, blocks, slot))
                slot += blocks * len(masks)
            return plan

        plans = plan_of(later_bits + c_bits), plan_of(c_bits + later_bits)

        def add(target, source, size):
            def rows_of(row):
                rows = pl.ds(row, 128)
                total = target.at[rows][...].astype(f32) + source.at[rows][...].astype(f32)
                target.at[rows][...] = total.astype(bf16)

            tiles(size, min(128, size), rows_of) if size % 128 == 0 else add_whole(target, source)

        def add_whole(target, source):
            target[...] = (target[...].astype(f32) + source[...].astype(f32)).astype(bf16)

        def first_copies():
            return [
                remote(
                    part.at[:, cols_of(m ^ first_bit)], RT.at[a, j],
                    ar_s.at[a, 0, j], ar_r.at[a, 0, j], tensor=t ^ first_bit,
                )
                for j, m in enumerate(first_kept)
            ]

        def copies(which, stage):
            axis, bit, masks, blocks, slot = plans[which][stage]
            where = {"ctx": c ^ bit} if axis == "c" else {"tensor": t ^ bit}
            start = (c ^ bit) // blocks * blocks if axis == "c" else c // blocks * blocks
            flip = 0 if axis == "c" else bit
            return [
                remote(
                    part.at[rows_at(start + b, which), cols_of(m ^ flip)],
                    RC.at[a, which, slot + b * len(masks) + j],
                    ar_s.at[a, 1 + which, slot + b * len(masks) + j],
                    ar_r.at[a, 1 + which, slot + b * len(masks) + j],
                    **where,
                )
                for b in range(blocks)
                for j, m in enumerate(masks)
            ]

        def arrive(which, stage):
            for copy in copies(which, stage):
                copy.wait_recv()
            axis, bit, masks, blocks, slot = plans[which][stage]
            if stage == len(plans[which]) - 1:
                return
            for b in range(blocks):
                for j, m in enumerate(masks):
                    add(
                        part.at[rows_at(c // blocks * blocks + b, which), cols_of(m)],
                        RC.at[a, which, slot + b * len(masks) + j],
                        rows_half,
                    )

        def begin(which, stage):
            for copy in copies(which, stage):
                copy.start()

        def run(step):
            if step == "1":
                for copy in first_copies():
                    copy.start()
                return
            which = "AB".index(step[0])
            if step[1] == "3":
                for stage in range(1, len(plans[which])):
                    arrive(which, stage - 1)
                    begin(which, stage)
                return
            if which == 0:
                for copy in first_copies():
                    copy.wait_recv()
                for j, m in enumerate(first_kept):
                    add(part.at[:, cols_of(m)], RT.at[a, j], L)
            begin(which, 0)

        def wait():
            for which in range(2):
                arrive(which, len(plans[which]) - 1)

        def total(row, size):
            which, slot = row // rows_half, None
            slot = plans[which][-1][4]
            rows = pl.ds(pl.multiple_of(c * piece + row, size), size)
            received = RC[a, which, slot, row % rows_half : row % rows_half + size]
            return part[rows, cols_of(0)].astype(f32) + received.astype(f32)

        def end():
            for copy in first_copies():
                copy.wait_send()
            for which in range(2):
                for stage in range(len(plans[which])):
                    for copy in copies(which, stage):
                        copy.wait_send()

        return run, wait, total, end

    n_run, n_wait, n_total, n_end = halving(0, COT)
    u_run, u_wait, u_total, u_end = halving(1, X)

    def norm_units():
        double_end("c")

        def step(u, cols):
            w1 = W1[pl.ds(pl.multiple_of(u * r, r), r)]
            wq = [side_by_side(pl.ds(pl.multiple_of(u * r, r), r), g) for g in range(groups)]

            def rows_of(row):
                rows = pl.ds(row, ROWS)
                total = fdot(DG[rows], w1, contract_cols)
                for g in range(groups):
                    total = total + fdot(QV[g, rows], wq[g], contract_cols)
                COT[rows, cols] = total.astype(bf16)

            tiles(L, ROWS, rows_of)

        over_each_unit(step)

    def out_units():
        def step(u, cols):
            def rows_of(row):
                rows = pl.ds(row, ROWS)
                X[rows, cols] = (fdot(ATT[rows], WD[u]) + fdot(ACT[rows], W2[u])).astype(bf16)

            tiles(L, ROWS, rows_of)

        over_each_unit(step)

    size = min(128, rows_half)

    def write_block():
        shift = dense_b[...] + fc2_b[...]
        for row in range(0, piece, size):
            rows = pl.ds(row, size)
            block_out[rows] = (hid[rows].astype(f32) + u_total(row, size) + shift).astype(bf16)
        final(0).start()

    def gain_own():
        return gain[:, pl.ds(pl.multiple_of(t * lw, lw), lw)]

    def standard_of(row):
        rows = pl.ds(pl.multiple_of(c * piece + row, size), size)
        inv = MI[rows, 1:2]
        return (hid[pl.ds(row, size)].astype(f32) - MI[rows, 0:1]) * inv, inv

    def norm_sums():
        for row in range(0, piece, size):
            grad = n_total(row, size)
            standard, _ = standard_of(row)
            scaled = grad * gain_own()
            first = jnp.sum(scaled, axis=1, keepdims=True)
            second = jnp.sum(scaled * standard, axis=1, keepdims=True)
            lane = lax.broadcasted_iota(jnp.int32, (size, 128), 1)
            pair = jnp.where(lane == 0, first, jnp.where(lane == 1, second, 0.0))
            ST[:, row : row + size] = pair.T[0:8]
            SM[3:4, :lw] += jnp.sum(grad * standard, axis=0, keepdims=True)
            SM[4:5, :lw] += jnp.sum(grad, axis=0, keepdims=True)

    def st_copy(o):
        return remote(ST, STR.at[o - 1], st_s.at[o - 1], st_r.at[o - 1], tensor=(t + o) % T)

    def sm_copy(dz, dc):
        o = dz * C + dc - 1
        return remote(
            SM, SMR.at[z * C + c], sm_s.at[o], sm_r.at[o], dp=(z + dz) % Z, ctx=(c + dc) % C
        )

    finals = (
        (block_out, r_block), (grad_input, r_input), (o_fc1b, r_fc1b), (o_qkvb, r_qkvb),
        (o_outb, r_outb), (o_gain, r_gain), (o_bias, r_bias),
    )

    def final(i):
        return pltpu.make_async_copy(*finals[i], res_s.at[i])

    offsets = [(dz, dc) for dz in range(Z) for dc in range(C) if dz or dc]

    def stats_start():
        for o in range(1, T):
            st_copy(o).start()
        for dz, dc in offsets:
            sm_copy(dz, dc).start()

    def stats_wait():
        for o in range(1, T):
            st_copy(o).wait()

    def write_input():
        for row in range(0, piece, size):
            stats = ST[:, row : row + size]
            for o in range(1, T):
                stats = stats + STR[o - 1, :, row : row + size]
            stats = jnp.concatenate([stats, jnp.zeros((120, size), f32)], axis=0).T * (1.0 / D)
            standard, inv = standard_of(row)
            scaled = n_total(row, size) * gain_own()
            rows = pl.ds(row, size)
            grad_input[rows] = cot_in[rows].astype(f32) + inv * (
                scaled - stats[:, 0:1] - standard * stats[:, 1:2]
            )
        final(1).start()

    def small_sums():
        SMR[z * C + c] = SM[...]
        for dz, dc in offsets:
            sm_copy(dz, dc).wait()

        def summed(row, size, units):
            total = SMR[units[0], row : row + 1, :size]
            for u in units[1:]:
                total = total + SMR[u, row : row + 1, :size]
            return total

        for k in range(C):
            units = [zs * C + k for zs in range(Z)]
            o_fc1b[:, k * fw : (k + 1) * fw] = summed(0, fw, units)
            for g in range(groups):
                sums = summed(5 + g, 3 * gw, units)
                for part in range(3):
                    lanes = slice(k * hw + g * gw, k * hw + (g + 1) * gw)
                    o_qkvb[part : part + 1, lanes] = sums[:, part * gw : (part + 1) * gw]
        for i, out in enumerate((o_outb, o_gain, o_bias)):
            out[...] = summed(2 + i, lw, list(range(U)))
        for i in range(2, len(finals)):
            final(i).start()

    computes = {"TAB": tables, "LN": layer_norm, "NORM": norm_units, "OUT": out_units}
    computes.update({"NS": norm_sums, "WI": write_input, "WB": write_block})
    for i, half in enumerate("ab"):
        computes["F1" + half] = partial(hidden, i)
        computes["U2" + half] = partial(unit_grads, "f2" + half)
        computes["U1" + half] = partial(unit_grads, "f1" + half)
        computes["HG" + half] = partial(hidden_grads, i)
        if i < groups:
            computes["PR" + half] = partial(project, i)
            computes["GA" + half] = partial(attended_grads, i)
            computes["AT" + half + "0"] = partial(attention_heads, i, False)
            computes["AT" + half + "1"] = partial(attention_heads, i, True)
            computes["UQ" + half] = partial(unit_grads, "qd" + half)

    def action(kind, name, *rest, at_end):
        if kind == "act" or kind == "actw":
            if name == "st":
                (stats_start if kind == "act" else stats_wait)()
            elif name[0] in "hc":
                if kind == "actw":
                    double_wait(name[0])
                elif name[1:] == "3":
                    double(name[0], "3")
                else:
                    double(name[:2], name[2])
            elif kind == "actw":
                (n_wait if name[0] == "n" else u_wait)()
            else:
                (n_run if name[0] == "n" else u_run)(name[1:])
        elif kind == "fr":
            grads_sent("f2" + name)
            half = "ab".index(name)

            def tell(to, way):
                pl.semaphore_signal(free.at[half, way], 1, device_id={"dp": to}, device_id_type=MESH)

            if at_end:
                tell(end_in, 0)
            else:
                tell(mid_in, 1)
                tell(mid_out, 1)
        elif kind == "fw":
            half = "ab".index(name)
            if not at_end:
                pl.semaphore_wait(free.at[half, 0], 1)
            pl.semaphore_wait(free.at[half, 1], 1)
        elif not exists(name):
            return
        elif kind == "y":
            y_start(name)
        elif kind == "o0":
            send_own(name, False, 0, end_in)
        elif kind == "o1":
            y_wait(name)
            send_own(name, True, 0, end_in)
        elif kind in ("o0i", "o0o", "o1i", "o1o"):
            if kind[1] == "1" and (name, "seen") not in seen:
                y_wait(name)
                seen.add((name, "seen"))
            way = "io".index(kind[2])
            send_own(name, kind[1] == "1", way, (mid_in, mid_out)[way])
        elif kind == "an":
            forward(name, mid_out, rest[0], 0, mid_in)
        elif kind == "af1":
            forward(name, mid_in, rest[0], 1, mid_out)
        elif kind == "af2":
            forward(name, last - mid_out, rest[0], 1, mid_out)
        elif kind == "rsend":
            rs_send(name)
        elif kind == "rn":
            rs_near(name, *rest)
        elif kind == "rf":
            rs_far(name, *rest)
        elif kind == "fin":
            finish(name, rest[0], at_end)

    seen = set()

    owns = (X, hid_hbm), (COT, cot_hbm)
    for i, (array, own) in enumerate(owns):
        place(array, own, own_s.at[8 + i]).start()
        load(i).start()

    barrier = pltpu.get_barrier_semaphore()

    def greet(**where):
        pl.semaphore_signal(barrier, 1, device_id=where, device_id_type=MESH)

    @pl.when(is_end)
    def _():
        greet(dp=end_in)

    @pl.when(is_mid)
    def _():
        greet(dp=mid_in)
        greet(dp=mid_out)

    for o in range(1, C):
        greet(ctx=(c + o) % C)
    for o in range(1, T):
        greet(tensor=(t + o) % T)
    pl.when(is_end)(lambda: pl.semaphore_wait(barrier, C + T - 1))
    pl.when(is_mid)(lambda: pl.semaphore_wait(barrier, C + T))
    for i, (array, own) in enumerate(owns):
        place(array, own, own_s.at[8 + i]).wait()

    for name, at_ends, inside in SCHEDULE:

        @pl.when(is_end)
        def _():
            for step in at_ends:
                action(*step, at_end=True)

        @pl.when(is_mid)
        def _():
            for step in inside:
                action(*step, at_end=False)

        if name not in computes:
            continue
        needed = NEEDS.get(name)
        if needed is not None:

            @pl.when(is_end)
            def _():
                for dz in range(1, Z):
                    for cs in range(C):
                        ag_wait(needed, ((z + dz) % Z) * C + cs)

            own_copy(needed).wait()
        computes[name]()

    small_sums()
    for q in GRADS:
        if exists(q):
            grads_arrived(q)
    n_end()
    u_end()
    for p in WEIGHTS:
        if exists(p):
            weights_end(p)
    for q in GRADS[2:]:
        if exists(q):
            grads_sent(q)
    for i in range(len(finals)):
        final(i).wait()


def body(
    hidden_in,
    segments,
    ln_gain,
    ln_bias,
    qkv_weight,
    qkv_bias,
    dense_weight,
    dense_bias,
    fc1_weight,
    fc1_bias,
    fc2_weight,
    fc2_bias,
    cotangent,
):
    _, piece, lw = hidden_in.shape
    C, T, Z = lax.axis_size("ctx"), lax.axis_size("tensor"), lax.axis_size("dp")
    L, D, U = piece * C, lw * T, Z * C
    r = qkv_weight.shape[0]
    hw, fw = lw // C, fc1_weight.shape[1] // C
    gw = min(hw, 128)
    groups, aligned = hw // gw, gw % 128 == 0
    lane = np.arange(gw) % HD
    freqs = rope_base ** (-((lane % (ROT // 2)) * 2.0) / ROT)
    freqs = jnp.asarray(np.where(lane < ROT, freqs, 0.0)[None], f32)
    if aligned:
        qkvw, own_bias = qkv_weight.transpose(1, 0, 2), qkv_bias
    else:
        qkvw = qkv_weight.reshape(r, 3, C, groups, gw).transpose(2, 3, 1, 0, 4)
        own_bias = lax.dynamic_slice_in_dim(qkv_bias, lax.axis_index("ctx") * hw, hw, 1)
    operands = [
        hidden_in[0],
        cotangent[0],
        fc1_weight,
        qkvw,
        dense_weight.reshape(C, hw, r),
        fc2_weight.reshape(C, fw, r),
        ln_gain[None],
        ln_bias[None],
        fc1_bias[None],
        own_bias,
        dense_bias[None],
        fc2_bias[None],
        segments,
        freqs,
    ]
    vmem, anywhere = pl.BlockSpec(memory_space=pltpu.VMEM), pl.BlockSpec(memory_space=pl.ANY)
    in_specs = [anywhere] * 6 + [vmem] * 8

    def out(shape, dtype=f32):
        return jax.ShapeDtypeStruct(shape, dtype)

    outs = [
        out((piece, lw), bf16),
        out((piece, lw)),
        out((C, fw, r), bf16),
        out((C, groups, 4 * gw, r), bf16),
        out((C, fw, r), bf16),
        out((1, C * fw)),
        out((3, lw)),
        out((1, lw)),
        out((1, lw)),
        out((1, lw)),
    ]
    out_specs = [anywhere] * 10
    most = max(fw, 3 * gw, lw)
    V = pltpu.VMEM
    dma = pltpu.SemaphoreType.DMA
    blocks, slots = C * T, max(halving_slots(C, T), T // 2)
    scratch = [
        V((L, D), bf16), V((L, D), bf16),
        V((D, fw), bf16), V((groups, 3, D, gw), bf16), V((U, hw, r), bf16), V((U, fw, r), bf16),
        V((L, fw), bf16), V((L, fw), bf16), V((max(fw, 4 * hw), L), bf16),
        V((groups, L, 3 * gw), bf16), V((L, gw), bf16), V((L, hw), bf16), V((L, 4), f32),
        V((L, gw), f32), V((L, gw), f32), V((piece, lw), bf16), V((piece, lw), bf16),
        V((U, fw, r), bf16), V((U + C, fw, r), bf16),
        V((groups, U, 4 * gw, r), bf16), V((groups, U + C, 4 * gw, r), bf16),
        V((2, T // 2, L, lw), bf16), V((2, 2, halving_slots(C, T), piece // 2, lw), bf16),
        V((8, most), f32), V((U, 8, most), f32), V((8, piece), f32), V((T - 1, 8, piece), f32),
        *[V((L, gw), bf16)] * 2, *[V((L, gw), f32)] * 3,
        *[V(o.shape, o.dtype) for o in outs[:2] + outs[5:]],
        dma((8, C - 1)), dma((8, C - 1)), dma((12,)), dma((8, 2)), dma((8, U)),
        dma((6, 2)), dma((6, 5 * C)), dma((6, C - 1)), dma((6, C - 1)), dma((6,)),
        dma((4, blocks)), dma((4, blocks)), dma((2, 3, slots)), dma((2, 3, slots)),
        dma((U - 1,)), dma((U - 1,)), dma((T - 1,)), dma((T - 1,)), dma((7,)),
        pltpu.SemaphoreType.REGULAR((2, 2)),
    ]
    results = pl.pallas_call(
        partial(block_kernel, (Z, C, T, r, fw, hw, lw, piece)),
        in_specs=in_specs,
        out_specs=out_specs,
        out_shape=outs,
        scratch_shapes=scratch,
        compiler_params=pltpu.CompilerParams(
            collective_id=0, has_side_effects=True, vmem_limit_bytes=67043328
        ),
        name="transformer_block",
    )(*operands)
    block_out, grad_input, g_fc1, g_qd, g_fc2, *sums = results
    if aligned and r % 128 == 0:
        block_out, grad_input, grad_fc1, grad_qkv, grad_dense, grad_fc2, *sums = unpack(results)
        grad_qkv = grad_qkv.transpose(1, 0, 2)
    else:
        sums.append(sums[2])
        grad_fc1 = g_fc1.astype(f32).transpose(2, 0, 1).reshape(r, C * fw)
        grad_qkv = g_qd[:, :, : 3 * gw].astype(f32).reshape(C, groups, 3, gw, r)
        grad_qkv = grad_qkv.transpose(4, 2, 0, 1, 3).reshape(r, 3, lw)
        grad_dense = g_qd[:, :, 3 * gw :].astype(f32).reshape(lw, r)
        grad_fc2 = g_fc2.astype(f32).reshape(C * fw, r)
    return (
        block_out[None],
        grad_input[None],
        grad_qkv,
        sums[1],
        grad_dense,
        sums[2][0],
        grad_fc1,
        sums[0][0],
        grad_fc2,
        sums[5][0],
        sums[3][0],
        sums[4][0],
    )


def unpack_kernel(gw, count, *refs):
    ins, outs, refs = refs[:count], refs[count : 2 * count + 2], refs[2 * count + 2 :]
    held, made, in_sem, out_sem = refs[:count], refs[count:-2], refs[-2], refs[-1]
    order = [4, 3, 2, 1, 0, *range(5, count)]
    reads = [pltpu.make_async_copy(ins[i], held[i], in_sem.at[i]) for i in range(count)]
    for i in order:
        reads[i].start()
    writes = []

    def write(src, out):
        copy = pltpu.make_async_copy(src, outs[out], out_sem.at[out])
        copy.start()
        writes.append(copy)

    blocks, quad = held[3].shape[:2]
    fc1, dense, qkv, fc2 = made
    for i in order:
        reads[i].wait()
        if i == 4:
            fc2[...] = held[4][...].astype(f32)
            write(fc2, 5)
        elif i == 3:
            for b in range(blocks):
                dense[b * gw : (b + 1) * gw] = held[3][b, 3 * gw :].astype(f32)
                for part in range(3):
                    source = held[3][b, part * gw : (part + 1) * gw].astype(f32)
                    qkv[part, :, b * gw : (b + 1) * gw] = source.T
            write(dense, 4)
            write(qkv, 3)
        elif i == 2:
            fc1[...] = held[2][...].astype(f32).T
            write(fc1, 2)
        elif i < 2:
            write(held[i], i)
        else:
            write(held[i], i + 1)
            if i == 7:
                write(held[i], count + 1)
    for copy in writes:
        copy.wait()


def unpack(results):
    block_out, grad_input, g_fc1, g_qd, g_fc2, *sums = results
    (piece, lw), (C, fw, r), (_, groups, quad, _) = block_out.shape, g_fc1.shape, g_qd.shape
    gw = quad // 4
    operands = [
        block_out, grad_input, g_fc1.reshape(C * fw, r), g_qd.reshape(C * groups, quad, r),
        g_fc2.reshape(C * fw, r), *sums,
    ]
    shapes = (r, C * fw), (3, r, lw), (lw, r), (C * fw, r)
    made = shapes[0], shapes[2], shapes[1], shapes[3]
    outs = [jax.ShapeDtypeStruct(a.shape, a.dtype) for a in operands[:2]]
    outs += [jax.ShapeDtypeStruct(s, f32) for s in (*shapes, *[s.shape for s in sums], sums[2].shape)]
    dma, count = pltpu.SemaphoreType.DMA, len(operands)
    anywhere = pl.BlockSpec(memory_space=pl.ANY)
    return pl.pallas_call(
        partial(unpack_kernel, gw, count),
        in_specs=[anywhere] * count,
        out_specs=[anywhere] * len(outs),
        out_shape=outs,
        scratch_shapes=[
            *[pltpu.VMEM(a.shape, a.dtype) for a in operands],
            *[pltpu.VMEM(s, f32) for s in made],
            dma((count,)), dma((len(outs),)),
        ],
        name="unpack_results",
    )(*operands)


def solution(mesh):
    in_specs = (
        P("dp", "ctx", "tensor"),
        P("dp", None),
        P(),
        P(),
        P(("dp", "ctx"), None, "tensor"),
        P(None, "tensor"),
        P("tensor", ("dp", "ctx")),
        P("tensor"),
        P(("dp", "ctx"), "tensor"),
        P("tensor"),
        P("tensor", ("dp", "ctx")),
        P("tensor"),
        P("dp", "ctx", "tensor"),
    )
    out_specs = (
        P("dp", "ctx", "tensor"),
        P("dp", "ctx", "tensor"),
        P(("dp", "ctx"), None, "tensor"),
        P(None, "tensor"),
        P("tensor", ("dp", "ctx")),
        P("tensor"),
        P(("dp", "ctx"), "tensor"),
        P("tensor"),
        P("tensor", ("dp", "ctx")),
        P("tensor"),
        P("tensor"),
        P("tensor"),
    )
    return jax.shard_map(body, mesh=mesh, in_specs=in_specs, out_specs=out_specs, check_vma=False)
```

```python
from functools import partial
import math

import jax
import jax.numpy as jnp
import numpy as np
from jax import lax
from jax.experimental import pallas as pl
from jax.experimental.pallas import tpu as pltpu
from jax.sharding import PartitionSpec as P

HD = 64
ROT = 32
DOC_MAX = 512
BLOCK = 256
ROWS = 512

ln_eps = 1e-05
rope_base = 10000.0
mask_fill = -1e30
contract_rows = (((0,), (0,)), ((), ()))
contract_cols = (((1,), (1,)), ((), ()))
contract_in = (((1,), (0,)), ((), ()))
f32, bf16 = jnp.float32, jnp.bfloat16
MESH = pl.DeviceIdType.MESH

WEIGHTS = ("F1a", "F1b", "Qa", "Qb", "Da", "Db", "F2a", "F2b")
GRADS = ("f2a", "f2b", "qda", "qdb", "f1a", "f1b")
NEEDS = {
    "F1a": "F1a", "F1b": "F1b", "PRa": "Qa", "PRb": "Qb",
    "GAa": "Da", "GAb": "Db", "HGa": "F2a", "HGb": "F2b",
}
ATa0_, ATa1_, ATb0_, ATb1_, C_, Da_, Db_, END_ = "ATa0", "ATa1", "ATb0", "ATb1", "C", "Da", "Db", "END"
F1a_, F1b_, F2a_, F2b_, GAa_, GAb_, HGa_, HGb_ = "F1a", "F1b", "F2a", "F2b", "GAa", "GAb", "HGa", "HGb"
LN_, NORM_, NS_, OUT_, PRa_, PRb_, Qa_, Qb_ = "LN", "NORM", "NS", "OUT", "PRa", "PRb", "Qa", "Qb"
TAB_, U1a_, U1b_, U2a_, U2b_, UQa_, UQb_, WB_ = "TAB", "U1a", "U1b", "U2a", "U2b", "UQa", "UQb", "WB"
WI_, a_, act_, actw_, af1_, af2_, an_, b_ = "WI", "a", "act", "actw", "af1", "af2", "an", "b"
c3_, cA1_, cA2_, cB1_, cB2_, f1a_, f1b_, f2a_ = "c3", "cA1", "cA2", "cB1", "cB2", "f1a", "f1b", "f2a"
f2b_, fin_, finw_, fr_, fw_, h3_, hA1_, hA2_ = "f2b", "fin", "finw", "fr", "fw", "h3", "hA1", "hA2"
hB1_, hB2_, n_, n1_, nA2_, nA3_, nB2_, nB3_ = "hB1", "hB2", "n", "n1", "nA2", "nA3", "nB2", "nB3"
o0_, o0i_, o0o_, o1_, o1i_, o1o_, qda_, qdb_ = "o0", "o0i", "o0o", "o1", "o1i", "o1o", "qda", "qdb"
rf_, rn_, rsend_, st_, u_, u1_, uA2_, uA3_ = "rf", "rn", "rsend", "st", "u", "u1", "uA2", "uA3"
uB2_, uB3_, y_ = "uB2", "uB3", "y"
SCHEDULE = (
    (
        LN_,
        (
            (o0_, Qa_), (o0_, F1b_), (y_, Da_), (act_, cA1_),
            (act_, cB1_), (act_, hB1_), (y_, Db_), (act_, hA1_),
            (act_, cB2_), (o0_, F1a_), (o0_, F2b_), (y_, F1b_),
            (o0_, Db_), (o0_, Qb_), (o0_, F2a_), (act_, cA2_),
            (y_, F1a_), (act_, hB2_), (act_, hA2_), (o0_, Da_),
            (o1_, F1b_), (act_, c3_), (o1_, F1a_), (o1_, Da_),
            (y_, F2b_), (o1_, Db_), (y_, F2a_), (actw_, c3_),
            (y_, Qb_), (act_, h3_), (y_, Qa_), (o1_, F2b_),
            (o1_, F2a_), (actw_, h3_),
        ),
        (
            (o0o_, F1b_), (o0o_, Qb_), (y_, F1b_), (act_, cA1_),
            (y_, Qa_), (o0i_, F1b_), (o0i_, F1a_), (y_, F1a_),
            (act_, hB1_), (o1i_, F1b_), (o1o_, F1b_), (o0i_, Db_),
            (o0i_, Qb_), (an_, F1b_, 0), (act_, hA1_), (an_, Qa_, 0),
            (af1_, F1b_, 0), (o0o_, F2a_), (act_, cB1_), (act_, cA2_),
            (y_, Qb_), (o1i_, F1a_), (af1_, F1a_, 0), (an_, F1a_, 0),
            (act_, cB2_), (af2_, F1b_, 0), (af1_, F1b_, 1), (act_, hA2_),
            (af2_, Qa_, 0), (act_, hB2_), (o1o_, Qb_), (an_, F1b_, 1),
            (an_, F1a_, 1), (af2_, F1b_, 1), (an_, Da_, 0), (an_, Qb_, 0),
            (o1o_, F1a_), (act_, h3_), (an_, Da_, 1), (o0o_, F1a_),
            (y_, Da_), (o0i_, Da_), (act_, c3_), (af2_, F1a_, 1),
            (af1_, F1a_, 1), (af2_, F1a_, 0), (o1i_, Da_), (y_, Db_),
            (o1i_, Db_), (an_, Db_, 0), (actw_, h3_), (af2_, Da_, 0),
            (o0i_, Qa_), (o0o_, Da_),
        ),
    ),
    (
        F1b_,
        (
            (o1_, Qb_),
        ),
        (
            (actw_, c3_), (o1i_, Qa_),
        ),
    ),
    (
        U2b_,
        (
            (o1_, Qa_),
        ),
        (
            (y_, F2b_), (af2_, Da_, 1), (o1o_, Da_),
        ),
    ),
    (
        F1a_,
        (
            (rsend_, f2b_),
        ),
        (
            (af1_, Da_, 1),
        ),
    ),
    (
        U2a_,
        (),
        (
            (o0i_, F2a_), (y_, F2a_), (an_, Qb_, 1), (an_, Qa_, 1),
            (o0o_, Qa_), (af1_, Da_, 0), (an_, F2b_, 1),
        ),
    ),
    (
        TAB_,
        (
            (rsend_, f2a_),
        ),
        (),
    ),
    (
        GAa_,
        (),
        (),
    ),
    (
        PRa_,
        (),
        (
            (o1i_, Qb_), (o0i_, F2b_), (rn_, f2b_, 3, 0), (an_, Db_, 1),
            (af2_, Qa_, 1), (af1_, Qa_, 0), (o1o_, Qa_), (rn_, f2b_, 3, 1),
            (af1_, Qa_, 1),
        ),
    ),
    (
        ATa0_,
        (),
        (
            (af1_, Qb_, 0), (o0o_, Db_), (rn_, f2b_, 2, 1),
        ),
    ),
    (
        ATa1_,
        (),
        (
            (af1_, Db_, 0),
        ),
    ),
    (
        UQa_,
        (),
        (
            (rn_, f2b_, 2, 0), (af2_, Db_, 0), (o1o_, Db_),
        ),
    ),
    (
        PRb_,
        (
            (rsend_, qda_),
        ),
        (
            (an_, F2a_, 0), (an_, F2b_, 0), (af1_, Qb_, 1), (af2_, Qb_, 0),
            (o1i_, F2a_), (af2_, Qb_, 1), (af1_, Db_, 1),
        ),
    ),
    (
        GAb_,
        (),
        (
            (af2_, Db_, 1), (rf_, f2b_, 0),
        ),
    ),
    (
        ATb0_,
        (),
        (),
    ),
    (
        ATb1_,
        (),
        (),
    ),
    (
        UQb_,
        (),
        (
            (o1i_, F2b_),
        ),
    ),
    (
        HGb_,
        (
            (rsend_, qdb_), (fin_, f2b_, 0), (fin_, f2b_, 1), (fr_, b_),
        ),
        (
            (rf_, f2b_, 1), (o1o_, F2b_), (af1_, F2b_, 0), (af2_, F2b_, 1),
            (rn_, f2a_, 3, 0), (an_, F2a_, 1), (o0o_, F2b_), (fin_, f2b_, 0),
            (fin_, f2b_, 1), (rn_, f2a_, 2, 0), (af1_, F2b_, 1), (af2_, F2b_, 0),
        ),
    ),
    (
        U1b_,
        (),
        (
            (fr_, b_),
        ),
    ),
    (
        HGa_,
        (
            (fw_, b_), (rsend_, f1b_), (finw_, f2b_),
        ),
        (
            (af1_, F2a_, 0), (fin_, f2a_, 0), (af2_, F2a_, 0), (rn_, f2a_, 2, 1),
            (o1o_, F2a_), (rn_, qda_, 3, 0), (finw_, f2b_), (rn_, qda_, 2, 0),
            (af1_, F2a_, 1), (af2_, F2a_, 1),
        ),
    ),
    (
        NORM_,
        (
            (fin_, f2a_, 0),
        ),
        (
            (rn_, f2a_, 3, 1), (rn_, qda_, 2, 1),
        ),
    ),
    (
        U1a_,
        (
            (act_, n1_), (fin_, qda_, 0), (fin_, f2a_, 1), (fr_, a_),
            (fw_, a_),
        ),
        (
            (rf_, f2a_, 0), (fw_, b_), (act_, n1_), (act_, nA2_),
            (rn_, qda_, 3, 1), (act_, nB2_), (fin_, qda_, 1), (rn_, qdb_, 3, 0),
            (rf_, f2a_, 1), (rn_, f1b_, 3, 0), (rn_, qdb_, 2, 0), (fin_, f2a_, 1),
            (rf_, qda_, 0), (act_, nA3_), (rn_, qdb_, 3, 1), (act_, nB3_),
            (finw_, f2a_), (rn_, f1b_, 3, 1), (fr_, a_),
        ),
    ),
    (
        OUT_,
        (
            (rsend_, f1a_), (fin_, qdb_, 0), (act_, nA2_), (act_, nB2_),
        ),
        (
            (rn_, f1b_, 2, 0), (actw_, n_), (rf_, qdb_, 0), (rn_, qdb_, 2, 1),
            (fin_, qda_, 0),
        ),
    ),
    (
        NS_,
        (
            (act_, u1_), (fin_, f1b_, 0), (act_, nB3_), (act_, nA3_),
            (act_, uA2_), (act_, uB2_), (act_, uA3_), (fin_, f1a_, 0),
            (act_, uB3_), (actw_, n_),
        ),
        (
            (act_, u1_), (rf_, qdb_, 1), (fin_, qdb_, 0), (act_, uA2_),
            (rf_, f1b_, 0), (act_, uB2_), (fin_, f1b_, 0), (fw_, a_),
            (rf_, qda_, 1), (rn_, f1a_, 3, 0), (rn_, f1b_, 2, 1), (rn_, f1a_, 2, 0),
            (rf_, f1b_, 1), (act_, uB3_), (fin_, f1b_, 1), (rn_, f1a_, 2, 1),
            (act_, uA3_), (rn_, f1a_, 3, 1), (finw_, f1b_), (rf_, f1a_, 0),
            (fin_, qdb_, 1), (fin_, f1a_, 0),
        ),
    ),
    (
        WI_,
        (
            (act_, st_), (fin_, f1b_, 1), (finw_, f1b_), (actw_, u_),
            (fin_, f1a_, 1), (actw_, st_),
        ),
        (
            (act_, st_), (fin_, f1a_, 1), (finw_, qda_), (actw_, st_),
            (actw_, u_),
        ),
    ),
    (
        WB_,
        (),
        (),
    ),
    (
        END_,
        (
            (fin_, qdb_, 1), (finw_, f2a_), (fin_, qda_, 1), (finw_, qdb_),
            (finw_, qda_), (finw_, f1a_),
        ),
        (
            (rf_, f1a_, 1), (finw_, qdb_), (finw_, f1a_),
        ),
    ),
)


def fdot(a, b, dims=contract_in):
    return lax.dot_general(a, b, dims, preferred_element_type=f32)


def tiles(total, size, step):
    if total == size:
        step(0)
    else:
        pl.loop(0, total // size)(lambda i: step(pl.multiple_of(i * size, size)))


def bits_of(count):
    return [1 << i for i in range(count.bit_length() - 1)]


def halving_slots(C, T):
    return max(C * (T // 2 - 1) + C - 1, (T // 2) * (C - 1) + T // 2 - 1)


def block_kernel(dims, *refs):
    Z, C, T, r, fw, hw, lw, piece = dims
    (
        hid_hbm, cot_hbm, fc1w, qkvw, densew, fc2w, gain, bias, fc1b, qkvb, dense_b, fc2_b, segs, freqs,
        r_block, r_input, g_fc1, g_qd, g_fc2, r_fc1b, r_qkvb, r_outb, r_gain, r_bias,
        X, COT, W1, WQ, WD, W2, ACT, DG, TT, QV, GA, ATT, MI, COS, SIN, hid, cot_in,
        G2, R2, GQ, RQ, RT, RC, SM, SMR, ST, STR, qs, ks, dq, dk, dv,
        block_out, grad_input, o_fc1b, o_qkvb, o_outb, o_gain, o_bias,
        y_s, y_r, own_s, ag_s, ag_r, rs_s, rs_r, fin_s, fin_r, out_s,
        aa_s, aa_r, ar_s, ar_r, sm_s, sm_r, st_s, st_r, res_s, free,
    ) = refs
    L, D, U, last = piece * C, T * lw, Z * C, Z - 1
    fh, gw = fw // 2, min(hw, 128)
    groups, in_group, aligned = hw // gw, gw // HD, gw % 128 == 0
    z, c, t = lax.axis_index("dp"), lax.axis_index("ctx"), lax.axis_index("tensor")
    end_side, mid_side = z // last, z - 1
    end_in, mid_in, mid_out = z + 1 - 2 * end_side, last - z, last * mid_side
    is_end, is_mid = (z == 0) | (z == last), (z > 0) & (z < last)

    def remote(src, dst, send, recv, **where):
        return pltpu.make_async_remote_copy(
            src_ref=src, dst_ref=dst, send_sem=send, recv_sem=recv,
            device_id=where, device_id_type=MESH,
        )

    def exists(name):
        return groups == 2 or name[:2] not in ("Qb", "Db") and name != "qdb"

    def sub_offsets(own):
        return [0] if own else list(range(1, C))

    def weight(p, u, count=1):
        half = "ab".index(p[-1])
        units = u if count == 1 else pl.ds(u, count)
        rows = pl.ds(pl.multiple_of(u * r, r), count * r)
        if p[:2] == "F1":
            return W1.at[rows, half * fh : (half + 1) * fh]
        if p[0] == "Q":
            return WQ.at[half, :, rows]
        if p[0] == "D":
            return WD.at[units, half * gw : (half + 1) * gw]
        return W2.at[units, half * fh : (half + 1) * fh]

    def shard(p, k):
        half = "ab".index(p[-1])
        if p[:2] == "F1":
            return fc1w.at[:, pl.ds(pl.multiple_of(k * fw + half * fh, fh), fh)]
        if p[0] == "Q":
            if not aligned:
                return qkvw.at[k, half]
            return qkvw.at[:, :, pl.ds(pl.multiple_of(k * hw + half * gw, gw), gw)]
        if p[0] == "D":
            return densew.at[k, half * gw : (half + 1) * gw]
        return fc2w.at[k, half * fh : (half + 1) * fh]

    def y_copy(p, o):
        i, k = WEIGHTS.index(p), (c + o) % C
        return remote(shard(p, k), weight(p, z * C + c), y_s.at[i, o - 1], y_r.at[i, o - 1], ctx=k)

    def own_copy(p):
        i = WEIGHTS.index(p)
        return pltpu.make_async_copy(shard(p, c), weight(p, z * C + c), own_s.at[i])

    def ag_copy(p, u, way, to, src=None):
        i = WEIGHTS.index(p)
        src = weight(p, u) if src is None else src
        return remote(src, weight(p, u), ag_s.at[i, way], ag_r.at[i, u], dp=to)

    def ag_wait(p, u):
        ag_copy(p, u, 0, end_in).wait_recv()

    def y_start(p):
        for o in range(1, C):
            y_copy(p, o).start()
        own_copy(p).start()

    def send_own(p, second, way, to):
        if not second:
            ag_copy(p, z * C + c, way, to, shard(p, c)).start()
        for o in range(1, C) if second else ():
            ag_copy(p, z * C + (c - o) % C, way, to).start()

    def y_wait(p):
        for o in range(1, C):
            i, u, k = WEIGHTS.index(p), z * C + (c - o) % C, (c + o) % C
            remote(shard(p, k), weight(p, u), y_s.at[i, o - 1], y_r.at[i, o - 1], ctx=k).wait_recv()

    def forward(p, chunk, sub, way, to):
        for o in sub_offsets(sub == 0):
            u = chunk * C + (c - o) % C
            ag_wait(p, u)
            ag_copy(p, u, way, to).start()

    def weights_end(p):
        i = WEIGHTS.index(p)
        for o in range(1, C):
            y_copy(p, o).wait_send()

        def sent(way, chunk, chunks):
            region = weight(p, chunk * C, chunks * C)
            remote(region, region, ag_s.at[i, way], ag_r.at[i, 0], dp=mid_in).wait_send()

        pl.when(is_end)(lambda: sent(0, z, 1))

        @pl.when(is_mid)
        def _():
            sent(0, 2 * mid_side, 2)
            sent(1, 1 - mid_side, 3)

    def doubling(index, array, own, part, order):
        quarter = piece // 4
        skip, count_rows = ((0, 3 * quarter), (3 * quarter, quarter))[part]
        masks, blocks, at, plan = [0], 1, 0, []
        for axis, bit in order:
            plan.append((axis, bit, blocks, tuple(masks), at))
            at += len(masks) * blocks
            if axis == "c":
                blocks *= 2
            else:
                masks = masks + [m ^ bit for m in masks]

        def copies(stage):
            axis, bit, count, sent, first = plan[stage]
            where = {"ctx": c ^ bit} if axis == "c" else {"tensor": t ^ bit}
            found = []
            for b in range(count):
                start = ((c // count) * count + b) * piece + skip
                for j, m in enumerate(sent):
                    dst = array.at[
                        pl.ds(pl.multiple_of(start, quarter), count_rows),
                        pl.ds(pl.multiple_of((t ^ m) * lw, lw), lw),
                    ]
                    src = own.at[skip : skip + count_rows] if stage == 0 else dst
                    sem = first + b * len(sent) + j
                    found.append(remote(src, dst, aa_s.at[index, sem], aa_r.at[index, sem], **where))
            return found

        def begin(stage):
            for copy in copies(stage):
                copy.start()

        def arrive(stage):
            for copy in copies(stage):
                copy.wait_recv()

        def end():
            for stage in range(len(plan)):
                for copy in copies(stage):
                    copy.wait_send()

        return begin, arrive, end

    cbits = [("c", b) for b in bits_of(C)]
    tbits = [("t", b) for b in reversed(bits_of(T))]
    routes = (cbits + tbits, tbits[:-1] + cbits + tbits[-1:])
    doubles = {
        name + "AB"[part]: doubling(2 * i + part, array, own, part, routes[part])
        for i, (name, array, own) in enumerate((("h", X, hid_hbm), ("c", COT, cot_hbm)))
        for part in range(2)
    }
    doubling_stages = len(cbits) + len(tbits)

    def place(array, own, sem):
        return pltpu.make_async_copy(
            own,
            array.at[
                pl.ds(pl.multiple_of(c * piece, piece), piece), pl.ds(pl.multiple_of(t * lw, lw), lw)
            ],
            sem,
        )

    def load(i):
        return pltpu.make_async_copy((hid_hbm, cot_hbm)[i], (hid, cot_in)[i], own_s.at[10 + i])

    def double(name, step):
        if step == "3":
            for part in "AB":
                begin, arrive, _ = doubles[name + part]
                arrive(doubling_stages - 2)
                begin(doubling_stages - 1)
        else:
            begin, arrive, _ = doubles[name]
            stages = [0] if step == "1" else range(1, doubling_stages - 1)
            for stage in stages:
                if stage:
                    arrive(stage - 1)
                begin(stage)

    def double_wait(name):
        for part in "AB":
            doubles[name + part][1](doubling_stages - 1)

    def double_end(name):
        for part in "AB":
            doubles[name + part][2]()

    def grad_rows(q):
        return 4 * gw if q[0] == "q" else fh

    def grad_at(q, u, row, size, slots=False):
        half = "ab".index(q[-1])
        if q[0] == "q":
            return (RQ if slots else GQ).at[half, u, pl.ds(row, size)]
        return (R2 if slots else G2).at[u, pl.ds(half * fh + row, size)]

    def whole_at(q, u, slots=False):
        return grad_at(q, u, 0, grad_rows(q), slots)

    def grad_out(q):
        half = "ab".index(q[-1])
        if q[0] == "q":
            return g_qd.at[c, half]
        return (g_fc2 if q[1] == "2" else g_fc1).at[c, half * fh : (half + 1) * fh]

    def rs_copy(q, u, slot, way, number, to):
        i = GRADS.index(q) % 4
        return remote(
            whole_at(q, u), whole_at(q, slot, True), rs_s.at[i, way],
            rs_r.at[i, number * C + u % C], dp=to,
        )

    def rs_add(q, u, slots):
        size = min(128, grad_rows(q))

        def add(row):
            ref = grad_at(q, u, row, size)
            total = ref[...].astype(f32)
            for slot in slots:
                total = total + grad_at(q, slot, row, size, True)[...].astype(f32)
            ref[...] = total.astype(bf16)

        tiles(grad_rows(q), size, add)

    def rs_send(q):
        for k in range(last):
            d = end_side * k + (1 - end_side) * (last - k)
            for own in (False, True):
                for o in sub_offsets(own):
                    u = d * C + (c + o) % C
                    rs_copy(q, u, u + C * (1 - end_side), 0, k, end_in).start()

    def rs_near(q, dist, sub):
        d = last * (1 - mid_side) if dist == last else last - z
        for o in sub_offsets(sub == 1):
            u = d * C + (c + o) % C
            slot = u + C * (1 - mid_side)
            near = 0 if dist == last else 1
            rs_copy(q, u, slot, 0, near, mid_in).wait_recv()
            rs_add(q, u, [slot])
            rs_copy(q, u, slot, 0, last + near, mid_in).start()

    def rs_far(q, sub):
        for o in sub_offsets(sub == 1):
            u = last * mid_side * C + (c + o) % C
            slot = u + C * mid_side
            rs_copy(q, u, slot, 1, last, mid_out).wait_recv()
            rs_add(q, u, [slot])
            rs_copy(q, u, slot, 1, last, mid_out).start()

    def fin_copy(q, o):
        i, k = GRADS.index(q), (c + o) % C
        return remote(whole_at(q, z * C + k), grad_out(q), fin_s.at[i, o - 1], fin_r.at[i, o - 1], ctx=k)

    def fin_own(q):
        return pltpu.make_async_copy(
            whole_at(q, z * C + c), grad_out(q), out_s.at[GRADS.index(q)]
        )

    def finish(q, sub, at_end):
        for o in sub_offsets(sub == 1):
            u = z * C + (c + o) % C
            if at_end:
                slots = [u + C * end_side]
                rs_copy(q, u, slots[0], 1, last, end_in).wait_recv()
            else:
                slots = [u + C * (1 - mid_side), u + C * mid_side]
                for slot, number in zip(slots, (last - 1, last + 1)):
                    rs_copy(q, u, slot, 0, number, mid_in).wait_recv()
            rs_add(q, u, slots)
            if o:
                fin_copy(q, o).start()
            else:
                fin_own(q).start()

    def grads_sent(q):
        i, half = GRADS.index(q) % 4, "ab".index(q[-1])

        def sent(way, chunk, chunks):
            units = pl.ds(chunk * C, chunks * C)
            if q[0] == "q":
                region = GQ.at[half, units]
            else:
                region = G2.at[units, half * fh : (half + 1) * fh]
            remote(region, region, rs_s.at[i, way], rs_r.at[i, 0], dp=mid_in).wait_send()

        pl.when(is_end)(lambda: sent(0, 1 - end_side, last))

        @pl.when(is_mid)
        def _():
            sent(0, 2 - 2 * mid_side, 2)
            sent(1, last * mid_side, 1)

        for o in range(1, C):
            fin_copy(q, o).wait_send()
        fin_own(q).wait()

    def grads_arrived(q):
        for o in range(1, C):
            fin_copy(q, o).wait_recv()

    def tables():
        lane = lax.broadcasted_iota(jnp.int32, (128, gw), 1) % HD

        def rows_of(row):
            rows = pl.ds(row, 128)
            every = segs[...].astype(f32)
            own = jnp.broadcast_to(segs[:, rows].astype(f32), (128, 128)).T[:, 0:1]
            start = jnp.sum((every < own).astype(f32), axis=1, keepdims=True)
            at = (lax.broadcasted_iota(jnp.int32, (128, 1), 0) + row).astype(f32)
            angle = (at - start) * freqs[...]
            MI[rows, 2:3] = start
            COS[rows] = jnp.cos(angle)
            sine = jnp.sin(angle)
            SIN[rows] = jnp.where(lane < ROT // 2, -sine, sine)

        tiles(L, 128, rows_of)
        SM[...] = jnp.zeros_like(SM)
        for i in range(2):
            load(i).wait()
        SM[2:3, :lw] = jnp.sum(cot_in[...].astype(f32), axis=0, keepdims=True)

    def layer_norm():
        double_end("h")

        def rows_of(row):
            rows = pl.ds(row, 128)
            x = X[rows].astype(f32)
            mean = jnp.mean(x, axis=1, keepdims=True)
            centered = x - mean
            inv = lax.rsqrt(jnp.mean(centered * centered, axis=1, keepdims=True) + ln_eps)
            MI[rows, 0:1] = mean
            MI[rows, 1:2] = inv
            X[rows] = (centered * inv * gain[...] + bias[...]).astype(bf16)

        tiles(L, 128, rows_of)

    cf = min(BLOCK, fh)
    gelu_c = math.sqrt(2.0 / math.pi)

    def hidden(half):
        def cols_of(col):
            cols = pl.ds(half * fh + col, cf)
            shift = fc1b[:, pl.ds(pl.multiple_of(c * fw + half * fh + col, cf), cf)]

            def rows_of(row):
                rows = pl.ds(row, ROWS)
                v = fdot(X[rows], W1[:, cols]) + shift
                tanh = jnp.tanh(gelu_c * (v + 0.044715 * (v * v * v)))
                act = 0.5 * v * (1.0 + tanh)
                slope = gelu_c * (1.0 + 3.0 * 0.044715 * (v * v))
                DG[rows, cols] = (0.5 * (1.0 + tanh) + 0.5 * v * (1.0 - tanh * tanh) * slope).astype(bf16)
                ACT[rows, cols] = act.astype(bf16)
                TT[cols, rows] = act.T.astype(bf16)

            tiles(L, ROWS, rows_of)

        tiles(fh, cf, cols_of)

    def over_each_unit(step):
        if r % 128 == 0:
            pl.loop(0, U)(lambda u: step(u, pl.ds(pl.multiple_of(u * r, r), r)))
        else:
            for u in range(U):
                step(u, slice(u * r, (u + 1) * r))

    def unit_grads(q):
        half = "ab".index(q[-1])

        def step(u, cols):
            if q[0] == "q":
                first = half * 4 * gw
                GQ[half, u, : 3 * gw] = fdot(TT[first : first + 3 * gw], X[:, cols]).astype(bf16)
                GQ[half, u, 3 * gw :] = fdot(TT[first + 3 * gw : first + 4 * gw], COT[:, cols]).astype(bf16)
            else:
                rows = slice(half * fh, (half + 1) * fh)
                source = COT if q[1] == "2" else X
                G2[u, rows] = fdot(TT[rows], source[:, cols]).astype(bf16)

        over_each_unit(step)

    def side_by_side(rows, group):
        return jnp.concatenate([WQ[group, part, rows] for part in range(3)], axis=1)

    def project(group):
        def shift(part):
            if not aligned:
                return qkvb[part : part + 1]
            return qkvb[part : part + 1, pl.ds(pl.multiple_of(c * hw + group * gw, gw), gw)]

        shifts = jnp.concatenate([shift(part) for part in range(3)], axis=1)

        def rows_of(row):
            rows = pl.ds(row, ROWS)
            QV[group, rows] = (fdot(X[rows], side_by_side(pl.ds(0, D), group)) + shifts).astype(bf16)

        tiles(L, ROWS, rows_of)

    def over_units(rows, weights):
        total = None
        for u in range(U):
            term = fdot(COT[rows, u * r : (u + 1) * r], weights(u), contract_cols)
            total = term if total is None else total + term
        return total

    def attended_grads(group):
        def rows_of(row):
            rows = pl.ds(row, ROWS)
            lanes = slice(group * gw, (group + 1) * gw)
            GA[rows] = over_units(rows, lambda u: WD[u, lanes]).astype(bf16)

        tiles(L, ROWS, rows_of)

    half_rot = ROT // 2
    scale = 1.0 / math.sqrt(HD)

    def turn(values, rows, sign):
        lane = lax.broadcasted_iota(jnp.int32, values.shape, 1) % HD
        other = jnp.where(
            lane < half_rot, pltpu.roll(values, gw - half_rot, 1), pltpu.roll(values, half_rot, 1)
        )
        turned = other * SIN[rows]
        return values * COS[rows] + (turned if sign > 0 else -turned)

    def attention_load(group):
        def load(row):
            rows = pl.ds(row, BLOCK)
            qs[rows] = turn(QV[group, rows, :gw].astype(f32), rows, 1).astype(bf16)
            ks[rows] = turn(QV[group, rows, gw : 2 * gw].astype(f32), rows, 1).astype(bf16)

        tiles(L, BLOCK, load)
        for ref in (dq, dk, dv):
            ref[...] = jnp.zeros_like(ref)
        ATT[:, group * gw : (group + 1) * gw] = jnp.zeros((L, gw), bf16)

    def attention_head(group, head):
        own = slice(group * gw, (group + 1) * gw)
        for row in range(0, L, BLOCK):
            low = max(0, row - DOC_MAX)
            span = row + BLOCK - low
            rows, cols = pl.ds(row, BLOCK), pl.ds(low, span)
            mine = lax.broadcasted_iota(jnp.int32, (BLOCK, gw), 1) // HD == head
            query = jnp.where(mine, qs[rows].astype(f32), 0.0).astype(bf16)
            grad = jnp.where(mine, GA[rows].astype(f32), 0.0)
            grad_b, key, value = grad.astype(bf16), ks[cols], QV[group, cols, 2 * gw :]
            query_pos = row + lax.broadcasted_iota(jnp.int32, (BLOCK, span), 0)
            key_pos = low + lax.broadcasted_iota(jnp.int32, (BLOCK, span), 1)
            allowed = (key_pos >= MI[rows, 2:3].astype(jnp.int32)) & (key_pos <= query_pos)
            scores = jnp.where(allowed, fdot(query, key, contract_cols) * scale, mask_fill)
            weights = jnp.exp(scores - jnp.max(scores, axis=1, keepdims=True))
            probs = weights * (1.0 / jnp.sum(weights, axis=1, keepdims=True))
            probs_b = probs.astype(bf16)
            attended = jnp.where(mine, fdot(probs_b, value), 0.0).astype(bf16)
            delta = jnp.sum(grad * attended.astype(f32), axis=1, keepdims=True)
            grad_probs = fdot(grad_b, value, contract_cols)
            grad_scores = (probs * (grad_probs - delta)).astype(bf16)
            dv[cols] += fdot(probs_b, grad_b, contract_rows)
            dk[cols] += fdot(grad_scores, query, contract_rows)
            dq[rows] += jnp.where(mine, fdot(grad_scores, key), 0.0)
            ATT[rows, own] += attended

    def attention_save(group):
        first = group * 4 * gw

        def save(row):
            rows = pl.ds(row, BLOCK)
            attended = ATT[rows, group * gw : (group + 1) * gw].astype(f32)
            TT[first + 3 * gw : first + 4 * gw, rows] = attended.T.astype(bf16)
            grads = turn(dq[rows] * scale, rows, -1), turn(dk[rows] * scale, rows, -1), dv[rows]
            for part, grad in enumerate(grads):
                lanes = slice(part * gw, (part + 1) * gw)
                QV[group, rows, lanes] = grad.astype(bf16)
                TT[first + part * gw : first + (part + 1) * gw, rows] = grad.T.astype(bf16)
                sums = jnp.sum(grad.astype(bf16).astype(f32), axis=0, keepdims=True)
                SM[5 + group : 6 + group, lanes] += sums

        tiles(L, BLOCK, save)

    def attention_heads(group, second):
        mine = range(in_group // 2, in_group) if second else range(in_group // 2)
        if in_group == 1:
            mine = [] if second else [0]
        if not second:
            attention_load(group)
        for head in mine:
            attention_head(group, head)
        if second:
            attention_save(group)

    def hidden_grads(half):
        for n in range(fh // cf):
            cols = slice(half * fh + n * cf, half * fh + (n + 1) * cf)

            def rows_of(row):
                rows = pl.ds(row, ROWS)
                grad = over_units(rows, lambda u: W2[u, cols]) * DG[rows, cols].astype(f32)
                SM[0:1, cols] += jnp.sum(grad, axis=0, keepdims=True)
                DG[rows, cols] = grad.astype(bf16)
                TT[cols, rows] = grad.T.astype(bf16)

            tiles(L, ROWS, rows_of)

    rows_half = piece // 2

    def halving(a, part):
        first_bit, later_bits = bits_of(T)[0], [("t", b) for b in bits_of(T)[1:]]
        first_kept = [m for m in range(T) if not m & first_bit]
        c_bits = [("c", b) for b in reversed(bits_of(C))]

        def cols_of(m):
            return pl.ds(pl.multiple_of((t ^ m) * lw, lw), lw)

        def rows_at(block, which):
            return pl.ds(pl.multiple_of(block * piece + which * rows_half, rows_half), rows_half)

        def plan_of(order):
            plan, masks, blocks, slot = [], first_kept, C, 0
            for axis, bit in order:
                if axis == "t":
                    masks = [m for m in masks if not m & bit]
                else:
                    blocks = bit
                plan.append((axis, bit, masks, blocks, slot))
                slot += blocks * len(masks)
            return plan

        plans = plan_of(later_bits + c_bits), plan_of(c_bits + later_bits)

        def add(target, source, size):
            def rows_of(row):
                rows = pl.ds(row, 128)
                total = target.at[rows][...].astype(f32) + source.at[rows][...].astype(f32)
                target.at[rows][...] = total.astype(bf16)

            tiles(size, min(128, size), rows_of) if size % 128 == 0 else add_whole(target, source)

        def add_whole(target, source):
            target[...] = (target[...].astype(f32) + source[...].astype(f32)).astype(bf16)

        def first_copies():
            return [
                remote(
                    part.at[:, cols_of(m ^ first_bit)], RT.at[a, j],
                    ar_s.at[a, 0, j], ar_r.at[a, 0, j], tensor=t ^ first_bit,
                )
                for j, m in enumerate(first_kept)
            ]

        def copies(which, stage):
            axis, bit, masks, blocks, slot = plans[which][stage]
            where = {"ctx": c ^ bit} if axis == "c" else {"tensor": t ^ bit}
            start = (c ^ bit) // blocks * blocks if axis == "c" else c // blocks * blocks
            flip = 0 if axis == "c" else bit
            return [
                remote(
                    part.at[rows_at(start + b, which), cols_of(m ^ flip)],
                    RC.at[a, which, slot + b * len(masks) + j],
                    ar_s.at[a, 1 + which, slot + b * len(masks) + j],
                    ar_r.at[a, 1 + which, slot + b * len(masks) + j],
                    **where,
                )
                for b in range(blocks)
                for j, m in enumerate(masks)
            ]

        def arrive(which, stage):
            for copy in copies(which, stage):
                copy.wait_recv()
            axis, bit, masks, blocks, slot = plans[which][stage]
            if stage == len(plans[which]) - 1:
                return
            for b in range(blocks):
                for j, m in enumerate(masks):
                    add(
                        part.at[rows_at(c // blocks * blocks + b, which), cols_of(m)],
                        RC.at[a, which, slot + b * len(masks) + j],
                        rows_half,
                    )

        def begin(which, stage):
            for copy in copies(which, stage):
                copy.start()

        def run(step):
            if step == "1":
                for copy in first_copies():
                    copy.start()
                return
            which = "AB".index(step[0])
            if step[1] == "3":
                for stage in range(1, len(plans[which])):
                    arrive(which, stage - 1)
                    begin(which, stage)
                return
            if which == 0:
                for copy in first_copies():
                    copy.wait_recv()
                for j, m in enumerate(first_kept):
                    add(part.at[:, cols_of(m)], RT.at[a, j], L)
            begin(which, 0)

        def wait():
            for which in range(2):
                arrive(which, len(plans[which]) - 1)

        def total(row, size):
            which, slot = row // rows_half, None
            slot = plans[which][-1][4]
            rows = pl.ds(pl.multiple_of(c * piece + row, size), size)
            received = RC[a, which, slot, row % rows_half : row % rows_half + size]
            return part[rows, cols_of(0)].astype(f32) + received.astype(f32)

        def end():
            for copy in first_copies():
                copy.wait_send()
            for which in range(2):
                for stage in range(len(plans[which])):
                    for copy in copies(which, stage):
                        copy.wait_send()

        return run, wait, total, end

    n_run, n_wait, n_total, n_end = halving(0, COT)
    u_run, u_wait, u_total, u_end = halving(1, X)

    def norm_units():
        double_end("c")

        def step(u, cols):
            w1 = W1[pl.ds(pl.multiple_of(u * r, r), r)]
            wq = [side_by_side(pl.ds(pl.multiple_of(u * r, r), r), g) for g in range(groups)]

            def rows_of(row):
                rows = pl.ds(row, ROWS)
                total = fdot(DG[rows], w1, contract_cols)
                for g in range(groups):
                    total = total + fdot(QV[g, rows], wq[g], contract_cols)
                COT[rows, cols] = total.astype(bf16)

            tiles(L, ROWS, rows_of)

        over_each_unit(step)

    def out_units():
        def step(u, cols):
            def rows_of(row):
                rows = pl.ds(row, ROWS)
                X[rows, cols] = (fdot(ATT[rows], WD[u]) + fdot(ACT[rows], W2[u])).astype(bf16)

            tiles(L, ROWS, rows_of)

        over_each_unit(step)

    size = min(128, rows_half)

    def write_block():
        shift = dense_b[...] + fc2_b[...]
        for row in range(0, piece, size):
            rows = pl.ds(row, size)
            block_out[rows] = (hid[rows].astype(f32) + u_total(row, size) + shift).astype(bf16)
        final(0).start()

    def gain_own():
        return gain[:, pl.ds(pl.multiple_of(t * lw, lw), lw)]

    def standard_of(row):
        rows = pl.ds(pl.multiple_of(c * piece + row, size), size)
        inv = MI[rows, 1:2]
        return (hid[pl.ds(row, size)].astype(f32) - MI[rows, 0:1]) * inv, inv

    def norm_sums():
        for row in range(0, piece, size):
            grad = n_total(row, size)
            standard, _ = standard_of(row)
            scaled = grad * gain_own()
            first = jnp.sum(scaled, axis=1, keepdims=True)
            second = jnp.sum(scaled * standard, axis=1, keepdims=True)
            lane = lax.broadcasted_iota(jnp.int32, (size, 128), 1)
            pair = jnp.where(lane == 0, first, jnp.where(lane == 1, second, 0.0))
            ST[:, row : row + size] = pair.T[0:8]
            SM[3:4, :lw] += jnp.sum(grad * standard, axis=0, keepdims=True)
            SM[4:5, :lw] += jnp.sum(grad, axis=0, keepdims=True)

    def st_copy(o):
        return remote(ST, STR.at[o - 1], st_s.at[o - 1], st_r.at[o - 1], tensor=(t + o) % T)

    def sm_copy(dz, dc):
        o = dz * C + dc - 1
        return remote(
            SM, SMR.at[z * C + c], sm_s.at[o], sm_r.at[o], dp=(z + dz) % Z, ctx=(c + dc) % C
        )

    finals = (
        (block_out, r_block), (grad_input, r_input), (o_fc1b, r_fc1b), (o_qkvb, r_qkvb),
        (o_outb, r_outb), (o_gain, r_gain), (o_bias, r_bias),
    )

    def final(i):
        return pltpu.make_async_copy(*finals[i], res_s.at[i])

    offsets = [(dz, dc) for dz in range(Z) for dc in range(C) if dz or dc]

    def stats_start():
        for o in range(1, T):
            st_copy(o).start()
        for dz, dc in offsets:
            sm_copy(dz, dc).start()

    def stats_wait():
        for o in range(1, T):
            st_copy(o).wait()

    def write_input():
        for row in range(0, piece, size):
            stats = ST[:, row : row + size]
            for o in range(1, T):
                stats = stats + STR[o - 1, :, row : row + size]
            stats = jnp.concatenate([stats, jnp.zeros((120, size), f32)], axis=0).T * (1.0 / D)
            standard, inv = standard_of(row)
            scaled = n_total(row, size) * gain_own()
            rows = pl.ds(row, size)
            grad_input[rows] = cot_in[rows].astype(f32) + inv * (
                scaled - stats[:, 0:1] - standard * stats[:, 1:2]
            )
        final(1).start()

    def small_sums():
        SMR[z * C + c] = SM[...]
        for dz, dc in offsets:
            sm_copy(dz, dc).wait()

        def summed(row, size, units):
            total = SMR[units[0], row : row + 1, :size]
            for u in units[1:]:
                total = total + SMR[u, row : row + 1, :size]
            return total

        for k in range(C):
            units = [zs * C + k for zs in range(Z)]
            o_fc1b[:, k * fw : (k + 1) * fw] = summed(0, fw, units)
            for g in range(groups):
                sums = summed(5 + g, 3 * gw, units)
                for part in range(3):
                    lanes = slice(k * hw + g * gw, k * hw + (g + 1) * gw)
                    o_qkvb[part : part + 1, lanes] = sums[:, part * gw : (part + 1) * gw]
        for i, out in enumerate((o_outb, o_gain, o_bias)):
            out[...] = summed(2 + i, lw, list(range(U)))
        for i in range(2, len(finals)):
            final(i).start()

    computes = {"TAB": tables, "LN": layer_norm, "NORM": norm_units, "OUT": out_units}
    computes.update({"NS": norm_sums, "WI": write_input, "WB": write_block})
    for i, half in enumerate("ab"):
        computes["F1" + half] = partial(hidden, i)
        computes["U2" + half] = partial(unit_grads, "f2" + half)
        computes["U1" + half] = partial(unit_grads, "f1" + half)
        computes["HG" + half] = partial(hidden_grads, i)
        if i < groups:
            computes["PR" + half] = partial(project, i)
            computes["GA" + half] = partial(attended_grads, i)
            computes["AT" + half + "0"] = partial(attention_heads, i, False)
            computes["AT" + half + "1"] = partial(attention_heads, i, True)
            computes["UQ" + half] = partial(unit_grads, "qd" + half)

    def action(kind, name, *rest, at_end):
        if kind == "act" or kind == "actw":
            if name == "st":
                (stats_start if kind == "act" else stats_wait)()
            elif name[0] in "hc":
                if kind == "actw":
                    double_wait(name[0])
                elif name[1:] == "3":
                    double(name[0], "3")
                else:
                    double(name[:2], name[2])
            elif kind == "actw":
                (n_wait if name[0] == "n" else u_wait)()
            else:
                (n_run if name[0] == "n" else u_run)(name[1:])
        elif kind == "fr":
            grads_sent("f2" + name)
            half = "ab".index(name)

            def tell(to, way):
                pl.semaphore_signal(free.at[half, way], 1, device_id={"dp": to}, device_id_type=MESH)

            if at_end:
                tell(end_in, 0)
            else:
                tell(mid_in, 1)
                tell(mid_out, 1)
        elif kind == "fw":
            half = "ab".index(name)
            if not at_end:
                pl.semaphore_wait(free.at[half, 0], 1)
            pl.semaphore_wait(free.at[half, 1], 1)
        elif not exists(name):
            return
        elif kind == "y":
            y_start(name)
        elif kind == "o0":
            send_own(name, False, 0, end_in)
        elif kind == "o1":
            y_wait(name)
            send_own(name, True, 0, end_in)
        elif kind in ("o0i", "o0o", "o1i", "o1o"):
            if kind[1] == "1" and (name, "seen") not in seen:
                y_wait(name)
                seen.add((name, "seen"))
            way = "io".index(kind[2])
            send_own(name, kind[1] == "1", way, (mid_in, mid_out)[way])
        elif kind == "an":
            forward(name, mid_out, rest[0], 0, mid_in)
        elif kind == "af1":
            forward(name, mid_in, rest[0], 1, mid_out)
        elif kind == "af2":
            forward(name, last - mid_out, rest[0], 1, mid_out)
        elif kind == "rsend":
            rs_send(name)
        elif kind == "rn":
            rs_near(name, *rest)
        elif kind == "rf":
            rs_far(name, *rest)
        elif kind == "fin":
            finish(name, rest[0], at_end)

    seen = set()

    owns = (X, hid_hbm), (COT, cot_hbm)
    for i, (array, own) in enumerate(owns):
        place(array, own, own_s.at[8 + i]).start()
        load(i).start()

    barrier = pltpu.get_barrier_semaphore()

    def greet(**where):
        pl.semaphore_signal(barrier, 1, device_id=where, device_id_type=MESH)

    @pl.when(is_end)
    def _():
        greet(dp=end_in)

    @pl.when(is_mid)
    def _():
        greet(dp=mid_in)
        greet(dp=mid_out)

    for o in range(1, C):
        greet(ctx=(c + o) % C)
    for o in range(1, T):
        greet(tensor=(t + o) % T)
    pl.when(is_end)(lambda: pl.semaphore_wait(barrier, C + T - 1))
    pl.when(is_mid)(lambda: pl.semaphore_wait(barrier, C + T))
    for i, (array, own) in enumerate(owns):
        place(array, own, own_s.at[8 + i]).wait()

    for name, at_ends, inside in SCHEDULE:

        @pl.when(is_end)
        def _():
            for step in at_ends:
                action(*step, at_end=True)

        @pl.when(is_mid)
        def _():
            for step in inside:
                action(*step, at_end=False)

        if name not in computes:
            continue
        needed = NEEDS.get(name)
        if needed is not None:

            @pl.when(is_end)
            def _():
                for dz in range(1, Z):
                    for cs in range(C):
                        ag_wait(needed, ((z + dz) % Z) * C + cs)

            own_copy(needed).wait()
        computes[name]()

    small_sums()
    for q in GRADS:
        if exists(q):
            grads_arrived(q)
    n_end()
    u_end()
    for p in WEIGHTS:
        if exists(p):
            weights_end(p)
    for q in GRADS[2:]:
        if exists(q):
            grads_sent(q)
    for i in range(len(finals)):
        final(i).wait()


def body(
    hidden_in,
    segments,
    ln_gain,
    ln_bias,
    qkv_weight,
    qkv_bias,
    dense_weight,
    dense_bias,
    fc1_weight,
    fc1_bias,
    fc2_weight,
    fc2_bias,
    cotangent,
):
    _, piece, lw = hidden_in.shape
    C, T, Z = lax.axis_size("ctx"), lax.axis_size("tensor"), lax.axis_size("dp")
    L, D, U = piece * C, lw * T, Z * C
    r = qkv_weight.shape[0]
    hw, fw = lw // C, fc1_weight.shape[1] // C
    gw = min(hw, 128)
    groups, aligned = hw // gw, gw % 128 == 0
    lane = np.arange(gw) % HD
    freqs = rope_base ** (-((lane % (ROT // 2)) * 2.0) / ROT)
    freqs = jnp.asarray(np.where(lane < ROT, freqs, 0.0)[None], f32)
    if aligned:
        qkvw, own_bias = qkv_weight.transpose(1, 0, 2), qkv_bias
    else:
        qkvw = qkv_weight.reshape(r, 3, C, groups, gw).transpose(2, 3, 1, 0, 4)
        own_bias = lax.dynamic_slice_in_dim(qkv_bias, lax.axis_index("ctx") * hw, hw, 1)
    operands = [
        hidden_in[0],
        cotangent[0],
        fc1_weight,
        qkvw,
        dense_weight.reshape(C, hw, r),
        fc2_weight.reshape(C, fw, r),
        ln_gain[None],
        ln_bias[None],
        fc1_bias[None],
        own_bias,
        dense_bias[None],
        fc2_bias[None],
        segments,
        freqs,
    ]
    vmem, anywhere = pl.BlockSpec(memory_space=pltpu.VMEM), pl.BlockSpec(memory_space=pl.ANY)
    in_specs = [anywhere] * 6 + [vmem] * 8

    def out(shape, dtype=f32):
        return jax.ShapeDtypeStruct(shape, dtype)

    outs = [
        out((piece, lw), bf16),
        out((piece, lw)),
        out((C, fw, r), bf16),
        out((C, groups, 4 * gw, r), bf16),
        out((C, fw, r), bf16),
        out((1, C * fw)),
        out((3, lw)),
        out((1, lw)),
        out((1, lw)),
        out((1, lw)),
    ]
    out_specs = [anywhere] * 10
    most = max(fw, 3 * gw, lw)
    V = pltpu.VMEM
    dma = pltpu.SemaphoreType.DMA
    blocks, slots = C * T, max(halving_slots(C, T), T // 2)
    scratch = [
        V((L, D), bf16), V((L, D), bf16),
        V((D, fw), bf16), V((groups, 3, D, gw), bf16), V((U, hw, r), bf16), V((U, fw, r), bf16),
        V((L, fw), bf16), V((L, fw), bf16), V((max(fw, 4 * hw), L), bf16),
        V((groups, L, 3 * gw), bf16), V((L, gw), bf16), V((L, hw), bf16), V((L, 4), f32),
        V((L, gw), f32), V((L, gw), f32), V((piece, lw), bf16), V((piece, lw), bf16),
        V((U, fw, r), bf16), V((U + C, fw, r), bf16),
        V((groups, U, 4 * gw, r), bf16), V((groups, U + C, 4 * gw, r), bf16),
        V((2, T // 2, L, lw), bf16), V((2, 2, halving_slots(C, T), piece // 2, lw), bf16),
        V((8, most), f32), V((U, 8, most), f32), V((8, piece), f32), V((T - 1, 8, piece), f32),
        *[V((L, gw), bf16)] * 2, *[V((L, gw), f32)] * 3,
        *[V(o.shape, o.dtype) for o in outs[:2] + outs[5:]],
        dma((8, C - 1)), dma((8, C - 1)), dma((12,)), dma((8, 2)), dma((8, U)),
        dma((4, 2)), dma((4, 5 * C)), dma((6, C - 1)), dma((6, C - 1)), dma((6,)),
        dma((4, blocks)), dma((4, blocks)), dma((2, 3, slots)), dma((2, 3, slots)),
        dma((U - 1,)), dma((U - 1,)), dma((T - 1,)), dma((T - 1,)), dma((7,)),
        pltpu.SemaphoreType.REGULAR((2, 2)),
    ]
    results = pl.pallas_call(
        partial(block_kernel, (Z, C, T, r, fw, hw, lw, piece)),
        in_specs=in_specs,
        out_specs=out_specs,
        out_shape=outs,
        scratch_shapes=scratch,
        compiler_params=pltpu.CompilerParams(
            collective_id=0, has_side_effects=True, vmem_limit_bytes=67043328
        ),
        name="transformer_block",
    )(*operands)
    block_out, grad_input, g_fc1, g_qd, g_fc2, *sums = results
    if aligned and r % 128 == 0:
        block_out, grad_input, grad_fc1, grad_qkv, grad_dense, grad_fc2, *sums = unpack(results)
        grad_qkv = grad_qkv.transpose(1, 0, 2)
    else:
        sums.append(sums[2])
        grad_fc1 = g_fc1.astype(f32).transpose(2, 0, 1).reshape(r, C * fw)
        grad_qkv = g_qd[:, :, : 3 * gw].astype(f32).reshape(C, groups, 3, gw, r)
        grad_qkv = grad_qkv.transpose(4, 2, 0, 1, 3).reshape(r, 3, lw)
        grad_dense = g_qd[:, :, 3 * gw :].astype(f32).reshape(lw, r)
        grad_fc2 = g_fc2.astype(f32).reshape(C * fw, r)
    return (
        block_out[None],
        grad_input[None],
        grad_qkv,
        sums[1],
        grad_dense,
        sums[2][0],
        grad_fc1,
        sums[0][0],
        grad_fc2,
        sums[5][0],
        sums[3][0],
        sums[4][0],
    )


def unpack_kernel(gw, count, *refs):
    ins, outs, refs = refs[:count], refs[count : 2 * count + 2], refs[2 * count + 2 :]
    held, made, in_sem, out_sem = refs[:count], refs[count:-2], refs[-2], refs[-1]
    order = [4, 3, 2, 1, 0, *range(5, count)]
    reads = [pltpu.make_async_copy(ins[i], held[i], in_sem.at[i]) for i in range(count)]
    for i in order:
        reads[i].start()
    writes = []

    def write(src, out):
        copy = pltpu.make_async_copy(src, outs[out], out_sem.at[out])
        copy.start()
        writes.append(copy)

    blocks, quad = held[3].shape[:2]
    fc1, dense, qkv, fc2 = made
    for i in order:
        reads[i].wait()
        if i == 4:
            fc2[...] = held[4][...].astype(f32)
            write(fc2, 5)
        elif i == 3:
            for b in range(blocks):
                dense[b * gw : (b + 1) * gw] = held[3][b, 3 * gw :].astype(f32)
                for part in range(3):
                    source = held[3][b, part * gw : (part + 1) * gw].astype(f32)
                    qkv[part, :, b * gw : (b + 1) * gw] = source.T
            write(dense, 4)
            write(qkv, 3)
        elif i == 2:
            fc1[...] = held[2][...].astype(f32).T
            write(fc1, 2)
        elif i < 2:
            write(held[i], i)
        else:
            write(held[i], i + 1)
            if i == 7:
                write(held[i], count + 1)
    for copy in writes:
        copy.wait()


def unpack(results):
    block_out, grad_input, g_fc1, g_qd, g_fc2, *sums = results
    (piece, lw), (C, fw, r), (_, groups, quad, _) = block_out.shape, g_fc1.shape, g_qd.shape
    gw = quad // 4
    operands = [
        block_out, grad_input, g_fc1.reshape(C * fw, r), g_qd.reshape(C * groups, quad, r),
        g_fc2.reshape(C * fw, r), *sums,
    ]
    shapes = (r, C * fw), (3, r, lw), (lw, r), (C * fw, r)
    made = shapes[0], shapes[2], shapes[1], shapes[3]
    outs = [jax.ShapeDtypeStruct(a.shape, a.dtype) for a in operands[:2]]
    outs += [jax.ShapeDtypeStruct(s, f32) for s in (*shapes, *[s.shape for s in sums], sums[2].shape)]
    dma, count = pltpu.SemaphoreType.DMA, len(operands)
    anywhere = pl.BlockSpec(memory_space=pl.ANY)
    return pl.pallas_call(
        partial(unpack_kernel, gw, count),
        in_specs=[anywhere] * count,
        out_specs=[anywhere] * len(outs),
        out_shape=outs,
        scratch_shapes=[
            *[pltpu.VMEM(a.shape, a.dtype) for a in operands],
            *[pltpu.VMEM(s, f32) for s in made],
            dma((count,)), dma((len(outs),)),
        ],
        name="unpack_results",
    )(*operands)


def solution(mesh):
    in_specs = (
        P("dp", "ctx", "tensor"),
        P("dp", None),
        P(),
        P(),
        P(("dp", "ctx"), None, "tensor"),
        P(None, "tensor"),
        P("tensor", ("dp", "ctx")),
        P("tensor"),
        P(("dp", "ctx"), "tensor"),
        P("tensor"),
        P("tensor", ("dp", "ctx")),
        P("tensor"),
        P("dp", "ctx", "tensor"),
    )
    out_specs = (
        P("dp", "ctx", "tensor"),
        P("dp", "ctx", "tensor"),
        P(("dp", "ctx"), None, "tensor"),
        P(None, "tensor"),
        P("tensor", ("dp", "ctx")),
        P("tensor"),
        P(("dp", "ctx"), "tensor"),
        P("tensor"),
        P("tensor", ("dp", "ctx")),
        P("tensor"),
        P("tensor"),
        P("tensor"),
    )
    return jax.shard_map(body, mesh=mesh, in_specs=in_specs, out_specs=out_specs, check_vma=False)
```
